256 devices in a mesh: pix: 32 (over z_hi, x, core), rep: 8 (over y, z_lo).
Axes of the slice: x: 4, y: 4, z: 8 (z_hi: 4, z_lo: 2; z = z_hi * 2 + z_lo), core: 2. Of those that a mesh axis runs over, the one named last changes fastest.
Arguments:
- tokens: bfloat16 [2048, 16, 1152], P(('pix', 'rep')), may hold values from -48 to 48
- out_grad: bfloat16 [2048, 16, 1152], P(('pix', 'rep')), may hold values from -6 to 6
- query_weight: bfloat16 [1152, 1152], P('pix'), may hold values from -0.1875 to 0.1875
- key_weight: bfloat16 [1152, 1152], P('pix'), may hold values from -0.1875 to 0.1875
- value_weight: bfloat16 [1152, 1152], P('pix'), may hold values from -0.1875 to 0.1875
- output_weight: bfloat16 [1152, 1152], P('pix'), may hold values from -0.1875 to 0.1875
Outputs:
- input_grad: bfloat16 [2048, 16, 1152], P(('pix', 'rep'))
- weight_grads: float32 [1152, 4608], P('pix')
The draws below stay inside these ranges and needn't reach their ends.
All inputs are finite; a program needn't handle non-finite values.
Results may differ from the reference program's by a relative error of at most 0.025.
The reference program's roundings to bfloat16 on the way count: a program that leaves them out, or rounds other values in their place, can miss the bound.
Values may be sent and summed in bfloat16 or wider, within the bound.
A program may use at most 128 MiB of HBM per device.

```python
import jax
import jax.numpy as jnp
from jax import lax

D = 1152
HEADS = 16
HEAD_DIM = 72
FRAMES = 16
SITE_DEV = 8
SITES = 2048
N_PIX = 32
N_REP = 8


def draw_tokens(key, part):
    base_key, perm_key = jax.random.split(jax.random.fold_in(key, 11), 2)
    base = jnp.clip(jax.random.normal(base_key, (SITES, FRAMES, D), jnp.float32), -4.0, 4.0)
    sites = jnp.arange(SITES, dtype=jnp.int32)
    pix_index = sites // SITE_DEV // N_REP
    paired = jax.random.permutation(perm_key, N_PIX)
    column_block = jnp.arange(D, dtype=jnp.int32) // (D // N_PIX)
    chosen = paired[pix_index]
    spike = jnp.where(column_block[None, :] == chosen[:, None], 3.0, 1.0)
    values = base * spike[:, None, :]
    return values.astype(jnp.bfloat16)


def block_scale(stream_key, extent, shards, least, high):
    def one(position, parts):
        heights = jax.random.uniform(jax.random.fold_in(jax.random.fold_in(stream_key, 6), position), (parts,), jnp.float32, least / len(shards), high / len(shards))
        return jnp.repeat(jnp.exp(heights), extent[position] // parts).reshape((-1,) + (1,) * (len(extent) - position - 1))

    level = one(*shards[0])
    for cut in shards[1:]:
        level = level * one(*cut)
    return level


def noise(stream_key, shape, deviation, limit, cuts=(), held_as=jnp.bfloat16):
    values = jax.random.normal(stream_key, shape, jnp.float32) * deviation
    if len(cuts) > 0:
        values = block_scale(stream_key, shape, cuts, -0.22, 0.18) * values
    return jnp.clip(values, min=-limit, max=limit).astype(held_as)


def setup_inputs(seed: int = 0) -> dict:
    key_of = jax.random.split(jax.random.key(seed), 7)
    return {
        "tokens": draw_tokens(jax.random.fold_in(key_of[6], 71), 0),
        "out_grad": noise(key_of[1], (SITES, FRAMES, D), 1.0, 6.0, ((0, 256),)),
        "query_weight": noise(key_of[2], (D, D), D ** -0.5, 0.1875, ((0, 32),)),
        "key_weight": noise(key_of[3], (D, D), D ** -0.5, 0.1875, ((0, 32),)),
        "value_weight": noise(key_of[4], (D, D), D ** -0.5, 0.1875, ((0, 32),)),
        "output_weight": noise(key_of[5], (D, D), D ** -0.5, 0.1875, ((0, 32),)),
    }


def contract_last(left, right):
    return lax.dot_general(left, right, (((1,), (1,)), ((), ())), preferred_element_type=jnp.float32)


def contract_first(left, right):
    return lax.dot_general(left, right, (((0,), (0,)), ((), ())), preferred_element_type=jnp.float32)


def block_step(block_x, block_d, query_weight, key_weight, value_weight, output_weight):
    count = block_x.shape[0]
    rows = block_x.reshape(-1, D)
    drows = block_d.reshape(-1, D)
    scale = 1.0 / (HEAD_DIM ** 0.5)
    query = jnp.dot(rows, query_weight, preferred_element_type=jnp.float32).astype(jnp.bfloat16)
    keyed = jnp.dot(rows, key_weight, preferred_element_type=jnp.float32).astype(jnp.bfloat16)
    valued = jnp.dot(rows, value_weight, preferred_element_type=jnp.float32).astype(jnp.bfloat16)
    shape4 = (count, FRAMES, HEADS, HEAD_DIM)
    qh = query.reshape(shape4).astype(jnp.float32)
    kh = keyed.reshape(shape4).astype(jnp.float32)
    vh = valued.reshape(shape4).astype(jnp.float32)
    scores = jnp.einsum('sfhe,sghe->shfg', qh, kh) * scale
    scores = scores - jnp.max(scores, axis=-1, keepdims=True)
    expo = jnp.exp(scores)
    probs = expo / jnp.sum(expo, axis=-1, keepdims=True)
    probs_b = probs.astype(jnp.bfloat16).astype(jnp.float32)
    attended = jnp.einsum('shfg,sghe->sfhe', probs_b, vh).reshape(-1, D).astype(jnp.bfloat16)
    dattn = contract_last(drows, output_weight).astype(jnp.bfloat16)
    dah = dattn.reshape(shape4).astype(jnp.float32)
    dvalue = jnp.einsum('shfg,sfhe->sghe', probs_b, dah).reshape(-1, D).astype(jnp.bfloat16)
    dprobs = jnp.einsum('sfhe,sghe->shfg', dah, vh)
    dscore = (probs * (dprobs - jnp.sum(dprobs * probs, axis=-1, keepdims=True)) * scale).astype(jnp.bfloat16).astype(jnp.float32)
    dquery = jnp.einsum('shfg,sghe->sfhe', dscore, kh).reshape(-1, D).astype(jnp.bfloat16)
    dkey = jnp.einsum('shfg,sfhe->sghe', dscore, qh).reshape(-1, D).astype(jnp.bfloat16)
    dinput = contract_last(dquery, query_weight) + contract_last(dkey, key_weight) + contract_last(dvalue, value_weight)
    partial_value = jnp.concatenate([contract_first(rows, dquery), contract_first(rows, dkey), contract_first(rows, dvalue), contract_first(attended, drows)], axis=1)
    partial_value = lax.optimization_barrier(partial_value.astype(jnp.bfloat16)).astype(jnp.float32)
    return dinput.astype(jnp.bfloat16).reshape(count, FRAMES, D), partial_value


def reference(tokens, out_grad, query_weight, key_weight, value_weight, output_weight):
    blocks = tokens.shape[0] // SITE_DEV
    xs = tokens.reshape(blocks, SITE_DEV, FRAMES, D)
    ds = out_grad.reshape(blocks, SITE_DEV, FRAMES, D)

    def step(total, pair):
        dinput, partial_value = block_step(pair[0], pair[1], query_weight, key_weight, value_weight, output_weight)
        return total + partial_value, dinput

    init = jnp.zeros((D, 4 * D), jnp.float32)
    total, dinputs = lax.scan(step, init, (xs, ds))
    return dinputs.reshape(tokens.shape), total
```

```python
import jax
import jax.numpy as jnp
from jax import lax
from jax.experimental import pallas as pl
from jax.experimental.pallas import tpu as pltpu
from jax.sharding import Mesh
from jax.sharding import PartitionSpec as P

D = 1152
FRAMES = 16
HEAD_DIM = 72
ZH, NX, NC, NY, ZL = 4, 4, 2, 4, 2
NZ = ZH * ZL
NPIX = ZH * NX * NC
NREP = NY * ZL
ROWS = 128
RP = D // NPIX
COLS = 2 * HEAD_DIM
RA = 128
RO = 48
RF = RA + RO
BF = jnp.bfloat16
F32 = jnp.float32
AXES = ("zh", "x", "c", "y", "zl")


def dot_nn(a, b):
    return lax.dot_general(a, b, (((1,), (0,)), ((), ())), preferred_element_type=F32)


def dot_nt(a, b):
    return lax.dot_general(a, b, (((1,), (1,)), ((), ())), preferred_element_type=F32)


def dot_tn(a, b):
    return lax.dot_general(a, b, (((0,), (0,)), ((), ())), preferred_element_type=F32)


def roll(v, shift):
    shift = shift % 128
    return v if shift == 0 else pltpu.roll(v, shift, 1)


def lanes(rows):
    return lax.broadcasted_iota(jnp.int32, (rows, 128), 1)


def kernel(
    x_ref, d_ref, wq_ref, wk_ref, wv_ref, wo_ref, gi_ref, gw_ref,
    XA, DA, WS, OSRC, WL, OL, WCAT, WOC, DQKV, AS, DXP, DXS, DXC, DXR,
    DWB, DWOB, DWS, RX, R2S, RZ, OS, OR, FL,
    lsem, a_s, a_r, w1s, w2s, w_r, o_s, o_r, xs_s, xs_r, xy_s, xy_r,
    r1_s, r1_r, r2_s, r2_r, ro_s, ro_r, f_s, f_r,
):
    zh, x, c, y, zl = [lax.axis_index(a) for a in AXES]
    pix = (zh * NX + x) * NC + c
    rep = y * ZL + zl
    z = zh * ZL + zl
    sib = 1 - c

    def rcopy(src, dst, ss, rs, dev):
        return pltpu.make_async_remote_copy(
            src_ref=src, dst_ref=dst, send_sem=ss, recv_sem=rs,
            device_id=dev, device_id_type=pl.DeviceIdType.MESH,
        )

    me = (zh, x, c, y, zl)
    acts = (XA, DA)

    def blk(kind, yb, cb):
        return acts[kind].at[yb, pl.ds(pl.multiple_of(cb * ROWS, ROWS), ROWS)]

    def act(kind, yb, cb, to_y, to_c, idx):
        return rcopy(
            blk(kind, yb, cb), blk(kind, yb, cb), a_s.at[idx],
            a_r.at[kind * 8 + yb * 2 + cb], (zh, x, to_c, to_y, zl),
        )

    own = [pltpu.make_async_copy(r, blk(k, y, c), lsem.at[k]) for k, r in enumerate((x_ref, d_ref))]
    for o in own:
        o.start()
    for o in own:
        o.wait()
    right, left, opp = (y + 1) % NY, (y + 3) % NY, (y + 2) % NY
    sends = [
        act(0, y, c, right, c, 0), act(1, y, c, left, c, 1),
        act(1, y, c, right, c, 2), act(0, y, c, left, c, 3),
        act(0, y, c, y, sib, 4), act(1, y, c, y, sib, 5),
    ]
    for s in sends:
        s.start()

    ii = lax.broadcasted_iota(jnp.int32, (D, 256), 0)
    nn = lax.broadcasted_iota(jnp.int32, (D, 256), 1)
    sel = jnp.where((ii == nn + COLS * rep) & (nn < COLS), 1.0, 0.0).astype(BF)
    tail = None
    for s, w in enumerate((wq_ref, wk_ref, wv_ref)):
        b = dot_nn(w[...], sel)
        WS[RP * s : RP * s + RP, :] = b[:, :128].astype(BF)
        t = b[:, 128:256]
        t = roll(t[: RP // 2], 32 * s) + roll(t[RP // 2 :], 32 * s + 16)
        tail = t if tail is None else tail + t
    WS[3 * RP : 3 * RP + RP // 2, :] = tail.astype(BF)
    want = jnp.where(nn < 128, nn + 128 * rep, nn - 128 + 1024 + 16 * rep)
    sel = jnp.where((ii == want) & (nn < COLS), 1.0, 0.0).astype(BF)
    b = dot_nn(wo_ref[...], sel)
    OSRC[:RP, :] = b[:, :128].astype(BF)
    t = b[:, 128:256]
    tail = t[:12] + roll(t[12:24], 16) + roll(t[24:36], 32)
    OSRC[RP : RP + 12, :] = tail.astype(BF)

    selfcore = zl == c

    @pl.when(selfcore)
    def _():
        WL[pix] = WS[...]

    def w1(i):
        zh2, zl2 = i // 2, i % 2
        return rcopy(WS, WL.at[pix], w1s.at[i], w_r.at[pix], (zh2, x, zl, y, zl2))

    def w1_not_self(i):
        return jnp.logical_not((i == z) & selfcore)

    @pl.loop(0, NZ)
    def _(i):
        @pl.when(w1_not_self(i))
        def _():
            w1(i).start()

    oslot = ((x % 2) * 2 + c) * NREP + rep
    oself = (zh == y) & (x // 2 == c)

    @pl.when(oself)
    def _():
        OL[oslot] = OSRC[...]

    def osend(i):
        dev = (i // 8, (i // 2) % 4, x // 2, zh, i % 2)
        return rcopy(OSRC, OL.at[oslot], o_s.at[i], o_r.at[oslot], dev)

    mine = (zh * NX + x) * ZL + zl

    def o_not_self(i):
        return jnp.logical_not((i == mine) & oself)

    @pl.loop(0, 32)
    def _(i):
        @pl.when(o_not_self(i))
        def _():
            osend(i).start()

    def w2(k, dx):
        p = ((k // 2) * NX + x) * NC + k % 2
        return rcopy(WL.at[p], WL.at[p], w2s.at[k * 3 + dx - 1], w_r.at[p], (zh, (x + dx) % NX, c, y, zl))

    def w_wait(p):
        rcopy(WL.at[p], WL.at[p], w2s.at[0], w_r.at[p], me).wait_recv()

    @pl.loop(0, 8)
    def _(k):
        p = ((k // 2) * NX + x) * NC + k % 2

        @pl.when(jnp.logical_not((p == pix) & selfcore))
        def _():
            w_wait(p)

        for dx in range(1, NX):
            w2(k, dx).start()

    def await_act(kind, yb, cb):
        act(kind, yb, cb, y, sib, 0).wait_recv()

    fwd = [
        act(0, left, c, right, c, 6), act(1, right, c, left, c, 7),
        act(0, left, c, y, sib, 8), act(1, right, c, y, sib, 9),
        act(1, left, c, y, sib, 10), act(0, right, c, y, sib, 11),
        act(0, opp, c, y, sib, 12), act(1, opp, c, y, sib, 13),
    ]
    await_act(0, left, c)
    fwd[0].start()
    fwd[2].start()
    await_act(1, right, c)
    fwd[1].start()
    fwd[3].start()
    await_act(1, left, c)
    fwd[4].start()
    await_act(0, right, c)
    fwd[5].start()
    await_act(0, opp, c)
    fwd[6].start()
    await_act(1, opp, c)
    fwd[7].start()

    @pl.loop(0, 24)
    def _(i):
        k, x2 = i % 8, (x + 1 + i // 8) % NX
        w_wait(((k // 2) * NX + x2) * NC + k % 2)

    @pl.loop(0, 32)
    def _(i):
        @pl.when(jnp.logical_not((i == oslot) & oself))
        def _():
            rcopy(OL.at[i], OL.at[i], o_s.at[0], o_r.at[i], me).wait_recv()

    low16 = lanes(RP // 2) < 16

    @pl.loop(0, 8)
    def _(g):
        out = WCAT.at[pl.ds(pl.multiple_of(g * 144, 16), 144)]
        for q in range(4):
            p = g * 4 + q
            base = RP * q
            tl = WL[p, 3 * RP : 3 * RP + RP // 2, :].astype(F32)
            for s in range(3):
                out[base : base + RP, 256 * s : 256 * s + 128] = WL[p, RP * s : RP * s + RP, :]
                for half in range(2):
                    v = jnp.where(low16, roll(tl, -(32 * s + 16 * half)), 0.0).astype(BF)
                    at = base + half * (RP // 2)
                    out[at : at + RP // 2, 256 * s + 128 : 256 * s + 256] = v

    WOC[COLS:, :] = jnp.zeros((256 - COLS, D), BF)
    lane12 = lanes(12)
    for q in range(4):
        parts = [None] * 3
        for r in range(NREP):
            WOC[RP * q : RP * q + RP, 128 * r : 128 * r + 128] = OL[q * NREP + r, :RP, :]
            tl = OL[q * NREP + r, RP : RP + 12, :].astype(F32)
            for t in range(3):
                v = jnp.where(lane12 // 16 == t, tl, 0.0)
                v = roll(v, 16 * (r - t))
                parts[t] = v if parts[t] is None else parts[t] + v
        for t in range(3):
            at = RP * q + 12 * t
            WOC[at : at + 12, 1024:1152] = parts[t].astype(BF)

    scale = 1.0 / HEAD_DIM**0.5
    row = lax.broadcasted_iota(jnp.int32, (ROWS, 128), 0)
    col = lax.broadcasted_iota(jnp.int32, (ROWS, 128), 1)
    inside = row // FRAMES == col // FRAMES
    lane256 = lax.broadcasted_iota(jnp.int32, (ROWS, 256), 1)
    first = lane256 < HEAD_DIM
    zero = jnp.zeros((ROWS, 256), BF)

    def two_heads(v):
        return jnp.concatenate([jnp.where(first, v, zero), jnp.where(first, zero, v)], axis=0)

    def dx_sib(i):
        return rcopy(
            DXP.at[i, pl.ds(pl.multiple_of(sib * ROWS, ROWS), ROWS)], DXS.at[i],
            xs_s.at[i], xs_r.at[i], (zh, x, sib, y, zl),
        )

    @pl.loop(0, NY)
    def _(off):
        i = (y + off) % NY

        @pl.when(off == 0)
        def _():
            await_act(0, y, sib)
            await_act(1, y, sib)

        @pl.when(off > 0)
        def _():
            await_act(0, i, sib)
            await_act(1, i, sib)

        qkv = dot_nn(XA[i], WCAT[...]).astype(BF)
        da = dot_nt(DA[i], WOC[...]).astype(BF)
        for h in range(2):
            rs = slice(h * ROWS, h * ROWS + ROWS)
            q, k, v, g = qkv[rs, :256], qkv[rs, 256:512], qkv[rs, 512:], da[rs]
            kk, vv = two_heads(k), two_heads(v)
            sc = dot_nt(q, kk) * scale
            dp = dot_nt(g, vv)
            probs, dscore = [], []
            for n in range(2):
                cs = slice(n * 128, n * 128 + 128)
                s1 = jnp.where(inside, sc[:, cs], -jnp.inf)
                e = jnp.exp(s1 - jnp.max(s1, axis=1, keepdims=True))
                p1 = e / jnp.sum(e, axis=1, keepdims=True)
                d1 = dp[:, cs]
                t1 = jnp.sum(d1 * p1, axis=1, keepdims=True)
                probs.append(p1.astype(BF))
                dscore.append((p1 * (d1 - t1) * scale).astype(BF))
            pb = jnp.concatenate(probs, axis=1)
            ds = jnp.concatenate(dscore, axis=1)
            AS[i, rs, :] = dot_nn(pb, vv).astype(BF)
            DQKV[i, rs, :256] = dot_nn(ds, kk).astype(BF)
            dk = dot_tn(ds, q)
            DQKV[i, rs, 256:512] = jnp.where(first, dk[:128], dk[128:]).astype(BF)
            dv = dot_tn(pb, g)
            DQKV[i, rs, 512:] = jnp.where(first, dv[:128], dv[128:]).astype(BF)
        DXP[i] = dot_nt(DQKV[i], WCAT[...]).astype(BF)
        dx_sib(i).start()

    dq_all = DQKV[...].reshape(NY * 256, 768)

    @pl.loop(0, 9)
    def _(i):
        at = pl.multiple_of(i * 128, 128)
        lhs = XA[:, :, pl.ds(at, 128)].reshape(NY * 256, 128)
        DWB[pl.ds(at, 128), :] = dot_tn(lhs, dq_all).astype(BF)

    @pl.loop(0, 8)
    def _(g):
        src = DWB.at[pl.ds(pl.multiple_of(g * 144, 16), 144)]
        for q in range(4):
            p = g * 4 + q
            x2, k = (p // 2) % NX, (p // 8) * 2 + p % 2
            base = RP * q
            tail = None
            for s in range(3):
                DWS[x2, k, RP * s : RP * s + RP, :] = src[base : base + RP, 256 * s : 256 * s + 128]
                t = src[base : base + RP, 256 * s + 128 : 256 * s + 256].astype(F32)
                t = roll(t[: RP // 2], 32 * s) + roll(t[RP // 2 :], 32 * s + 16)
                tail = t if tail is None else tail + t
            DWS[x2, k, 3 * RP : 3 * RP + RP // 2, :] = tail.astype(BF)

    def r1(dx):
        x2 = (x + dx) % NX
        return rcopy(DWS.at[x2], RX.at[x], r1_s.at[dx - 1], r1_r.at[x], (zh, x2, c, y, zl))

    for dx in range(1, NX):
        r1(dx).start()

    DWOB[...] = dot_tn(AS[...].reshape(NY * 256, 256), DA[...].reshape(NY * 256, D)).astype(BF)
    for q in range(4):
        tt = [DWOB[RP * q + 12 * t : RP * q + 12 * t + 12, 1024:1152].astype(F32) for t in range(3)]
        for r in range(NREP):
            OS[q * NREP + r, :RP, :] = DWOB[RP * q : RP * q + RP, 128 * r : 128 * r + 128]
            tail = None
            for t in range(3):
                v = roll(jnp.where(lane12 // 16 == r, tt[t], 0.0), 16 * (t - r))
                tail = v if tail is None else tail + v
            OS[q * NREP + r, RP : RP + 12, :] = tail.astype(BF)

    def ro(i):
        q, r = i // NREP, i % NREP
        dev = (y, 2 * c + q // 2, q % 2, r // ZL, r % ZL)
        return rcopy(OS.at[i], OR.at[mine], ro_s.at[i], ro_r.at[mine], dev)

    def ro_not_self(i):
        return jnp.logical_not((i == oslot) & oself)

    @pl.loop(0, 32)
    def _(i):
        @pl.when(ro_not_self(i))
        def _():
            ro(i).start()

    @pl.when(oself)
    def _():
        OR[mine] = OS[oslot]

    def dx_y(dy):
        i = (y + dy) % NY
        return rcopy(DXC.at[i], DXR.at[dy - 1], xy_s.at[dy - 1], xy_r.at[dy - 1], (zh, x, c, i, zl))

    for dy in (1, 3, 2, 0):
        i = (y + dy) % NY
        dx_sib(i).wait_recv()
        both = DXP[i, pl.ds(pl.multiple_of(c * ROWS, ROWS), ROWS), :].astype(F32) + DXS[i].astype(F32)
        if dy:
            DXC[i] = both.astype(BF)
            dx_y(dy).start()

    for dx in range(1, NX):
        x2 = (x + dx) % NX
        rcopy(RX.at[x2], RX.at[x2], r1_s.at[0], r1_r.at[x2], me).wait_recv()

    def r2(k):
        return rcopy(R2S.at[k], RZ.at[z], r2_s.at[k], r2_r.at[z], (k // 2, x, k % 2, y, c))

    kown = zh * 2 + c

    @pl.loop(0, 8)
    def _(k):
        acc = DWS[x, k].astype(F32)
        for dx in range(1, NX):
            acc = acc + RX[(x + dx) % NX, k].astype(F32)
        R2S[k] = acc.astype(BF)

        @pl.when(jnp.logical_not((k == kown) & selfcore))
        def _():
            r2(k).start()

    @pl.when(selfcore)
    def _():
        RZ[z] = R2S[kown]

    for dy in range(1, NY):
        dx_y(dy).wait_recv()
    both = both + DXR[0].astype(F32) + DXR[1].astype(F32) + DXR[2].astype(F32)
    gi_ref[...] = both.astype(BF)

    @pl.loop(0, 32)
    def _(i):
        @pl.when(jnp.logical_not((i == mine) & oself))
        def _():
            rcopy(OR.at[i], OR.at[i], ro_s.at[0], ro_r.at[i], me).wait_recv()

    osum = OR[0].astype(F32)
    for i in range(1, 32):
        osum = osum + OR[i].astype(F32)
    FL[rep, RA:, :] = osum.astype(BF)

    @pl.loop(0, NZ)
    def _(i):
        @pl.when(jnp.logical_not((i == z) & selfcore))
        def _():
            rcopy(RZ.at[i], RZ.at[i], r2_s.at[0], r2_r.at[i], me).wait_recv()

    asum = RZ[0].astype(F32)
    for i in range(1, NZ):
        asum = asum + RZ[i].astype(F32)
    FL[rep, :RA, :] = asum.astype(BF)

    def fin(dr):
        r = (rep + dr) % NREP
        return rcopy(FL.at[rep], FL.at[rep], f_s.at[dr - 1], f_r.at[rep], (zh, x, c, r // ZL, r % ZL))

    @pl.loop(1, NREP)
    def _(dr):
        fin(dr).start()

    for i, s in enumerate(sends + fwd):
        s.wait_send()

    @pl.loop(0, NZ)
    def _(i):
        @pl.when(w1_not_self(i))
        def _():
            w1(i).wait_send()

    @pl.loop(0, 32)
    def _(i):
        @pl.when(o_not_self(i))
        def _():
            osend(i).wait_send()

        @pl.when(ro_not_self(i))
        def _():
            ro(i).wait_send()

    @pl.loop(0, 8)
    def _(k):
        for dx in range(1, NX):
            w2(k, dx).wait_send()

        @pl.when(jnp.logical_not((k == kown) & selfcore))
        def _():
            r2(k).wait_send()

    for i in range(NY):
        dx_sib(i).wait_send()
    for dy in range(1, NY):
        dx_y(dy).wait_send()
    for dx in range(1, NX):
        r1(dx).wait_send()

    @pl.loop(1, NREP)
    def _(dr):
        r = (rep + dr) % NREP
        rcopy(FL.at[r], FL.at[r], f_s.at[0], f_r.at[r], me).wait_recv()
        fin(dr).wait_send()

    lane36 = lanes(RP)
    for s in range(3):
        last, lastt = None, None
        for t in range(9):
            if t < 8:
                main = roll(FL[t, RP * s : RP * s + RP, :].astype(F32), 16 * t)
            out = main
            if t > 0:
                prev = jnp.where(lane36 < 16 * (t - 1), last, lastt)
                out = prev if t == 8 else jnp.where(lane36 >= 16 * t, main, prev)
            gw_ref[:, s * D + 128 * t : s * D + 128 * t + 128] = out
            if t < 8:
                last = main
                tl = FL[t, 3 * RP : 3 * RP + RP // 2, :].astype(F32)
                halves = [roll(tl, 16 * t - 32 * s - 16 * h) for h in range(2)]
                lastt = jnp.concatenate(halves, axis=0)
    parts = [None] * 3
    for r in range(NREP):
        gw_ref[:, 3 * D + 128 * r : 3 * D + 128 * r + 128] = FL[r, RA : RA + RP, :].astype(F32)
        tl = FL[r, RA + RP : RA + RP + 12, :].astype(F32)
        for t in range(3):
            v = roll(jnp.where(lane12 // 16 == t, tl, 0.0), 16 * (r - t))
            parts[t] = v if parts[t] is None else parts[t] + v
    gw_ref[:, 3 * D + 1024 :] = jnp.concatenate(parts, axis=0)


def vm(*shape, dtype=BF):
    return pltpu.VMEM(shape, dtype)


def local(tokens, out_grad, wq, wk, wv, wo):
    rows = tokens.reshape(-1, D)
    drows = out_grad.reshape(-1, D)
    dma = lambda n: pltpu.SemaphoreType.DMA((n,))
    vmem = pl.BlockSpec(memory_space=pltpu.VMEM)
    hbm = pl.BlockSpec(memory_space=pl.ANY)
    gi, gw = pl.pallas_call(
        kernel,
        out_shape=(
            jax.ShapeDtypeStruct((ROWS, D), BF),
            jax.ShapeDtypeStruct((RP, 4 * D), F32),
        ),
        in_specs=[hbm, hbm, vmem, vmem, vmem, vmem],
        out_specs=(vmem, vmem),
        scratch_shapes=[
            vm(NY, 256, D), vm(NY, 256, D),
            vm(RA, 128), vm(RO, 128), vm(NPIX, RA, 128), vm(32, RO, 128),
            vm(D, 768), vm(256, D), vm(NY, 256, 768), vm(NY, 256, 256),
            vm(NY, 256, D), vm(NY, ROWS, D), vm(NY, ROWS, D), vm(3, ROWS, D),
            vm(D, 768), vm(256, D), vm(NX, 8, RA, 128), vm(NX, 8, RA, 128),
            vm(8, RA, 128), vm(NZ, RA, 128), vm(32, RO, 128), vm(32, RO, 128),
            vm(NREP, RF, 128),
            dma(2), dma(14), dma(16), dma(8), dma(24), dma(32), dma(32), dma(32),
            dma(4), dma(4), dma(3), dma(3), dma(3), dma(4), dma(8), dma(8),
            dma(32), dma(32), dma(7), dma(8),
        ],
        compiler_params=pltpu.CompilerParams(has_side_effects=True, vmem_limit_bytes=60 * 2**20),
    )(rows, drows, wq, wk, wv, wo)
    return gi.reshape(tokens.shape), gw


def solution(mesh):
    torus = Mesh(mesh.devices.reshape(ZH, NX, NC, NY, ZL), AXES)
    act = P(AXES, None, None)
    w = P(("zh", "x", "c"), None)
    return jax.shard_map(
        local,
        mesh=torus,
        in_specs=(act, act, w, w, w, w),
        out_specs=(act, w),
        check_vma=False,
    )
```

```python
import jax
import jax.numpy as jnp
from jax import lax
from jax.experimental import pallas as pl
from jax.experimental.pallas import tpu as pltpu
from jax.sharding import Mesh
from jax.sharding import PartitionSpec as P

D = 1152
FRAMES = 16
HEAD_DIM = 72
ZH, NX, NC, NY, ZL = 4, 4, 2, 4, 2
NZ = ZH * ZL
NPIX = ZH * NX * NC
NREP = NY * ZL
ROWS = 128
RP = D // NPIX
COLS = 2 * HEAD_DIM
RA = 128
RO = 48
RF = RA + RO
BF = jnp.bfloat16
F32 = jnp.float32
AXES = ("zh", "x", "c", "y", "zl")


def dot_nn(a, b):
    return lax.dot_general(a, b, (((1,), (0,)), ((), ())), preferred_element_type=F32)


def dot_nt(a, b):
    return lax.dot_general(a, b, (((1,), (1,)), ((), ())), preferred_element_type=F32)


def dot_tn(a, b):
    return lax.dot_general(a, b, (((0,), (0,)), ((), ())), preferred_element_type=F32)


def roll(v, shift):
    shift = shift % 128
    return v if shift == 0 else pltpu.roll(v, shift, 1)


def lanes(rows):
    return lax.broadcasted_iota(jnp.int32, (rows, 128), 1)


def kernel(
    x_ref, d_ref, wq_ref, wk_ref, wv_ref, wo_ref, gi_ref, gw_ref,
    XA, DA, WIN, WS, OSRC, OH, WL, OL, WCAT, WOC, DQKV, AS, DXP, DXS, DXC, DXH, DXR,
    DWB, DWOB, DWS, RXA, SMB, RL, RR, R2S, RZ, FO, FL,
    lsem, a_s, a_r, h_s, h_r, w1s, w2s, w_r, o1s, o2s, o_r, xs_s, xs_r, xh_s, xh_r, xy_s, xy_r,
    a2_s, a2_r, im_s, im_r, sm_s, sm_r, r2_s, r2_r, t_s, t_r, fa_s, fa_r, fo_s, fo_r,
):
    zh, x, c, y, zl = [lax.axis_index(a) for a in AXES]
    pix = (zh * NX + x) * NC + c
    rep = y * ZL + zl
    z = zh * ZL + zl
    sib = 1 - c
    me = (zh, x, c, y, zl)
    selfcore = zl == c
    right, left, opp = (y + 1) % NY, (y + 3) % NY, (y + 2) % NY
    xr, xl, xo = (x + 1) % NX, (x + 3) % NX, (x + 2) % NX
    hub = (y, (x % 2) * 2 + zl, c, zh, x // 2)
    home = (y, 2 * zl + x // 2, c, zh, x % 2)
    hub_self = (y == zh) & ((x % 2) * 2 + zl == x) & (zl == x // 2)
    hub_other = jnp.logical_not(hub_self)

    def rcopy(src, dst, ss, rs, dev):
        return pltpu.make_async_remote_copy(
            src_ref=src, dst_ref=dst, send_sem=ss, recv_sem=rs,
            device_id=dev, device_id_type=pl.DeviceIdType.MESH,
        )

    def blk(kind, yb, cb):
        return (XA, DA)[kind].at[yb, pl.ds(pl.multiple_of(cb * ROWS, ROWS), ROWS)]

    wins = [
        pltpu.make_async_copy(r, WIN.at[k], lsem.at[2 + k])
        for k, r in enumerate((wq_ref, wk_ref, wv_ref, wo_ref))
    ]
    own = [pltpu.make_async_copy(r, blk(k, y, c), lsem.at[k]) for k, r in enumerate((x_ref, d_ref))]
    for o in own + wins:
        o.start()
    bar = pltpu.get_barrier_semaphore()

    def greet(dev):
        pl.semaphore_signal(bar, inc=1, device_id=dev, device_id_type=pl.DeviceIdType.MESH)

    @pl.loop(0, 16)
    def _(i):
        @pl.when(i != z * 2 + c)
        def _():
            greet((i // 4, x, i % 2, y, (i // 2) % 2))

    for dy in range(1, NY):
        greet((zh, x, c, (y + dy) % NY, zl))
        greet((zh, x, c, (y + dy) % NY, 1 - zl))
    greet((zh, xr, c, y, zl))
    greet((zh, xl, c, y, zl))

    @pl.when(hub_other)
    def _():
        greet(hub)
        greet(home)

    ii = lax.broadcasted_iota(jnp.int32, (D, 256), 0)
    nn = lax.broadcasted_iota(jnp.int32, (D, 256), 1)
    sel = jnp.where((ii == nn + COLS * rep) & (nn < COLS), 1.0, 0.0).astype(BF)
    want = jnp.where(nn < 128, nn + 128 * rep, nn - 128 + 1024 + 16 * rep)
    osel = jnp.where((ii == want) & (nn < COLS), 1.0, 0.0).astype(BF)
    for w in wins:
        w.wait()
    tail = None
    for s in range(3):
        b = dot_nn(WIN[s], sel)
        WS[RP * s : RP * s + RP, :] = b[:, :128].astype(BF)
        t = b[:, 128:256]
        t = roll(t[: RP // 2], 32 * s) + roll(t[RP // 2 :], 32 * s + 16)
        tail = t if tail is None else tail + t
    WS[3 * RP : 3 * RP + RP // 2, :] = tail.astype(BF)
    b = dot_nn(WIN[3], osel)
    OSRC[:RP, :] = b[:, :128].astype(BF)
    t = b[:, 128:256]
    tail = t[:12] + roll(t[12:24], 16) + roll(t[24:36], 32)
    OSRC[RP : RP + 12, :] = tail.astype(BF)
    for o in own:
        o.wait()

    @pl.when(hub_self)
    def _():
        pl.semaphore_wait(bar, 15 + 6 + 2)

    @pl.when(hub_other)
    def _():
        pl.semaphore_wait(bar, 15 + 6 + 2 + 2)

    def act(kind, yb, cb, to_y, to_c, idx):
        return rcopy(
            blk(kind, yb, cb), blk(kind, yb, cb), a_s.at[idx],
            a_r.at[kind * 8 + yb * 2 + cb], (zh, x, to_c, to_y, zl),
        )

    def hub_copy():
        return rcopy(OSRC, OH, h_s.at[0], h_r.at[0], hub)

    sends = [
        act(0, y, c, right, c, 0), act(1, y, c, left, c, 1),
        act(1, y, c, right, c, 2), act(0, y, c, left, c, 3),
        act(0, y, c, y, sib, 4), act(1, y, c, y, sib, 5),
    ]

    @pl.when(hub_other)
    def _():
        hub_copy().start()

    for s in sends[:4]:
        s.start()

    def col(k, xs):
        return ((k // 2) * NX + xs) * NC + k % 2

    def along_z(src, buf, ss, rs, i):
        return rcopy(src, buf.at[pix], ss.at[i], rs.at[pix], (i // 2, x, zl, y, i % 2))

    def not_self(i):
        return jnp.logical_not((i == z) & selfcore)

    def spread(src, buf, ss, rs):
        @pl.when(selfcore)
        def _():
            buf[pix] = src[...]

        @pl.loop(0, NZ)
        def _(i):
            @pl.when(not_self(i))
            def _():
                along_z(src, buf, ss, rs, i).start()

    def around_x(buf, ss, rs, p, to, idx):
        return rcopy(buf.at[p], buf.at[p], ss.at[idx], rs.at[p], (zh, to, c, y, zl))

    def arrived(buf, rs, p):
        rcopy(buf.at[p], buf.at[p], w1s.at[0], rs.at[p], me).wait_recv()

    def both_ways(buf, ss, rs):
        @pl.loop(0, 8)
        def _(k):
            p = col(k, x)

            @pl.when(jnp.logical_not((p == pix) & selfcore))
            def _():
                arrived(buf, rs, p)

            around_x(buf, ss, rs, p, xr, k).start()
            around_x(buf, ss, rs, p, xl, 8 + k).start()

    def onward(buf, ss, rs):
        @pl.loop(0, 4)
        def _(k):
            p, q = col(k, xl), col(k + 4, xr)
            arrived(buf, rs, p)
            around_x(buf, ss, rs, p, xr, 16 + k).start()
            arrived(buf, rs, q)
            around_x(buf, ss, rs, q, xl, 20 + k).start()

    def rest(buf, rs):
        @pl.loop(0, 4)
        def _(k):
            arrived(buf, rs, col(k + 4, xl))
            arrived(buf, rs, col(k, xr))
            arrived(buf, rs, col(k, xo))
            arrived(buf, rs, col(k + 4, xo))

    spread(WS, WL, w1s, w_r)
    for s in sends[4:]:
        s.start()

    @pl.when(hub_other)
    def _():
        hub_copy().wait_recv()

    @pl.when(hub_self)
    def _():
        OH[...] = OSRC[...]

    spread(OH, OL, o1s, o_r)
    both_ways(WL, w2s, w_r)
    both_ways(OL, o2s, o_r)

    def await_act(kind, yb, cb):
        act(kind, yb, cb, y, sib, 0).wait_recv()

    fwd = [
        act(0, left, c, right, c, 6), act(1, right, c, left, c, 7),
        act(0, left, c, y, sib, 8), act(1, right, c, y, sib, 9),
        act(1, left, c, y, sib, 10), act(0, right, c, y, sib, 11),
        act(0, opp, c, y, sib, 12), act(1, opp, c, y, sib, 13),
    ]
    await_act(0, left, c)
    fwd[0].start()
    fwd[2].start()
    await_act(1, right, c)
    fwd[1].start()
    fwd[3].start()
    onward(WL, w2s, w_r)
    onward(OL, o2s, o_r)
    rest(WL, w_r)
    rest(OL, o_r)

    low16 = lanes(RP // 2) < 16

    @pl.loop(0, 8)
    def _(g):
        out = WCAT.at[pl.ds(pl.multiple_of(g * 144, 16), 144)]
        for q in range(4):
            p = g * 4 + q
            base = RP * q
            tl = WL[p, 3 * RP : 3 * RP + RP // 2, :].astype(F32)
            for s in range(3):
                out[base : base + RP, 256 * s : 256 * s + 128] = WL[p, RP * s : RP * s + RP, :]
                for half in range(2):
                    v = jnp.where(low16, roll(tl, -(32 * s + 16 * half)), 0.0).astype(BF)
                    at = base + half * (RP // 2)
                    out[at : at + RP // 2, 256 * s + 128 : 256 * s + 256] = v

    def oslot(q, r):
        return ((r // 2) * NX + (q // 2) * 2 + r % 2) * NC + q % 2

    WOC[COLS:, :] = jnp.zeros((256 - COLS, D), BF)
    lane12 = lanes(12)
    for q in range(4):
        parts = [None] * 3
        for r in range(NREP):
            WOC[RP * q : RP * q + RP, 128 * r : 128 * r + 128] = OL[oslot(q, r), :RP, :]
            tl = OL[oslot(q, r), RP : RP + 12, :].astype(F32)
            for t in range(3):
                v = jnp.where(lane12 // 16 == t, tl, 0.0)
                v = roll(v, 16 * (r - t))
                parts[t] = v if parts[t] is None else parts[t] + v
        for t in range(3):
            at = RP * q + 12 * t
            WOC[at : at + 12, 1024:1152] = parts[t].astype(BF)

    await_act(1, left, c)
    fwd[4].start()
    await_act(0, right, c)
    fwd[5].start()

    scale = 1.0 / HEAD_DIM**0.5
    row = lax.broadcasted_iota(jnp.int32, (ROWS, 128), 0)
    col_ = lax.broadcasted_iota(jnp.int32, (ROWS, 128), 1)
    inside = row // FRAMES == col_ // FRAMES
    lane256 = lax.broadcasted_iota(jnp.int32, (ROWS, 256), 1)
    first = lane256 < HEAD_DIM
    zero = jnp.zeros((ROWS, 256), BF)

    def two_heads(v):
        return jnp.concatenate([jnp.where(first, v, zero), jnp.where(first, zero, v)], axis=0)

    def dx_sib(i):
        return rcopy(
            DXP.at[i, pl.ds(pl.multiple_of(sib * ROWS, ROWS), ROWS)], DXS.at[i],
            xs_s.at[i], xs_r.at[i], (zh, x, sib, y, zl),
        )

    @pl.loop(0, NY)
    def _(n):
        off = jnp.where(n == 1, 3, jnp.where(n == 2, 1, jnp.where(n == 3, 2, 0)))
        i = (y + off) % NY

        @pl.when(n == 3)
        def _():
            await_act(0, opp, c)
            fwd[6].start()
            await_act(1, opp, c)
            fwd[7].start()

        await_act(0, i, sib)
        await_act(1, i, sib)
        qkv = dot_nn(XA[i], WCAT[...]).astype(BF)
        da = dot_nt(DA[i], WOC[...]).astype(BF)
        for h in range(2):
            rs = slice(h * ROWS, h * ROWS + ROWS)
            q, k, v, g = qkv[rs, :256], qkv[rs, 256:512], qkv[rs, 512:], da[rs]
            kk, vv = two_heads(k), two_heads(v)
            sc = dot_nt(q, kk) * scale
            dp = dot_nt(g, vv)
            probs, dscore = [], []
            for n2 in range(2):
                cs = slice(n2 * 128, n2 * 128 + 128)
                s1 = jnp.where(inside, sc[:, cs], -jnp.inf)
                e = jnp.exp(s1 - jnp.max(s1, axis=1, keepdims=True))
                p1 = e / jnp.sum(e, axis=1, keepdims=True)
                d1 = dp[:, cs]
                t1 = jnp.sum(d1 * p1, axis=1, keepdims=True)
                probs.append(p1.astype(BF))
                dscore.append((p1 * (d1 - t1) * scale).astype(BF))
            pb = jnp.concatenate(probs, axis=1)
            ds = jnp.concatenate(dscore, axis=1)
            AS[i, rs, :] = dot_nn(pb, vv).astype(BF)
            DQKV[i, rs, :256] = dot_nn(ds, kk).astype(BF)
            dk = dot_tn(ds, q)
            DQKV[i, rs, 256:512] = jnp.where(first, dk[:128], dk[128:]).astype(BF)
            dv = dot_tn(pb, g)
            DQKV[i, rs, 512:] = jnp.where(first, dv[:128], dv[128:]).astype(BF)
        DXP[i] = dot_nt(DQKV[i], WCAT[...]).astype(BF)
        dx_sib(i).start()

    dq_all = DQKV[...].reshape(NY * 256, 768)

    @pl.loop(0, 9)
    def _(i):
        at = pl.multiple_of(i * 128, 128)
        lhs = XA[:, :, pl.ds(at, 128)].reshape(NY * 256, 128)
        DWB[pl.ds(at, 128), :] = dot_tn(lhs, dq_all).astype(BF)

    DWOB[...] = dot_tn(AS[...].reshape(NY * 256, 256), DA[...].reshape(NY * 256, D)).astype(BF)

    @pl.loop(0, 8)
    def _(g):
        src = DWB.at[pl.ds(pl.multiple_of(g * 144, 16), 144)]
        for q in range(4):
            p = g * 4 + q
            x2, k = (p // 2) % NX, (p // 8) * 2 + p % 2
            base = RP * q
            tail = None
            for s in range(3):
                DWS[x2, k, RP * s : RP * s + RP, :] = src[base : base + RP, 256 * s : 256 * s + 128]
                t = src[base : base + RP, 256 * s + 128 : 256 * s + 256].astype(F32)
                t = roll(t[: RP // 2], 32 * s) + roll(t[RP // 2 :], 32 * s + 16)
                tail = t if tail is None else tail + t
            DWS[x2, k, 3 * RP : 3 * RP + RP // 2, :] = tail.astype(BF)

    for q in range(4):
        tt = [DWOB[RP * q + 12 * t : RP * q + 12 * t + 12, 1024:1152].astype(F32) for t in range(3)]
        for r in range(NREP):
            p = oslot(q, r)
            x2, k = (p // 2) % NX, (p // 8) * 2 + p % 2
            DWS[x2, k, RA : RA + RP, :] = DWOB[RP * q : RP * q + RP, 128 * r : 128 * r + 128]
            tail = None
            for t in range(3):
                v = roll(jnp.where(lane12 // 16 == r, tt[t], 0.0), 16 * (t - r))
                tail = v if tail is None else tail + v
            DWS[x2, k, RA + RP : RF, :] = tail.astype(BF)

    def two(k):
        return pl.ds(k, 2)

    def to_x(src, dst, ss, rs, h, side):
        return rcopy(src, dst, ss.at[h * 2 + side], rs.at[h * 2 + side], (zh, (xr, xl)[side], c, y, zl))

    def far(h, side):
        ks = two((2 * h, 4 + 2 * h)[side])
        return to_x(DWS.at[xo, ks], RXA.at[ks], a2_s, a2_r, h, side)

    def near(h, side):
        ks = two((4 + 2 * h, 2 * h)[side])
        return to_x(DWS.at[(xr, xl)[side], ks], (RL, RR)[side].at[ks], im_s, im_r, h, side)

    def summed(h, side):
        ks = two((2 * h, 4 + 2 * h)[side])
        return to_x(SMB.at[ks], (RL, RR)[side].at[ks], sm_s, sm_r, h, side)

    def add_far(h):
        for side in range(2):
            far(h, side).wait_recv()
            k0 = (2 * h, 4 + 2 * h)[side]
            for k in (k0, k0 + 1):
                t = DWS[(xr, xl)[side], k].astype(F32) + RXA[k].astype(F32)
                SMB[k] = t.astype(BF)
            summed(h, side).start()

    for side in range(2):
        far(0, side).start()
    for side in range(2):
        near(0, side).start()
    for side in range(2):
        far(1, side).start()

    def own_sum(i):
        half = pl.ds(pl.multiple_of(c * ROWS, ROWS), ROWS)
        return DXP[i, half, :].astype(F32) + DXS[i].astype(F32)

    def dx_far(side):
        rows = pl.ds(64 * side, 64)
        return rcopy(
            DXC.at[0, rows], DXH.at[side], xh_s.at[side], xh_r.at[side],
            (zh, x, c, (right, left)[side], zl),
        )

    def dx_near(side):
        return rcopy(
            DXC.at[1 + side], DXR.at[side], xy_s.at[side], xy_r.at[side],
            (zh, x, c, (right, left)[side], zl),
        )

    for i in range(NY):
        dx_sib(i).wait_recv()
    DXC[0] = own_sum(opp).astype(BF)
    for side in range(2):
        dx_far(side).start()

    add_far(0)
    for side in range(2):
        near(1, side).start()
    for side in range(2):
        dx_far(side).wait_recv()
        t = own_sum((right, left)[side])
        a, b = t[:64], t[64:]
        if side == 0:
            a = a + DXH[0].astype(F32)
        else:
            b = b + DXH[1].astype(F32)
        DXC[1 + side, :64, :] = a.astype(BF)
        DXC[1 + side, 64:, :] = b.astype(BF)
        dx_near(side).start()
    add_far(1)

    def r2(k):
        return rcopy(R2S.at[k], RZ.at[z], r2_s.at[k], r2_r.at[z], (k // 2, x, k % 2, y, c))

    kown = zh * 2 + c

    def k_not_self(k):
        return jnp.logical_not((k == kown) & selfcore)

    for h in range(2):
        for side in range(2):
            near(h, side).wait_recv()
            summed(h, side).wait_recv()
        for k in (2 * h, 2 * h + 1, 4 + 2 * h, 5 + 2 * h):
            t = DWS[x, k].astype(F32) + RL[k].astype(F32) + RR[k].astype(F32)
            R2S[k] = t.astype(BF)

            @pl.when(k_not_self(k))
            def _():
                r2(k).start()

    @pl.when(selfcore)
    def _():
        RZ[z] = R2S[kown]

    for side in range(2):
        dx_near(side).wait_recv()
    gi_ref[...] = (own_sum(y) + DXR[0].astype(F32) + DXR[1].astype(F32)).astype(BF)

    @pl.loop(0, NZ)
    def _(i):
        @pl.when(not_self(i))
        def _():
            rcopy(RZ.at[i], RZ.at[i], r2_s.at[0], r2_r.at[i], me).wait_recv()

    asum = RZ[0].astype(F32)
    for i in range(1, NZ):
        asum = asum + RZ[i].astype(F32)
    FO[...] = asum[RA:].astype(BF)
    FL[rep, :RA, :] = asum[:RA].astype(BF)

    head, foot = pl.ds(0, RA), pl.ds(RA, RO)

    def home_copy():
        return rcopy(FO, FL.at[zh * 2 + x % 2, foot], t_s.at[0], t_r.at[0], home)

    def home_arrival():
        return rcopy(FO, FL.at[rep, foot], t_s.at[0], t_r.at[0], me)

    def fin(dr, part, ss, rs):
        r = (rep + dr) % NREP
        b = FL.at[rep, part]
        return rcopy(b, b, ss.at[dr - 1], rs.at[rep], (zh, x, c, r // ZL, r % ZL))

    def fin_wait(dr, part, rs):
        r = (rep + dr) % NREP
        b = FL.at[r, part]
        rcopy(b, b, fa_s.at[0], rs.at[r], me).wait_recv()

    @pl.when(hub_other)
    def _():
        home_copy().start()

    @pl.loop(1, NREP)
    def _(dr):
        fin(dr, head, fa_s, fa_r).start()

    @pl.when(hub_self)
    def _():
        FL[rep, RA:, :] = FO[...]

    @pl.when(hub_other)
    def _():
        home_arrival().wait_recv()

    @pl.loop(1, NREP)
    def _(dr):
        fin(dr, foot, fo_s, fo_r).start()

    for s in sends + fwd:
        s.wait_send()

    @pl.when(hub_other)
    def _():
        hub_copy().wait_send()
        home_copy().wait_send()

    @pl.loop(0, NZ)
    def _(i):
        @pl.when(not_self(i))
        def _():
            along_z(WS, WL, w1s, w_r, i).wait_send()
            along_z(OH, OL, o1s, o_r, i).wait_send()

    @pl.loop(0, 24)
    def _(i):
        around_x(WL, w2s, w_r, pix, xr, i).wait_send()
        around_x(OL, o2s, o_r, pix, xr, i).wait_send()

    @pl.loop(0, 8)
    def _(k):
        @pl.when(k_not_self(k))
        def _():
            r2(k).wait_send()

    for i in range(NY):
        dx_sib(i).wait_send()
    for side in range(2):
        dx_far(side).wait_send()
        dx_near(side).wait_send()
        for h in range(2):
            far(h, side).wait_send()
            near(h, side).wait_send()
            summed(h, side).wait_send()

    @pl.loop(1, NREP)
    def _(dr):
        fin_wait(dr, head, fa_r)
        fin_wait(dr, foot, fo_r)
        fin(dr, head, fa_s, fa_r).wait_send()
        fin(dr, foot, fo_s, fo_r).wait_send()

    lane36 = lanes(RP)
    for s in range(3):
        last, lastt = None, None
        for t in range(9):
            if t < 8:
                main = roll(FL[t, RP * s : RP * s + RP, :].astype(F32), 16 * t)
            out = main
            if t > 0:
                prev = jnp.where(lane36 < 16 * (t - 1), last, lastt)
                out = prev if t == 8 else jnp.where(lane36 >= 16 * t, main, prev)
            gw_ref[:, s * D + 128 * t : s * D + 128 * t + 128] = out.astype(gw_ref.dtype)
            if t < 8:
                last = main
                tl = FL[t, 3 * RP : 3 * RP + RP // 2, :].astype(F32)
                halves = [roll(tl, 16 * t - 32 * s - 16 * h) for h in range(2)]
                lastt = jnp.concatenate(halves, axis=0)
    parts = [None] * 3
    for r in range(NREP):
        at = 3 * D + 128 * r
        gw_ref[:, at : at + 128] = FL[r, RA : RA + RP, :].astype(gw_ref.dtype)
        tl = FL[r, RA + RP : RA + RP + 12, :].astype(F32)
        for t in range(3):
            v = roll(jnp.where(lane12 // 16 == t, tl, 0.0), 16 * (r - t))
            parts[t] = v if parts[t] is None else parts[t] + v
    gw_ref[:, 3 * D + 1024 :] = jnp.concatenate(parts, axis=0).astype(gw_ref.dtype)


def vm(*shape, dtype=BF):
    return pltpu.VMEM(shape, dtype)


def local(tokens, out_grad, wq, wk, wv, wo):
    rows = tokens.reshape(-1, D)
    drows = out_grad.reshape(-1, D)
    dma = lambda n: pltpu.SemaphoreType.DMA((n,))
    vmem = pl.BlockSpec(memory_space=pltpu.VMEM)
    hbm = pl.BlockSpec(memory_space=pl.ANY)
    gi, gw = pl.pallas_call(
        kernel,
        out_shape=(
            jax.ShapeDtypeStruct((ROWS, D), BF),
            jax.ShapeDtypeStruct((RP, 4 * D), BF),
        ),
        in_specs=[hbm] * 6,
        out_specs=(vmem, vmem),
        scratch_shapes=[
            vm(NY, 256, D), vm(NY, 256, D), vm(4, RP, D),
            vm(RA, 128), vm(RO, 128), vm(RO, 128), vm(NPIX, RA, 128), vm(NPIX, RO, 128),
            vm(D, 768), vm(256, D), vm(NY, 256, 768), vm(NY, 256, 256),
            vm(NY, 256, D), vm(NY, ROWS, D), vm(3, ROWS, D), vm(2, 64, D), vm(2, ROWS, D),
            vm(D, 768), vm(256, D), vm(NX, 8, RF, 128), vm(8, RF, 128), vm(8, RF, 128),
            vm(8, RF, 128), vm(8, RF, 128), vm(8, RF, 128), vm(NZ, RF, 128),
            vm(RO, 128), vm(NREP, RF, 128),
            dma(6), dma(14), dma(16), dma(1), dma(1), dma(8), dma(24), dma(32),
            dma(8), dma(24), dma(32), dma(4), dma(4), dma(2), dma(2), dma(2), dma(2),
            dma(4), dma(4), dma(4), dma(4), dma(4), dma(4), dma(8), dma(8),
            dma(1), dma(1), dma(7), dma(8), dma(7), dma(8),
        ],
        compiler_params=pltpu.CompilerParams(
            collective_id=0, has_side_effects=True, vmem_limit_bytes=60 * 2**20
        ),
    )(rows, drows, wq, wk, wv, wo)
    return gi.reshape(tokens.shape), gw.astype(F32)


def solution(mesh):
    torus = Mesh(mesh.devices.reshape(ZH, NX, NC, NY, ZL), AXES)
    act = P(AXES, None, None)
    w = P(("zh", "x", "c"), None)
    return jax.shard_map(
        local,
        mesh=torus,
        in_specs=(act, act, w, w, w, w),
        out_specs=(act, w),
        check_vma=False,
    )
```

```python
import jax
import jax.numpy as jnp
from jax import lax
from jax.experimental import pallas as pl
from jax.experimental.pallas import tpu as pltpu
from jax.sharding import Mesh
from jax.sharding import PartitionSpec as P

D = 1152
FRAMES = 16
HEAD_DIM = 72
ZH, NX, NC, NY, ZL = 4, 4, 2, 4, 2
NZ = ZH * ZL
NPIX = ZH * NX * NC
NREP = NY * ZL
ROWS = 128
RP = D // NPIX
COLS = 2 * HEAD_DIM
RA = 128
RO = 48
RF = RA + RO
BF = jnp.bfloat16
F32 = jnp.float32
AXES = ("zh", "x", "c", "y", "zl")


def dot_nn(a, b):
    return lax.dot_general(a, b, (((1,), (0,)), ((), ())), preferred_element_type=F32)


def dot_nt(a, b):
    return lax.dot_general(a, b, (((1,), (1,)), ((), ())), preferred_element_type=F32)


def dot_tn(a, b):
    return lax.dot_general(a, b, (((0,), (0,)), ((), ())), preferred_element_type=F32)


def roll(v, shift):
    shift = shift % 128
    return v if shift == 0 else pltpu.roll(v, shift, 1)


def lanes(rows):
    return lax.broadcasted_iota(jnp.int32, (rows, 128), 1)


def kernel(
    x_ref, d_ref, wq_ref, wk_ref, wv_ref, wo_ref, gi_ref, gw_ref,
    XA, DA, WIN, WS, OSRC, OH, WL, OL, WCAT, WOC, DQKV, AS, DXP, DXS, DXC, DXH, DXR,
    DWB, DWOB, DWS, RXA, SMB, RL, RR, R2S, RZ, DWO, OXA, OSM, ORL, ORR, O2S, OZ, FO, FL, GI, GW,
    lsem, a_s, a_r, h_s, h_r, w1s, w2s, w_r, o1s, o2s, o_r, xs_s, xs_r, xh_s, xh_r, xy_s, xy_r,
    a2_s, a2_r, im_s, im_r, sm_s, sm_r, r2_s, r2_r, ro_s, ro_r, t_s, t_r, fa_s, fa_r, fo_s, fo_r,
):
    zh, x, c, y, zl = [lax.axis_index(a) for a in AXES]
    pix = (zh * NX + x) * NC + c
    rep = y * ZL + zl
    z = zh * ZL + zl
    sib = 1 - c
    me = (zh, x, c, y, zl)
    selfcore = zl == c
    right, left, opp = (y + 1) % NY, (y + 3) % NY, (y + 2) % NY
    xr, xl, xo = (x + 1) % NX, (x + 3) % NX, (x + 2) % NX
    pair = jnp.where(x % 2 == 0, (x + 3) % NX, xr)
    hub = ((2 * zh + 2 - y + 4) % ZH, jnp.where(zl == x // 2, x, pair), c, zh, x // 2)
    back = jnp.where(x % 2 == 0, (x + 3) % NX, xr)
    there = x // 2 == zl
    home = (y, jnp.where(there, x, back), c, (2 * y + 2 - zh + 4) % NY, jnp.where(there, zl, 1 - zl))

    def rcopy(src, dst, ss, rs, dev):
        return pltpu.make_async_remote_copy(
            src_ref=src, dst_ref=dst, send_sem=ss, recv_sem=rs,
            device_id=dev, device_id_type=pl.DeviceIdType.MESH,
        )

    def blk(kind, yb, cb):
        return (XA, DA)[kind].at[yb, pl.ds(pl.multiple_of(cb * ROWS, ROWS), ROWS)]

    wins = [
        pltpu.make_async_copy(r, WIN.at[k], lsem.at[2 + k])
        for k, r in enumerate((wq_ref, wk_ref, wv_ref, wo_ref))
    ]
    own = [pltpu.make_async_copy(r, blk(k, y, c), lsem.at[k]) for k, r in enumerate((x_ref, d_ref))]
    for o in own + wins:
        o.start()
    bar = pltpu.get_barrier_semaphore()

    def greet(dev):
        pl.semaphore_signal(bar, inc=1, device_id=dev, device_id_type=pl.DeviceIdType.MESH)

    @pl.loop(0, 16)
    def _(i):
        @pl.when(i != z * 2 + c)
        def _():
            greet((i // 4, x, i % 2, y, (i // 2) % 2))

    for dy in range(1, NY):
        greet((zh, x, c, (y + dy) % NY, zl))
        greet((zh, x, c, (y + dy) % NY, 1 - zl))
    greet((zh, xr, c, y, zl))
    greet((zh, xl, c, y, zl))

    greet(hub)
    greet(home)

    ii = lax.broadcasted_iota(jnp.int32, (D, 256), 0)
    nn = lax.broadcasted_iota(jnp.int32, (D, 256), 1)
    sel = jnp.where((ii == nn + COLS * rep) & (nn < COLS), 1.0, 0.0).astype(BF)
    want = jnp.where(nn < 128, nn + 128 * rep, nn - 128 + 1024 + 16 * rep)
    osel = jnp.where((ii == want) & (nn < COLS), 1.0, 0.0).astype(BF)
    for w in wins:
        w.wait()
    tail = None
    for s in range(3):
        b = dot_nn(WIN[s], sel)
        WS[RP * s : RP * s + RP, :] = b[:, :128].astype(BF)
        t = b[:, 128:256]
        t = roll(t[: RP // 2], 32 * s) + roll(t[RP // 2 :], 32 * s + 16)
        tail = t if tail is None else tail + t
    WS[3 * RP : 3 * RP + RP // 2, :] = tail.astype(BF)
    b = dot_nn(WIN[3], osel)
    OSRC[:RP, :] = b[:, :128].astype(BF)
    t = b[:, 128:256]
    tail = t[:12] + roll(t[12:24], 16) + roll(t[24:36], 32)
    OSRC[RP : RP + 12, :] = tail.astype(BF)
    for o in own:
        o.wait()

    pl.semaphore_wait(bar, 15 + 6 + 2 + 2)

    def act(kind, yb, cb, to_y, to_c, idx):
        return rcopy(
            blk(kind, yb, cb), blk(kind, yb, cb), a_s.at[idx],
            a_r.at[kind * 8 + yb * 2 + cb], (zh, x, to_c, to_y, zl),
        )

    def hub_copy():
        return rcopy(OSRC, OH, h_s.at[0], h_r.at[0], hub)

    sends = [
        act(0, y, c, right, c, 0), act(1, y, c, left, c, 1),
        act(1, y, c, right, c, 2), act(0, y, c, left, c, 3),
        act(0, y, c, y, sib, 4), act(1, y, c, y, sib, 5),
    ]

    hub_copy().start()
    for s in sends[:4]:
        s.start()

    def col(k, xs):
        return ((k // 2) * NX + xs) * NC + k % 2

    def along_z(src, buf, ss, rs, i):
        return rcopy(src, buf.at[pix], ss.at[i], rs.at[pix], (i // 2, x, zl, y, i % 2))

    def not_self(i):
        return jnp.logical_not((i == z) & selfcore)

    def spread(src, buf, ss, rs):
        @pl.when(selfcore)
        def _():
            buf[pix] = src[...]

        for dz in (1, 7, 2, 6, 3, 5, 4):
            along_z(src, buf, ss, rs, (z + dz) % NZ).start()

        @pl.when(jnp.logical_not(selfcore))
        def _():
            along_z(src, buf, ss, rs, z).start()

    def around_x(buf, ss, rs, p, to, idx):
        return rcopy(buf.at[p], buf.at[p], ss.at[idx], rs.at[p], (zh, to, c, y, zl))

    def arrived(buf, rs, p):
        rcopy(buf.at[p], buf.at[p], w1s.at[0], rs.at[p], me).wait_recv()

    def both_ways(buf, ss, rs):
        @pl.loop(0, 8)
        def _(n):
            n = jnp.where(n < 4, n, jnp.where(n < 6, n + 2, n - 2))
            k = (2 * zh + n) % 8
            p = col(k, x)

            @pl.when(jnp.logical_not((p == pix) & selfcore))
            def _():
                arrived(buf, rs, p)

            around_x(buf, ss, rs, p, xr, k).start()
            around_x(buf, ss, rs, p, xl, 8 + k).start()

    def onward(buf, ss, rs):
        @pl.loop(0, 4)
        def _(k):
            p, q = col(k, xl), col(k + 4, xr)
            arrived(buf, rs, p)
            around_x(buf, ss, rs, p, xr, 16 + k).start()
            arrived(buf, rs, q)
            around_x(buf, ss, rs, q, xl, 20 + k).start()

    def rest(buf, rs):
        @pl.loop(0, 4)
        def _(k):
            arrived(buf, rs, col(k + 4, xl))
            arrived(buf, rs, col(k, xr))
            arrived(buf, rs, col(k, xo))
            arrived(buf, rs, col(k + 4, xo))

    spread(WS, WL, w1s, w_r)
    for s in sends[4:]:
        s.start()

    both_ways(WL, w2s, w_r)
    hub_copy().wait_recv()
    spread(OH, OL, o1s, o_r)

    def await_act(kind, yb, cb):
        act(kind, yb, cb, y, sib, 0).wait_recv()

    fwd = [
        act(0, left, c, right, c, 6), act(1, right, c, left, c, 7),
        act(0, left, c, y, sib, 8), act(1, right, c, y, sib, 9),
        act(1, left, c, y, sib, 10), act(0, right, c, y, sib, 11),
        act(0, opp, c, y, sib, 12), act(1, opp, c, y, sib, 13),
    ]
    await_act(0, left, c)
    fwd[0].start()
    fwd[2].start()
    await_act(1, right, c)
    fwd[1].start()
    fwd[3].start()
    onward(WL, w2s, w_r)
    both_ways(OL, o2s, o_r)
    onward(OL, o2s, o_r)
    rest(WL, w_r)
    rest(OL, o_r)

    low16 = lanes(RP // 2) < 16

    @pl.loop(0, 8)
    def _(g):
        out = WCAT.at[pl.ds(pl.multiple_of(g * 144, 16), 144)]
        for q in range(4):
            p = g * 4 + q
            base = RP * q
            tl = WL[p, 3 * RP : 3 * RP + RP // 2, :].astype(F32)
            for s in range(3):
                out[base : base + RP, 256 * s : 256 * s + 128] = WL[p, RP * s : RP * s + RP, :]
                for half in range(2):
                    v = jnp.where(low16, roll(tl, -(32 * s + 16 * half)), 0.0).astype(BF)
                    at = base + half * (RP // 2)
                    out[at : at + RP // 2, 256 * s + 128 : 256 * s + 256] = v

    def oslot(q, r):
        xs = 2 * c + q // 2
        other = (xs + 3) % NX if q // 2 == 0 else (xs + 1) % NX
        xh = jnp.where(c == r % 2, xs, other)
        return (2 * y + 2 - r // 2 + 4) % ZH, xh, q % 2

    def opix(q, r):
        zs, xh, cs = oslot(q, r)
        return (zs * NX + xh) * NC + cs

    WOC[COLS:, :] = jnp.zeros((256 - COLS, D), BF)
    lane12 = lanes(12)
    for q in range(4):
        parts = [None] * 3
        for r in range(NREP):
            WOC[RP * q : RP * q + RP, 128 * r : 128 * r + 128] = OL[opix(q, r), :RP, :]
            tl = OL[opix(q, r), RP : RP + 12, :].astype(F32)
            for t in range(3):
                v = jnp.where(lane12 // 16 == t, tl, 0.0)
                v = roll(v, 16 * (r - t))
                parts[t] = v if parts[t] is None else parts[t] + v
        for t in range(3):
            at = RP * q + 12 * t
            WOC[at : at + 12, 1024:1152] = parts[t].astype(BF)

    await_act(1, left, c)
    fwd[4].start()
    await_act(0, right, c)
    fwd[5].start()

    scale = 1.0 / HEAD_DIM**0.5
    row = lax.broadcasted_iota(jnp.int32, (ROWS, 128), 0)
    col_ = lax.broadcasted_iota(jnp.int32, (ROWS, 128), 1)
    inside = row // FRAMES == col_ // FRAMES
    lane256 = lax.broadcasted_iota(jnp.int32, (ROWS, 256), 1)
    first = lane256 < HEAD_DIM
    zero = jnp.zeros((ROWS, 256), BF)

    def two_heads(v):
        return jnp.concatenate([jnp.where(first, v, zero), jnp.where(first, zero, v)], axis=0)

    def dx_sib(i):
        return rcopy(
            DXP.at[i, pl.ds(pl.multiple_of(sib * ROWS, ROWS), ROWS)], DXS.at[i],
            xs_s.at[i], xs_r.at[i], (zh, x, sib, y, zl),
        )

    @pl.loop(0, NY)
    def _(n):
        off = jnp.where(n == 1, 3, jnp.where(n == 2, 1, jnp.where(n == 3, 2, 0)))
        i = (y + off) % NY

        @pl.when(n == 2)
        def _():
            await_act(0, opp, c)
            fwd[6].start()
            await_act(1, opp, c)
            fwd[7].start()

        await_act(0, i, sib)
        await_act(1, i, sib)
        qkv = dot_nn(XA[i], WCAT[...]).astype(BF)
        da = dot_nt(DA[i], WOC[...]).astype(BF)
        for h in range(2):
            rs = slice(h * ROWS, h * ROWS + ROWS)
            q, k, v, g = qkv[rs, :256], qkv[rs, 256:512], qkv[rs, 512:], da[rs]
            kk, vv = two_heads(k), two_heads(v)
            sc = dot_nt(q, kk) * scale
            dp = dot_nt(g, vv)
            probs, dscore = [], []
            for n2 in range(2):
                cs = slice(n2 * 128, n2 * 128 + 128)
                s1 = jnp.where(inside, sc[:, cs], -jnp.inf)
                e = jnp.exp(s1 - jnp.max(s1, axis=1, keepdims=True))
                p1 = e / jnp.sum(e, axis=1, keepdims=True)
                d1 = dp[:, cs]
                t1 = jnp.sum(d1 * p1, axis=1, keepdims=True)
                probs.append(p1.astype(BF))
                dscore.append((p1 * (d1 - t1) * scale).astype(BF))
            pb = jnp.concatenate(probs, axis=1)
            ds = jnp.concatenate(dscore, axis=1)
            AS[i, rs, :] = dot_nn(pb, vv).astype(BF)
            DQKV[i, rs, :256] = dot_nn(ds, kk).astype(BF)
            dk = dot_tn(ds, q)
            DQKV[i, rs, 256:512] = jnp.where(first, dk[:128], dk[128:]).astype(BF)
            dv = dot_tn(pb, g)
            DQKV[i, rs, 512:] = jnp.where(first, dv[:128], dv[128:]).astype(BF)
        DXP[i] = dot_nt(DQKV[i], WCAT[...]).astype(BF)
        dx_sib(i).start()

    OGRP, first_k = 2, (lambda h, side: 4 * side if h == 2 else 2 * h + 4 * side)
    bufs = lambda h: (DWO, OXA, OSM, ORL, ORR, O2S) if h == OGRP else (DWS, RXA, SMB, RL, RR, R2S)

    def some(h, side):
        return pl.ds(first_k(h, side), 4 if h == OGRP else 2)

    def to_x(src, dst, ss, rs, h, side):
        return rcopy(src, dst, ss.at[h * 2 + side], rs.at[h * 2 + side], (zh, (xr, xl)[side], c, y, zl))

    def far(h, side):
        ks = some(h, side)
        return to_x(bufs(h)[0].at[xo, ks], bufs(h)[1].at[ks], a2_s, a2_r, h, side)

    def near(h, side):
        ks = some(h, 1 - side)
        return to_x(bufs(h)[0].at[(xr, xl)[side], ks], bufs(h)[3 + side].at[ks], im_s, im_r, h, side)

    def summed(h, side):
        ks = some(h, side)
        return to_x(bufs(h)[2].at[ks], bufs(h)[3 + side].at[ks], sm_s, sm_r, h, side)

    def start_both(f, h):
        for side in range(2):
            f(h, side).start()

    def add_far(h):
        own_, got, out = bufs(h)[:3]
        for side in range(2):
            far(h, side).wait_recv()
            for k in range(first_k(h, side), first_k(h, side) + (4 if h == OGRP else 2)):
                out[k] = (own_[(xr, xl)[side], k].astype(F32) + got[k].astype(F32)).astype(BF)
            summed(h, side).start()

    kown = zh * 2 + c

    def r2(h, k):
        src, dst, ss, rs = (O2S, OZ, ro_s, ro_r) if h == OGRP else (R2S, RZ, r2_s, r2_r)
        return rcopy(src.at[k], dst.at[z], ss.at[k], rs.at[z], (k // 2, x, k % 2, y, c))

    def k_not_self(k):
        return jnp.logical_not((k == kown) & selfcore)

    def send_z(h):
        for side in range(2):
            near(h, side).wait_recv()
            summed(h, side).wait_recv()
        own_, _, _, fl, fr, out = bufs(h)
        for side in range(2):
            for k in range(first_k(h, side), first_k(h, side) + (4 if h == OGRP else 2)):
                t = own_[x, k].astype(F32) + fl[k].astype(F32) + fr[k].astype(F32)
                out[k] = t.astype(BF)

                @pl.when(k_not_self(k))
                def _():
                    r2(h, k).start()

    def z_sum(h, buf, src):
        @pl.when(selfcore)
        def _():
            buf[z] = src[kown]

        @pl.loop(0, NZ)
        def _(i):
            @pl.when(not_self(i))
            def _():
                rs = ro_r if h == OGRP else r2_r
                rcopy(buf.at[i], buf.at[i], r2_s.at[0], rs.at[i], me).wait_recv()

        t = buf[0].astype(F32)
        for i in range(1, NZ):
            t = t + buf[i].astype(F32)
        return t.astype(BF)

    DWOB[...] = dot_tn(AS[...].reshape(NY * 256, 256), DA[...].reshape(NY * 256, D)).astype(BF)
    for q in range(4):
        tt = [DWOB[RP * q + 12 * t : RP * q + 12 * t + 12, 1024:1152].astype(F32) for t in range(3)]
        for r in range(NREP):
            zs, x2, cs = oslot(q, r)
            k = zs * 2 + cs
            DWO[x2, k, :RP, :] = DWOB[RP * q : RP * q + RP, 128 * r : 128 * r + 128]
            tail = None
            for t in range(3):
                v = roll(jnp.where(lane12 // 16 == r, tt[t], 0.0), 16 * (t - r))
                tail = v if tail is None else tail + v
            DWO[x2, k, RP:RO, :] = tail.astype(BF)
    start_both(far, OGRP)
    start_both(near, OGRP)

    dq_all = DQKV[...].reshape(NY * 256, 768)

    def dw_tile(i):
        lhs = XA[:, :, 128 * i : 128 * i + 128].reshape(NY * 256, 128)
        DWB[128 * i : 128 * i + 128, :] = dot_tn(lhs, dq_all).astype(BF)

    def pack(g):
        for q in range(4):
            p = g * 4 + q
            x2, k = (p // 2) % NX, (p // 8) * 2 + p % 2
            base = RP * p
            tail = None
            for s in range(3):
                DWS[x2, k, RP * s : RP * s + RP, :] = DWB[base : base + RP, 256 * s : 256 * s + 128]
                t = DWB[base : base + RP, 256 * s + 128 : 256 * s + 256].astype(F32)
                t = roll(t[: RP // 2], 32 * s) + roll(t[RP // 2 :], 32 * s + 16)
                tail = t if tail is None else tail + t
            DWS[x2, k, 3 * RP : 3 * RP + RP // 2, :] = tail.astype(BF)

    def own_sum(i):
        half = pl.ds(pl.multiple_of(c * ROWS, ROWS), ROWS)
        return DXP[i, half, :].astype(F32) + DXS[i].astype(F32)

    def dx_far(side):
        rows = pl.ds(64 * side, 64)
        return rcopy(
            DXC.at[0, rows], DXH.at[side], xh_s.at[side], xh_r.at[side],
            (zh, x, c, (right, left)[side], zl),
        )

    def dx_near(side):
        return rcopy(
            DXC.at[1 + side], DXR.at[side], xy_s.at[side], xy_r.at[side],
            (zh, x, c, (right, left)[side], zl),
        )

    for i in (0, 1, 2, 4, 5, 6):
        dw_tile(i)
    for g in (0, 1, 4, 5):
        pack(g)
    start_both(far, 0)
    start_both(near, 0)
    add_far(OGRP)
    for i in range(NY):
        dx_sib(i).wait_recv()
    DXC[0] = own_sum(opp).astype(BF)
    for side in range(2):
        dx_far(side).start()
    for i in (3, 7, 8):
        dw_tile(i)
    for g in (2, 3, 6, 7):
        pack(g)
    start_both(far, 1)
    add_far(0)
    start_both(near, 1)
    send_z(OGRP)
    for side in range(2):
        dx_far(side).wait_recv()
        t = own_sum((right, left)[side])
        a, b = t[:64], t[64:]
        if side == 0:
            a = a + DXH[0].astype(F32)
        else:
            b = b + DXH[1].astype(F32)
        DXC[1 + side, :64, :] = a.astype(BF)
        DXC[1 + side, 64:, :] = b.astype(BF)
        dx_near(side).start()
    add_far(1)
    send_z(0)

    head, foot = pl.ds(0, RA), pl.ds(RA, RO)

    def home_copy():
        r = home[3] * ZL + home[4]
        return rcopy(FO, FL.at[r, foot], t_s.at[0], t_r.at[0], home)

    def home_arrival():
        return rcopy(FO, FL.at[rep, foot], t_s.at[0], t_r.at[0], me)

    def fin(dr, part, ss, rs):
        r = (rep + dr) % NREP
        b = FL.at[rep, part]
        return rcopy(b, b, ss.at[dr - 1], rs.at[rep], (zh, x, c, r // ZL, r % ZL))

    def fin_wait(dr, part, rs):
        r = (rep + dr) % NREP
        b = FL.at[r, part]
        rcopy(b, b, fa_s.at[0], rs.at[r], me).wait_recv()

    FO[...] = z_sum(OGRP, OZ, O2S)
    home_copy().start()
    send_z(1)
    for side in range(2):
        dx_near(side).wait_recv()
    GI[...] = (own_sum(y) + DXR[0].astype(F32) + DXR[1].astype(F32)).astype(BF)
    gi_out = pltpu.make_async_copy(GI, gi_ref, lsem.at[6])
    gi_out.start()
    home_arrival().wait_recv()

    @pl.loop(1, NREP)
    def _(dr):
        fin(dr, foot, fo_s, fo_r).start()

    FL[rep, :RA, :] = z_sum(0, RZ, R2S)

    @pl.loop(1, NREP)
    def _(dr):
        fin(dr, head, fa_s, fa_r).start()

    for s in sends + fwd:
        s.wait_send()

    hub_copy().wait_send()
    home_copy().wait_send()

    @pl.loop(0, NZ)
    def _(i):
        @pl.when(not_self(i))
        def _():
            along_z(WS, WL, w1s, w_r, i).wait_send()
            along_z(OH, OL, o1s, o_r, i).wait_send()

    @pl.loop(0, 24)
    def _(i):
        around_x(WL, w2s, w_r, pix, xr, i).wait_send()
        around_x(OL, o2s, o_r, pix, xr, i).wait_send()

    @pl.loop(0, 8)
    def _(k):
        @pl.when(k_not_self(k))
        def _():
            r2(0, k).wait_send()
            r2(OGRP, k).wait_send()

    for i in range(NY):
        dx_sib(i).wait_send()
    for side in range(2):
        dx_far(side).wait_send()
        dx_near(side).wait_send()
        for h in range(3):
            far(h, side).wait_send()
            near(h, side).wait_send()
            summed(h, side).wait_send()

    @pl.loop(1, NREP)
    def _(dr):
        fin_wait(dr, head, fa_r)
        fin_wait(dr, foot, fo_r)
        fin(dr, head, fa_s, fa_r).wait_send()
        fin(dr, foot, fo_s, fo_r).wait_send()

    lane36 = lanes(RP)
    for s in range(3):
        last, lastt = None, None
        for t in range(9):
            if t < 8:
                main = roll(FL[t, RP * s : RP * s + RP, :].astype(F32), 16 * t)
            out = main
            if t > 0:
                prev = jnp.where(lane36 < 16 * (t - 1), last, lastt)
                out = prev if t == 8 else jnp.where(lane36 >= 16 * t, main, prev)
            GW[:, s * D + 128 * t : s * D + 128 * t + 128] = out.astype(GW.dtype)
            if t < 8:
                last = main
                tl = FL[t, 3 * RP : 3 * RP + RP // 2, :].astype(F32)
                halves = [roll(tl, 16 * t - 32 * s - 16 * h) for h in range(2)]
                lastt = jnp.concatenate(halves, axis=0)
    parts = [None] * 3
    for r in range(NREP):
        at = 3 * D + 128 * r
        GW[:, at : at + 128] = FL[r, RA : RA + RP, :].astype(GW.dtype)
        tl = FL[r, RA + RP : RA + RP + 12, :].astype(F32)
        for t in range(3):
            v = roll(jnp.where(lane12 // 16 == t, tl, 0.0), 16 * (r - t))
            parts[t] = v if parts[t] is None else parts[t] + v
    GW[:, 3 * D + 1024 :] = jnp.concatenate(parts, axis=0).astype(GW.dtype)
    gw_out = pltpu.make_async_copy(GW, gw_ref, lsem.at[7])
    gw_out.start()
    gi_out.wait()
    gw_out.wait()


def vm(*shape, dtype=BF):
    return pltpu.VMEM(shape, dtype)


def local(tokens, out_grad, wq, wk, wv, wo):
    rows = tokens.reshape(-1, D)
    drows = out_grad.reshape(-1, D)
    dma = lambda n: pltpu.SemaphoreType.DMA((n,))
    hbm = pl.BlockSpec(memory_space=pl.ANY)
    gi, gw = pl.pallas_call(
        kernel,
        out_shape=(
            jax.ShapeDtypeStruct((ROWS, D), BF),
            jax.ShapeDtypeStruct((RP, 4 * D), BF),
        ),
        in_specs=[hbm] * 6,
        out_specs=(hbm, hbm),
        scratch_shapes=[
            vm(NY, 256, D), vm(NY, 256, D), vm(4, RP, D),
            vm(RA, 128), vm(RO, 128), vm(RO, 128), vm(NPIX, RA, 128), vm(NPIX, RO, 128),
            vm(D, 768), vm(256, D), vm(NY, 256, 768), vm(NY, 256, 256),
            vm(NY, 256, D), vm(NY, ROWS, D), vm(3, ROWS, D), vm(2, 64, D), vm(2, ROWS, D),
            vm(D, 768), vm(256, D), vm(NX, 8, RA, 128), *[vm(8, RA, 128)] * 5, vm(NZ, RA, 128),
            vm(NX, 8, RO, 128), *[vm(8, RO, 128)] * 5, vm(NZ, RO, 128),
            vm(RO, 128), vm(NREP, RF, 128), vm(ROWS, D), vm(RP, 4 * D),
            dma(8), dma(14), dma(16), dma(1), dma(1), dma(8), dma(24), dma(32),
            dma(8), dma(24), dma(32), dma(4), dma(4), dma(2), dma(2), dma(2), dma(2),
            dma(6), dma(6), dma(6), dma(6), dma(6), dma(6), dma(8), dma(8), dma(8), dma(8),
            dma(1), dma(1), dma(7), dma(8), dma(7), dma(8),
        ],
        compiler_params=pltpu.CompilerParams(
            collective_id=0, has_side_effects=True, vmem_limit_bytes=60 * 2**20
        ),
    )(rows, drows, wq, wk, wv, wo)
    return gi.reshape(tokens.shape), gw.astype(F32)


def solution(mesh):
    torus = Mesh(mesh.devices.reshape(ZH, NX, NC, NY, ZL), AXES)
    act = P(AXES, None, None)
    w = P(("zh", "x", "c"), None)
    return jax.shard_map(
        local,
        mesh=torus,
        in_specs=(act, act, w, w, w, w),
        out_specs=(act, w),
        check_vma=False,
    )
```

```python
import jax
import jax.numpy as jnp
from jax import lax
from jax.experimental import pallas as pl
from jax.experimental.pallas import tpu as pltpu
from jax.sharding import Mesh
from jax.sharding import PartitionSpec as P

D = 1152
FRAMES = 16
HEAD_DIM = 72
ZH, NX, NC, NY, ZL = 4, 4, 2, 4, 2
NZ = ZH * ZL
NPIX = ZH * NX * NC
NREP = NY * ZL
ROWS = 128
RP = D // NPIX
COLS = 2 * HEAD_DIM
RA = 128
RO = 48
RF = RA + RO
BF = jnp.bfloat16
F32 = jnp.float32
AXES = ("zh", "x", "c", "y", "zl")


def dot_nn(a, b):
    return lax.dot_general(a, b, (((1,), (0,)), ((), ())), preferred_element_type=F32)


def dot_nt(a, b):
    return lax.dot_general(a, b, (((1,), (1,)), ((), ())), preferred_element_type=F32)


def dot_tn(a, b):
    return lax.dot_general(a, b, (((0,), (0,)), ((), ())), preferred_element_type=F32)


def roll(v, shift):
    shift = shift % 128
    return v if shift == 0 else pltpu.roll(v, shift, 1)


def lanes(rows):
    return lax.broadcasted_iota(jnp.int32, (rows, 128), 1)


def kernel(
    x_ref, d_ref, wq_ref, wk_ref, wv_ref, wo_ref, gi_ref, gw_ref,
    XA, DA, WIN, WS, OSRC, OH, WL, OL, WCAT, WOC, DQKV, AS, DXP, DXS, DXC, DXH, DXR,
    DWB, DWOB, DWS, RXA, SMB, RL, RR, R2S, RZ, DWO, OXA, OSM, ORL, ORR, O2S, OZ, FO, FL, GI, GW,
    lsem, sent, a_r, s_r, h_r, w_r, o_r, dx_r, xh_r, far_r, near_r, z_r, t_r, f_r,
):
    zh, x, c, y, zl = [lax.axis_index(a) for a in AXES]
    pix = (zh * NX + x) * NC + c
    rep = y * ZL + zl
    z = zh * ZL + zl
    sib = 1 - c
    me = (zh, x, c, y, zl)
    selfcore = zl == c
    right, left, opp = (y + 1) % NY, (y + 3) % NY, (y + 2) % NY
    xr, xl, xo = (x + 1) % NX, (x + 3) % NX, (x + 2) % NX
    pair = jnp.where(x % 2 == 0, (x + 3) % NX, xr)
    hub = ((2 * zh + 2 - y + 4) % ZH, jnp.where(zl == x // 2, x, pair), c, zh, x // 2)
    back = jnp.where(x % 2 == 0, (x + 3) % NX, xr)
    there = x // 2 == zl
    home = (y, jnp.where(there, x, back), c, (2 * y + 2 - zh + 4) % NY, jnp.where(there, zl, 1 - zl))

    def rcopy(src, dst, ss, rs, dev):
        return pltpu.make_async_remote_copy(
            src_ref=src, dst_ref=dst, send_sem=ss, recv_sem=rs,
            device_id=dev, device_id_type=pl.DeviceIdType.MESH,
        )

    def blk(kind, yb, cb):
        return (XA, DA)[kind].at[yb, pl.ds(pl.multiple_of(cb * ROWS, ROWS), ROWS)]

    wins = [
        pltpu.make_async_copy(r, WIN.at[k], lsem.at[2 + k])
        for k, r in enumerate((wq_ref, wk_ref, wv_ref, wo_ref))
    ]
    own = [pltpu.make_async_copy(r, blk(k, y, c), lsem.at[k]) for k, r in enumerate((x_ref, d_ref))]
    for o in own + wins:
        o.start()
    bar = pltpu.get_barrier_semaphore()

    def greet(dev):
        pl.semaphore_signal(bar, inc=1, device_id=dev, device_id_type=pl.DeviceIdType.MESH)

    @pl.loop(0, 16)
    def _(i):
        @pl.when(i != z * 2 + c)
        def _():
            greet((i // 4, x, i % 2, y, (i // 2) % 2))

    for dy in range(1, NY):
        greet((zh, x, c, (y + dy) % NY, zl))
        greet((zh, x, c, (y + dy) % NY, 1 - zl))
    greet((zh, xr, c, y, zl))
    greet((zh, xl, c, y, zl))

    greet(hub)
    greet(home)

    ii = lax.broadcasted_iota(jnp.int32, (D, 256), 0)
    nn = lax.broadcasted_iota(jnp.int32, (D, 256), 1)
    sel = jnp.where((ii == nn + COLS * rep) & (nn < COLS), 1.0, 0.0).astype(BF)
    want = jnp.where(nn < 128, nn + 128 * rep, nn - 128 + 1024 + 16 * rep)
    osel = jnp.where((ii == want) & (nn < COLS), 1.0, 0.0).astype(BF)
    for w in wins:
        w.wait()
    tail = None
    for s in range(3):
        b = dot_nn(WIN[s], sel)
        WS[RP * s : RP * s + RP, :] = b[:, :128].astype(BF)
        t = b[:, 128:256]
        t = roll(t[: RP // 2], 32 * s) + roll(t[RP // 2 :], 32 * s + 16)
        tail = t if tail is None else tail + t
    WS[3 * RP : 3 * RP + RP // 2, :] = tail.astype(BF)
    b = dot_nn(WIN[3], osel)
    OSRC[:RP, :] = b[:, :128].astype(BF)
    t = b[:, 128:256]
    tail = t[:12] + roll(t[12:24], 16) + roll(t[24:36], 32)
    OSRC[RP : RP + 12, :] = tail.astype(BF)
    for o in own:
        o.wait()

    pl.semaphore_wait(bar, 15 + 6 + 2 + 2)

    def act(kind, yb, cb, to_y, to_c, idx):
        rs = s_r.at[yb] if to_c is sib else a_r.at[kind * 4 + yb]
        return rcopy(blk(kind, yb, cb), blk(kind, yb, cb), sent.at[idx // 6], rs, (zh, x, to_c, to_y, zl))

    def hub_copy():
        return rcopy(OSRC, OH, sent.at[3], h_r.at[0], hub)

    sends = [
        act(0, y, c, right, c, 0), act(1, y, c, left, c, 1),
        act(1, y, c, right, c, 2), act(0, y, c, left, c, 3),
        act(0, y, c, y, sib, 4), act(1, y, c, y, sib, 5),
    ]

    hub_copy().start()
    for s in sends[:4]:
        s.start()

    def col(k, xs):
        return ((k // 2) * NX + xs) * NC + k % 2

    def along_z(src, buf, ss, rs, i):
        return rcopy(src, buf.at[pix], sent.at[ss], rs.at[zh * 2 + c], (i // 2, x, zl, y, i % 2))

    def not_self(i):
        return jnp.logical_not((i == z) & selfcore)

    def spread(src, buf, ss, rs):
        @pl.when(selfcore)
        def _():
            buf[pix] = src[...]

        for dz in (1, 7, 2, 6, 3, 5, 4):
            along_z(src, buf, ss, rs, (z + dz) % NZ).start()

        @pl.when(jnp.logical_not(selfcore))
        def _():
            along_z(src, buf, ss, rs, z).start()

    def around_x(buf, ss, rs, p, to, idx):
        return rcopy(buf.at[p], buf.at[p], sent.at[ss + 1], rs.at[idx], (zh, to, c, y, zl))

    def arrived(ref, rs, idx):
        rcopy(ref, ref, sent.at[0], rs.at[idx], me).wait_recv()

    def both_ways(buf, ss, rs, lo, hi):
        @pl.loop(lo, hi)
        def _(n):
            n = jnp.where(n < 4, n, jnp.where(n < 6, n + 2, n - 2))
            k = (2 * zh + n) % 8
            p = col(k, x)

            @pl.when(jnp.logical_not((p == pix) & selfcore))
            def _():
                arrived(buf.at[p], rs, k)

            around_x(buf, ss, rs, p, xr, jnp.where(k % 2 == 0, 8 + k, 16)).start()
            around_x(buf, ss, rs, p, xl, jnp.where(k % 2 == 0, 16, 8 + k)).start()

    def onward(buf, ss, rs, lo, hi):
        @pl.loop(lo, hi)
        def _(n):
            k = 2 * ((zh + jnp.where(n < 2, n, 5 - n)) % ZH)
            p, q = col(k, xl), col(k + 1, xr)
            arrived(buf.at[p], rs, 8 + k)
            around_x(buf, ss, rs, p, xr, 16).start()
            arrived(buf.at[q], rs, 9 + k)
            around_x(buf, ss, rs, q, xl, 16).start()

    def rest(buf, rs):
        arrived(buf.at[pl.ds(0, 16)], rs, 16)

    spread(WS, WL, 4, w_r)
    for s in sends[4:]:
        s.start()
    both_ways(WL, 4, w_r, 0, 2)
    hub_copy().wait_recv()
    spread(OH, OL, 6, o_r)
    both_ways(WL, 4, w_r, 2, 4)
    onward(WL, 4, w_r, 0, 2)
    both_ways(WL, 4, w_r, 4, 8)

    def await_act(kind, yb):
        rcopy(blk(kind, yb, c), blk(kind, yb, c), sent.at[0], a_r.at[kind * 4 + yb], me).wait_recv()

    def await_sib(yb):
        rcopy(XA.at[yb], XA.at[yb], sent.at[0], s_r.at[yb], me).wait_recv()

    fwd = [
        act(0, left, c, right, c, 6), act(1, right, c, left, c, 7),
        act(0, left, c, y, sib, 8), act(1, right, c, y, sib, 9),
        act(1, left, c, y, sib, 10), act(0, right, c, y, sib, 11),
        act(0, opp, c, y, sib, 12), act(1, opp, c, y, sib, 13),
    ]
    await_act(0, left)
    fwd[0].start()
    fwd[2].start()
    await_act(1, right)
    fwd[1].start()
    fwd[3].start()
    both_ways(OL, 6, o_r, 0, 8)
    onward(WL, 4, w_r, 2, 4)
    onward(OL, 6, o_r, 0, 4)
    rest(WL, w_r)

    low16 = lanes(RP // 2) < 16

    @pl.loop(0, 8)
    def _(g):
        out = WCAT.at[pl.ds(pl.multiple_of(g * 144, 16), 144)]
        for q in range(4):
            p = g * 4 + q
            base = RP * q
            tl = WL[p, 3 * RP : 3 * RP + RP // 2, :].astype(F32)
            for s in range(3):
                out[base : base + RP, 256 * s : 256 * s + 128] = WL[p, RP * s : RP * s + RP, :]
                for half in range(2):
                    v = jnp.where(low16, roll(tl, -(32 * s + 16 * half)), 0.0).astype(BF)
                    at = base + half * (RP // 2)
                    out[at : at + RP // 2, 256 * s + 128 : 256 * s + 256] = v

    scale = 1.0 / HEAD_DIM**0.5
    row = lax.broadcasted_iota(jnp.int32, (ROWS, 128), 0)
    col_ = lax.broadcasted_iota(jnp.int32, (ROWS, 128), 1)
    inside = row // FRAMES == col_ // FRAMES
    lane256 = lax.broadcasted_iota(jnp.int32, (ROWS, 256), 1)
    first = lane256 < HEAD_DIM
    zero = jnp.zeros((ROWS, 256), BF)

    def two_heads(v):
        return jnp.concatenate([jnp.where(first, v, zero), jnp.where(first, zero, v)], axis=0)

    def chunk(ids):
        qkv = dot_nn(jnp.concatenate([XA[i] for i in ids], axis=0), WCAT[...]).astype(BF)
        da = dot_nt(jnp.concatenate([DA[i] for i in ids], axis=0), WOC[...]).astype(BF)
        for h in range(2 * len(ids)):
            i, rs, at = ids[h // 2], pl.ds(h % 2 * ROWS, ROWS), slice(h * ROWS, h * ROWS + ROWS)
            q, k, v, g = qkv[at, :256], qkv[at, 256:512], qkv[at, 512:], da[at]
            kk, vv = two_heads(k), two_heads(v)
            sc = dot_nt(kk, q) * scale
            dp = dot_nt(vv, g)
            probs, dscore = [], []
            for n2 in range(2):
                cs = slice(n2 * 128, n2 * 128 + 128)
                s1 = jnp.where(inside, sc[cs], -jnp.inf)
                e = jnp.exp(s1 - jnp.max(s1, axis=0, keepdims=True))
                p1 = e * (1.0 / jnp.sum(e, axis=0, keepdims=True))
                d1 = dp[cs]
                t1 = jnp.sum(d1 * p1, axis=0, keepdims=True)
                probs.append(p1.astype(BF))
                dscore.append((p1 * (d1 - t1) * scale).astype(BF))
            pb = jnp.concatenate(probs, axis=0)
            ds = jnp.concatenate(dscore, axis=0)
            AS[i, rs, :] = dot_tn(pb, vv).astype(BF)
            DQKV[i, rs, :256] = dot_tn(ds, kk).astype(BF)
            dk = dot_nn(ds, q)
            DQKV[i, rs, 256:512] = jnp.where(first, dk[:128], dk[128:]).astype(BF)
            dv = dot_nn(pb, g)
            DQKV[i, rs, 512:] = jnp.where(first, dv[:128], dv[128:]).astype(BF)
        back = dot_nt(jnp.concatenate([DQKV[i] for i in ids], axis=0), WCAT[...]).astype(BF)
        for m, i in enumerate(ids):
            DXP[i] = back[256 * m : 256 * m + 256]

    await_act(1, left)
    fwd[4].start()
    await_act(0, right)
    fwd[5].start()
    rest(OL, o_r)

    def oslot(q, r):
        xs = 2 * c + q // 2
        other = (xs + 3) % NX if q // 2 == 0 else (xs + 1) % NX
        xh = jnp.where(c == r % 2, xs, other)
        return (2 * y + 2 - r // 2 + 4) % ZH, xh, q % 2

    def opix(q, r):
        zs, xh, cs = oslot(q, r)
        return (zs * NX + xh) * NC + cs

    WOC[COLS:, :] = jnp.zeros((256 - COLS, D), BF)
    lane12 = lanes(12)
    for q in range(4):
        parts = [None] * 3
        for r in range(NREP):
            WOC[RP * q : RP * q + RP, 128 * r : 128 * r + 128] = OL[opix(q, r), :RP, :]
            tl = OL[opix(q, r), RP : RP + 12, :].astype(F32)
            for t in range(3):
                v = jnp.where(lane12 // 16 == t, tl, 0.0)
                v = roll(v, 16 * (r - t))
                parts[t] = v if parts[t] is None else parts[t] + v
        for t in range(3):
            at = RP * q + 12 * t
            WOC[at : at + 12, 1024:1152] = parts[t].astype(BF)

    def dx_sib(i):
        return rcopy(
            DXP.at[i, pl.ds(pl.multiple_of(sib * ROWS, ROWS), ROWS)], DXS.at[i],
            sent.at[8], dx_r.at[0], (zh, x, sib, y, zl),
        )

    @pl.loop(0, NY)
    def _(n):
        off = jnp.where(n == 1, 3, jnp.where(n == 2, 1, jnp.where(n == 3, 2, 0)))
        i = (y + off) % NY

        @pl.when(n == 2)
        def _():
            await_act(0, opp)
            fwd[6].start()
            await_act(1, opp)
            fwd[7].start()

        await_sib(i)
        chunk((i,))
        dx_sib(i).start()

    OGRP, first_k = 4, (lambda h, side: 4 * side + h % 4)
    bufs = lambda h: (DWO, OXA, OSM, ORL, ORR, O2S) if h == OGRP else (DWS, RXA, SMB, RL, RR, R2S)

    def some(h, side):
        return pl.ds(first_k(h, side), 4 if h == OGRP else 1)

    def to_x(src, dst, rs, h, side):
        return rcopy(src, dst, sent.at[9 + (h == OGRP)], rs, (zh, (xr, xl)[side], c, y, zl))

    def far(h, side):
        ks = some(h, side)
        return to_x(bufs(h)[0].at[xo, ks], bufs(h)[1].at[ks], far_r.at[h * 2 + side], h, side)

    def near(h, side):
        ks = some(h, 1 - side)
        return to_x(bufs(h)[0].at[(xr, xl)[side], ks], bufs(h)[3 + side].at[ks], near_r.at[h], h, side)

    def summed(h, side):
        ks = some(h, side)
        return to_x(bufs(h)[2].at[ks], bufs(h)[3 + side].at[ks], near_r.at[h], h, side)

    def start_both(f, h):
        for side in range(2):
            f(h, side).start()

    def add_far(h):
        own_, got, out = bufs(h)[:3]
        for side in range(2):
            far(h, side).wait_recv()
            for k in range(first_k(h, side), first_k(h, side) + (4 if h == OGRP else 1)):
                out[k] = (own_[(xr, xl)[side], k].astype(F32) + got[k].astype(F32)).astype(BF)
            summed(h, side).start()

    kown = zh * 2 + c

    def r2(h, k):
        src, dst, o = (O2S, OZ, 1) if h == OGRP else (R2S, RZ, 0)
        return rcopy(src.at[k], dst.at[z], sent.at[11 + o], z_r.at[o], (k // 2, x, k % 2, y, c))

    def k_not_self(k):
        return jnp.logical_not((k == kown) & selfcore)

    def send_z(h):
        arrived(DWO.at[pl.ds(0, 2)] if h == OGRP else RL.at[pl.ds(0, 4)], near_r, h)
        own_, _, _, fl, fr, out = bufs(h)
        for side in range(2):
            for k in range(first_k(h, side), first_k(h, side) + (4 if h == OGRP else 1)):
                t = own_[x, k].astype(F32) + fl[k].astype(F32) + fr[k].astype(F32)
                out[k] = t.astype(BF)

                @pl.when(k_not_self(k))
                def _():
                    r2(h, k).start()

    def z_sum(h, buf, src):
        @pl.when(selfcore)
        def _():
            buf[z] = src[kown]

        @pl.when(selfcore)
        def _():
            arrived(buf.at[pl.ds(0, 7)], z_r, h // 4)

        @pl.when(jnp.logical_not(selfcore))
        def _():
            arrived(buf, z_r, h // 4)

        t = buf[0].astype(F32)
        for i in range(1, NZ):
            t = t + buf[i].astype(F32)
        return t.astype(BF)

    DWOB[...] = dot_tn(AS[...].reshape(NY * 256, 256), DA[...].reshape(NY * 256, D)).astype(BF)
    for q in range(4):
        tt = [DWOB[RP * q + 12 * t : RP * q + 12 * t + 12, 1024:1152].astype(F32) for t in range(3)]
        for r in range(NREP):
            zs, x2, cs = oslot(q, r)
            k = zs * 2 + cs
            DWO[x2, k, :RP, :] = DWOB[RP * q : RP * q + RP, 128 * r : 128 * r + 128]
            tail = None
            for t in range(3):
                v = roll(jnp.where(lane12 // 16 == r, tt[t], 0.0), 16 * (t - r))
                tail = v if tail is None else tail + v
            DWO[x2, k, RP:RO, :] = tail.astype(BF)
    start_both(far, OGRP)
    start_both(near, OGRP)

    dq_all = DQKV[...].reshape(NY * 256, 768)

    def dw_tile(i):
        lhs = XA[:, :, 128 * i : 128 * i + 128].reshape(NY * 256, 128)
        DWB[128 * i : 128 * i + 128, :] = dot_tn(lhs, dq_all).astype(BF)

    def pack(g):
        for q in range(4):
            p = g * 4 + q
            x2, k = (p // 2) % NX, (p // 8) * 2 + p % 2
            base = RP * p
            tail = None
            for s in range(3):
                DWS[x2, k, RP * s : RP * s + RP, :] = DWB[base : base + RP, 256 * s : 256 * s + 128]
                t = DWB[base : base + RP, 256 * s + 128 : 256 * s + 256].astype(F32)
                t = roll(t[: RP // 2], 32 * s) + roll(t[RP // 2 :], 32 * s + 16)
                tail = t if tail is None else tail + t
            DWS[x2, k, 3 * RP : 3 * RP + RP // 2, :] = tail.astype(BF)

    def own_sum(i):
        half = pl.ds(pl.multiple_of(c * ROWS, ROWS), ROWS)
        return DXP[i, half, :].astype(F32) + DXS[i].astype(F32)

    def dx_far(side):
        rows = pl.ds(64 * side, 64)
        return rcopy(
            DXC.at[0, rows], DXH.at[side], sent.at[13], xh_r.at[side],
            (zh, x, c, (right, left)[side], zl),
        )

    def dx_near(side):
        return rcopy(
            DXC.at[1 + side], DXR.at[side], sent.at[14], dx_r.at[1],
            (zh, x, c, (right, left)[side], zl),
        )

    for i in (0, 1, 2, 4, 5, 6):
        dw_tile(i)
    for g in (0, 1, 4, 5):
        pack(g)
    start_both(far, 0)
    start_both(near, 0)
    start_both(far, 1)
    add_far(OGRP)
    arrived(DXS, dx_r, 0)
    DXC[0] = own_sum(opp).astype(BF)
    for side in range(2):
        dx_far(side).start()
    for i in (3, 7, 8):
        dw_tile(i)
    for g in (2, 3, 6, 7):
        pack(g)
    start_both(far, 2)
    add_far(0)
    start_both(near, 1)
    add_far(1)
    start_both(far, 3)
    start_both(near, 2)
    send_z(OGRP)
    for side in range(2):
        dx_far(side).wait_recv()
        t = own_sum((right, left)[side])
        a, b = t[:64], t[64:]
        if side == 0:
            a = a + DXH[0].astype(F32)
        else:
            b = b + DXH[1].astype(F32)
        DXC[1 + side, :64, :] = a.astype(BF)
        DXC[1 + side, 64:, :] = b.astype(BF)
        dx_near(side).start()
    add_far(2)
    start_both(near, 3)
    send_z(0)
    add_far(3)
    send_z(1)

    head, foot = pl.ds(0, RA), pl.ds(RA, RO)

    def home_copy():
        r = home[3] * ZL + home[4]
        return rcopy(FO, FL.at[r, foot], sent.at[15], t_r.at[0], home)

    def home_arrival():
        return rcopy(FO, FL.at[rep, foot], sent.at[15], t_r.at[0], me)

    def fin(dr, part, o):
        r = (rep + dr) % NREP
        b = FL.at[rep, part]
        return rcopy(b, b, sent.at[16 + o], f_r.at[o], (zh, x, c, r // ZL, r % ZL))

    FO[...] = z_sum(OGRP, OZ, O2S)
    home_copy().start()
    send_z(2)
    send_z(3)
    home_arrival().wait_recv()

    @pl.loop(1, NREP)
    def _(dr):
        fin(dr, foot, 1).start()

    FL[rep, :RA, :] = z_sum(0, RZ, R2S)

    @pl.loop(1, NREP)
    def _(dr):
        fin(dr, head, 0).start()

    arrived(DXR, dx_r, 1)
    GI[...] = (own_sum(y) + DXR[0].astype(F32) + DXR[1].astype(F32)).astype(BF)
    gi_out = pltpu.make_async_copy(GI, gi_ref, lsem.at[6])
    gi_out.start()

    def left_from(ref, idx):
        rcopy(ref, ref, sent.at[idx], t_r.at[0], me).wait_send()

    left_from(XA.at[pl.ds(0, 3)], 0)
    left_from(XA.at[pl.ds(0, 3)], 1)
    left_from(XA.at[0], 2)
    hub_copy().wait_send()

    @pl.when(selfcore)
    def _():
        for b, idx in ((WL, 4), (OL, 6), (RZ, 11), (OZ, 12)):
            left_from(b.at[pl.ds(0, 7)], idx)

    @pl.when(jnp.logical_not(selfcore))
    def _():
        for b, idx in ((WL, 4), (OL, 6), (RZ, 11), (OZ, 12)):
            left_from(b.at[pl.ds(0, 8)], idx)

    left_from(WL.at[pl.ds(0, 24)], 5)
    left_from(OL.at[pl.ds(0, 24)], 7)
    left_from(DXS, 8)
    left_from(DWS.at[pl.ds(0, 3)], 9)
    left_from(DWO.at[pl.ds(0, 3)], 10)
    left_from(DXH, 13)
    left_from(DXR, 14)
    home_copy().wait_send()

    for o, part in enumerate((head, foot)):
        b = FL.at[pl.ds(0, 7), part]
        arrived(b, f_r, o)
        left_from(b, 16 + o)

    lane36 = lanes(RP)
    for s in range(3):
        last, lastt = None, None
        for t in range(9):
            if t < 8:
                main = roll(FL[t, RP * s : RP * s + RP, :].astype(F32), 16 * t)
            out = main
            if t > 0:
                prev = jnp.where(lane36 < 16 * (t - 1), last, lastt)
                out = prev if t == 8 else jnp.where(lane36 >= 16 * t, main, prev)
            GW[:, s * D + 128 * t : s * D + 128 * t + 128] = out.astype(GW.dtype)
            if t < 8:
                last = main
                tl = FL[t, 3 * RP : 3 * RP + RP // 2, :].astype(F32)
                halves = [roll(tl, 16 * t - 32 * s - 16 * h) for h in range(2)]
                lastt = jnp.concatenate(halves, axis=0)
    parts = [None] * 3
    for r in range(NREP):
        at = 3 * D + 128 * r
        GW[:, at : at + 128] = FL[r, RA : RA + RP, :].astype(GW.dtype)
        tl = FL[r, RA + RP : RA + RP + 12, :].astype(F32)
        for t in range(3):
            v = roll(jnp.where(lane12 // 16 == t, tl, 0.0), 16 * (r - t))
            parts[t] = v if parts[t] is None else parts[t] + v
    GW[:, 3 * D + 1024 :] = jnp.concatenate(parts, axis=0).astype(GW.dtype)
    gw_out = pltpu.make_async_copy(GW, gw_ref, lsem.at[7])
    gw_out.start()
    gi_out.wait()
    gw_out.wait()


def vm(*shape, dtype=BF):
    return pltpu.VMEM(shape, dtype)


def local(tokens, out_grad, wq, wk, wv, wo):
    rows = tokens.reshape(-1, D)
    drows = out_grad.reshape(-1, D)
    dma = lambda n: pltpu.SemaphoreType.DMA((n,))
    hbm = pl.BlockSpec(memory_space=pl.ANY)
    gi, gw = pl.pallas_call(
        kernel,
        out_shape=(
            jax.ShapeDtypeStruct((ROWS, D), BF),
            jax.ShapeDtypeStruct((RP, 4 * D), BF),
        ),
        in_specs=[hbm] * 6,
        out_specs=(hbm, hbm),
        scratch_shapes=[
            vm(NY, 256, D), vm(NY, 256, D), vm(4, RP, D),
            vm(RA, 128), vm(RO, 128), vm(RO, 128), vm(NPIX, RA, 128), vm(NPIX, RO, 128),
            vm(D, 768), vm(256, D), vm(NY, 256, 768), vm(NY, 256, 256),
            vm(NY, 256, D), vm(NY, ROWS, D), vm(3, ROWS, D), vm(2, 64, D), vm(2, ROWS, D),
            vm(D, 768), vm(256, D), vm(NX, 8, RA, 128), *[vm(8, RA, 128)] * 5, vm(NZ, RA, 128),
            vm(NX, 8, RO, 128), *[vm(8, RO, 128)] * 5, vm(NZ, RO, 128),
            vm(RO, 128), vm(NREP, RF, 128), vm(ROWS, D), vm(RP, 4 * D),
            dma(8), dma(20), dma(8), dma(4), dma(1), dma(17), dma(17), dma(2), dma(2), dma(10),
            dma(5), dma(2), dma(1), dma(4),
        ],
        compiler_params=pltpu.CompilerParams(
            collective_id=0, has_side_effects=True, vmem_limit_bytes=60 * 2**20
        ),
    )(rows, drows, wq, wk, wv, wo)
    return gi.reshape(tokens.shape), gw.astype(F32)


def solution(mesh):
    torus = Mesh(mesh.devices.reshape(ZH, NX, NC, NY, ZL), AXES)
    act = P(AXES, None, None)
    w = P(("zh", "x", "c"), None)
    return jax.shard_map(
        local,
        mesh=torus,
        in_specs=(act, act, w, w, w, w),
        out_specs=(act, w),
        check_vma=False,
    )
```

```python
import jax
import jax.numpy as jnp
from jax import lax
from jax.experimental import pallas as pl
from jax.experimental.pallas import tpu as pltpu
from jax.sharding import Mesh
from jax.sharding import PartitionSpec as P

D = 1152
FRAMES = 16
HEAD_DIM = 72
ZH, NX, NC, NY, ZL = 4, 4, 2, 4, 2
NZ = ZH * ZL
NPIX = ZH * NX * NC
NREP = NY * ZL
ROWS = 128
RP = D // NPIX
COLS = 2 * HEAD_DIM
RA = 128
RO = 48
RF = RA + RO
BF = jnp.bfloat16
F32 = jnp.float32
AXES = ("zh", "x", "c", "y", "zl")


def dot_nn(a, b):
    return lax.dot_general(a, b, (((1,), (0,)), ((), ())), preferred_element_type=F32)


def dot_nt(a, b):
    return lax.dot_general(a, b, (((1,), (1,)), ((), ())), preferred_element_type=F32)


def dot_tn(a, b):
    return lax.dot_general(a, b, (((0,), (0,)), ((), ())), preferred_element_type=F32)


def roll(v, shift):
    shift = shift % 128
    return v if shift == 0 else pltpu.roll(v, shift, 1)


def lanes(rows):
    return lax.broadcasted_iota(jnp.int32, (rows, 128), 1)


def kernel(
    x_ref, d_ref, wq_ref, wk_ref, wv_ref, wo_ref, gi_ref, gw_ref,
    XA, DA, WIN, WS, OSRC, OH, WL, OL, WCAT, WOC, DQKV, AS, DXP, DXS, DXC, DXH, DXR,
    DWB, DWOB, DWS, RXA, SMB, RL, RR, R2S, RZ, DWO, OXA, OSM, ORL, ORR, O2S, OZ, FO, FL, GI, GW,
    lsem, sent, a_r, s_r, h_r, w_r, o_r, dx_r, xh_r, far_r, near_r, z_r, t_r, f_r,
):
    zh, x, c, y, zl = [lax.axis_index(a) for a in AXES]
    pix = (zh * NX + x) * NC + c
    rep = y * ZL + zl
    z = zh * ZL + zl
    sib = 1 - c
    me = (zh, x, c, y, zl)
    selfcore = zl == c
    right, left, opp = (y + 1) % NY, (y + 3) % NY, (y + 2) % NY
    xr, xl, xo = (x + 1) % NX, (x + 3) % NX, (x + 2) % NX
    pair = jnp.where(x % 2 == 0, (x + 3) % NX, xr)
    hub = ((2 * zh + 2 - y + 4) % ZH, jnp.where(zl == x // 2, x, pair), c, zh, x // 2)
    back = jnp.where(x % 2 == 0, (x + 3) % NX, xr)
    there = x // 2 == zl
    home = (y, jnp.where(there, x, back), c, (2 * y + 2 - zh + 4) % NY, jnp.where(there, zl, 1 - zl))

    def rcopy(src, dst, ss, rs, dev):
        return pltpu.make_async_remote_copy(
            src_ref=src, dst_ref=dst, send_sem=ss, recv_sem=rs,
            device_id=dev, device_id_type=pl.DeviceIdType.MESH,
        )

    def blk(kind, yb, cb):
        return (XA, DA)[kind].at[yb, pl.ds(pl.multiple_of(cb * ROWS, ROWS), ROWS)]

    wins = [
        pltpu.make_async_copy(r, WIN.at[k], lsem.at[2 + k])
        for k, r in enumerate((wq_ref, wk_ref, wv_ref, wo_ref))
    ]
    own = [pltpu.make_async_copy(r, blk(k, y, c), lsem.at[k]) for k, r in enumerate((x_ref, d_ref))]
    for o in own + wins:
        o.start()
    bar = pltpu.get_barrier_semaphore()

    def greet(dev):
        pl.semaphore_signal(bar, inc=1, device_id=dev, device_id_type=pl.DeviceIdType.MESH)

    @pl.loop(0, 16)
    def _(i):
        @pl.when(i != z * 2 + c)
        def _():
            greet((i // 4, x, i % 2, y, (i // 2) % 2))

    for dy in range(1, NY):
        greet((zh, x, c, (y + dy) % NY, zl))
        greet((zh, x, c, (y + dy) % NY, 1 - zl))
    greet((zh, xr, c, y, zl))
    greet((zh, xl, c, y, zl))

    greet(hub)
    greet(home)

    ii = lax.broadcasted_iota(jnp.int32, (D, 256), 0)
    nn = lax.broadcasted_iota(jnp.int32, (D, 256), 1)
    sel = jnp.where((ii == nn + COLS * rep) & (nn < COLS), 1.0, 0.0).astype(BF)
    want = jnp.where(nn < 128, nn + 128 * rep, nn - 128 + 1024 + 16 * rep)
    osel = jnp.where((ii == want) & (nn < COLS), 1.0, 0.0).astype(BF)
    for w in wins:
        w.wait()
    tail = None
    for s in range(3):
        b = dot_nn(WIN[s], sel)
        WS[RP * s : RP * s + RP, :] = b[:, :128].astype(BF)
        t = b[:, 128:256]
        t = roll(t[: RP // 2], 32 * s) + roll(t[RP // 2 :], 32 * s + 16)
        tail = t if tail is None else tail + t
    WS[3 * RP : 3 * RP + RP // 2, :] = tail.astype(BF)
    b = dot_nn(WIN[3], osel)
    OSRC[:RP, :] = b[:, :128].astype(BF)
    t = b[:, 128:256]
    tail = t[:12] + roll(t[12:24], 16) + roll(t[24:36], 32)
    OSRC[RP : RP + 12, :] = tail.astype(BF)
    for o in own:
        o.wait()

    pl.semaphore_wait(bar, 15 + 6 + 2 + 2)

    def act(kind, yb, cb, to_y, to_c, idx):
        rs = s_r.at[yb] if to_c is sib else a_r.at[kind * 4 + yb]
        return rcopy(blk(kind, yb, cb), blk(kind, yb, cb), sent.at[idx // 6], rs, (zh, x, to_c, to_y, zl))

    def hub_copy():
        return rcopy(OSRC, OH, sent.at[3], h_r.at[0], hub)

    sends = [
        act(0, y, c, right, c, 0), act(1, y, c, left, c, 1),
        act(1, y, c, right, c, 2), act(0, y, c, left, c, 3),
        act(0, y, c, y, sib, 4), act(1, y, c, y, sib, 5),
    ]

    hub_copy().start()
    for s in sends[:4]:
        s.start()

    def col(k, xs):
        return ((k // 2) * NX + xs) * NC + k % 2

    def along_z(src, buf, ss, rs, i):
        return rcopy(src, buf.at[pix], sent.at[ss], rs.at[zh * 2 + c], (i // 2, x, zl, y, i % 2))

    def not_self(i):
        return jnp.logical_not((i == z) & selfcore)

    def spread(src, buf, ss, rs):
        @pl.when(selfcore)
        def _():
            buf[pix] = src[...]

        for dz in (1, 7, 2, 6, 3, 5, 4):
            along_z(src, buf, ss, rs, (z + dz) % NZ).start()

        @pl.when(jnp.logical_not(selfcore))
        def _():
            along_z(src, buf, ss, rs, z).start()

    def around_x(buf, ss, rs, p, to, idx):
        return rcopy(buf.at[p], buf.at[p], sent.at[ss + 1], rs.at[idx], (zh, to, c, y, zl))

    def arrived(ref, rs, idx):
        rcopy(ref, ref, sent.at[0], rs.at[idx], me).wait_recv()

    def both_ways(buf, ss, rs, lo, hi):
        @pl.loop(lo, hi)
        def _(n):
            n = jnp.where(n < 4, n, jnp.where(n < 6, n + 2, n - 2))
            k = (2 * zh + n) % 8
            p = col(k, x)

            @pl.when(jnp.logical_not((p == pix) & selfcore))
            def _():
                arrived(buf.at[p], rs, k)

            around_x(buf, ss, rs, p, xr, jnp.where(k % 2 == 0, 8 + k, 16)).start()
            around_x(buf, ss, rs, p, xl, jnp.where(k % 2 == 0, 16, 8 + k)).start()

    def onward(buf, ss, rs, lo, hi):
        @pl.loop(lo, hi)
        def _(n):
            k = 2 * ((zh + jnp.where(n < 2, n, 5 - n)) % ZH)
            p, q = col(k, xl), col(k + 1, xr)
            arrived(buf.at[p], rs, 8 + k)
            around_x(buf, ss, rs, p, xr, 17).start()
            arrived(buf.at[q], rs, 9 + k)
            around_x(buf, ss, rs, q, xl, 17).start()

    def rest(buf, rs):
        arrived(buf.at[pl.ds(0, 8)], rs, 16)
        arrived(buf.at[pl.ds(0, 8)], rs, 17)

    spread(WS, WL, 4, w_r)
    for s in sends[4:]:
        s.start()
    both_ways(WL, 4, w_r, 0, 2)
    hub_copy().wait_recv()
    spread(OH, OL, 6, o_r)
    both_ways(WL, 4, w_r, 2, 6)
    onward(WL, 4, w_r, 0, 1)
    both_ways(WL, 4, w_r, 6, 8)

    low16 = lanes(RP // 2) < 16

    def unpack(xs):
        for x2 in range(NX):
            @pl.when(xs == x2)
            def _():
                @pl.loop(0, ZH)
                def _(zs):
                    out = WCAT.at[pl.ds(pl.multiple_of(zs * 288, 16), 288)]
                    for cs in range(NC):
                        p, base = (zs * NX + x2) * NC + cs, RP * (x2 * NC + cs)
                        tl = WL[p, 3 * RP : 3 * RP + RP // 2, :].astype(F32)
                        for s in range(3):
                            out[base : base + RP, 256 * s : 256 * s + 128] = WL[p, RP * s : RP * s + RP, :]
                            for half in range(2):
                                v = jnp.where(low16, roll(tl, -(32 * s + 16 * half)), 0.0).astype(BF)
                                at = base + half * (RP // 2)
                                out[at : at + RP // 2, 256 * s + 128 : 256 * s + 256] = v

    def await_act(kind, yb):
        rcopy(blk(kind, yb, c), blk(kind, yb, c), sent.at[0], a_r.at[kind * 4 + yb], me).wait_recv()

    def await_sib(yb):
        rcopy(XA.at[yb], XA.at[yb], sent.at[0], s_r.at[yb], me).wait_recv()

    fwd = [
        act(0, left, c, right, c, 6), act(1, right, c, left, c, 7),
        act(0, left, c, y, sib, 8), act(1, right, c, y, sib, 9),
        act(1, left, c, y, sib, 10), act(0, right, c, y, sib, 11),
        act(0, opp, c, y, sib, 12), act(1, opp, c, y, sib, 13),
    ]
    await_act(0, left)
    fwd[0].start()
    fwd[2].start()
    await_act(1, right)
    fwd[1].start()
    fwd[3].start()
    both_ways(OL, 6, o_r, 0, 8)
    unpack(x)
    onward(WL, 4, w_r, 1, 4)
    onward(OL, 6, o_r, 0, 4)
    arrived(WL.at[pl.ds(0, 8)], w_r, 16)
    unpack(xl)
    unpack(xr)
    arrived(WL.at[pl.ds(0, 8)], w_r, 17)
    unpack(xo)

    scale = 1.0 / HEAD_DIM**0.5
    row = lax.broadcasted_iota(jnp.int32, (ROWS, 128), 0)
    col_ = lax.broadcasted_iota(jnp.int32, (ROWS, 128), 1)
    inside = row // FRAMES == col_ // FRAMES
    lane256 = lax.broadcasted_iota(jnp.int32, (ROWS, 256), 1)
    first = lane256 < HEAD_DIM
    zero = jnp.zeros((ROWS, 256), BF)

    def two_heads(v):
        return jnp.concatenate([jnp.where(first, v, zero), jnp.where(first, zero, v)], axis=0)

    def chunk(ids):
        qkv = dot_nn(jnp.concatenate([XA[i] for i in ids], axis=0), WCAT[...]).astype(BF)
        da = dot_nt(jnp.concatenate([DA[i] for i in ids], axis=0), WOC[...]).astype(BF)
        for h in range(2 * len(ids)):
            i, rs, at = ids[h // 2], pl.ds(h % 2 * ROWS, ROWS), slice(h * ROWS, h * ROWS + ROWS)
            q, k, v, g = qkv[at, :256], qkv[at, 256:512], qkv[at, 512:], da[at]
            kk, vv = two_heads(k), two_heads(v)
            sc = dot_nt(kk, q) * scale
            dp = dot_nt(vv, g)
            probs, dscore = [], []
            for n2 in range(2):
                cs = slice(n2 * 128, n2 * 128 + 128)
                s1 = jnp.where(inside, sc[cs], -jnp.inf)
                e = jnp.exp(s1 - jnp.max(s1, axis=0, keepdims=True))
                p1 = e * (1.0 / jnp.sum(e, axis=0, keepdims=True))
                d1 = dp[cs]
                t1 = jnp.sum(d1 * p1, axis=0, keepdims=True)
                probs.append(p1.astype(BF))
                dscore.append((p1 * (d1 - t1) * scale).astype(BF))
            pb = jnp.concatenate(probs, axis=0)
            ds = jnp.concatenate(dscore, axis=0)
            AS[i, rs, :] = dot_tn(pb, vv).astype(BF)
            DQKV[i, rs, :256] = dot_tn(ds, kk).astype(BF)
            dk = dot_nn(ds, q)
            DQKV[i, rs, 256:512] = jnp.where(first, dk[:128], dk[128:]).astype(BF)
            dv = dot_nn(pb, g)
            DQKV[i, rs, 512:] = jnp.where(first, dv[:128], dv[128:]).astype(BF)

    await_act(1, left)
    fwd[4].start()
    await_act(0, right)
    fwd[5].start()
    rest(OL, o_r)

    def oslot(q, r):
        xs = 2 * c + q // 2
        other = (xs + 3) % NX if q // 2 == 0 else (xs + 1) % NX
        xh = jnp.where(c == r % 2, xs, other)
        return (2 * y + 2 - r // 2 + 4) % ZH, xh, q % 2

    def opix(q, r):
        zs, xh, cs = oslot(q, r)
        return (zs * NX + xh) * NC + cs

    WOC[COLS:, :] = jnp.zeros((256 - COLS, D), BF)
    lane12 = lanes(12)
    for q in range(4):
        parts = [None] * 3
        for r in range(NREP):
            WOC[RP * q : RP * q + RP, 128 * r : 128 * r + 128] = OL[opix(q, r), :RP, :]
            tl = OL[opix(q, r), RP : RP + 12, :].astype(F32)
            for t in range(3):
                v = jnp.where(lane12 // 16 == t, tl, 0.0)
                v = roll(v, 16 * (r - t))
                parts[t] = v if parts[t] is None else parts[t] + v
        for t in range(3):
            at = RP * q + 12 * t
            WOC[at : at + 12, 1024:1152] = parts[t].astype(BF)

    def dx_sib(i):
        return rcopy(
            DXP.at[i, pl.ds(pl.multiple_of(sib * ROWS, ROWS), ROWS)], DXS.at[i],
            sent.at[8], dx_r.at[i], (zh, x, sib, y, zl),
        )

    @pl.loop(0, NY)
    def _(n):
        off = jnp.where(n == 1, 3, jnp.where(n == 2, 1, jnp.where(n == 3, 2, 0)))
        i = (y + off) % NY

        @pl.when(n == 1)
        def _():
            await_act(0, opp)
            fwd[6].start()
            await_act(1, opp)
            fwd[7].start()

        await_sib(i)
        chunk((i,))

    OGRP, first_k = 4, (lambda h, side: 4 * side if h == 4 else (0, 1, 4, 5)[h] + 2 * side)
    bufs = lambda h: (DWO, OXA, OSM, ORL, ORR, O2S) if h == OGRP else (DWS, RXA, SMB, RL, RR, R2S)

    def some(h, side):
        return pl.ds(first_k(h, side), 4 if h == OGRP else 1)

    def to_x(src, dst, rs, h, side):
        return rcopy(src, dst, sent.at[9 + (h == OGRP)], rs, (zh, (xr, xl)[side], c, y, zl))

    def far(h, side):
        ks = some(h, side)
        return to_x(bufs(h)[0].at[xo, ks], bufs(h)[1].at[ks], far_r.at[h * 2 + side], h, side)

    def near(h, side):
        ks = some(h, 1 - side)
        return to_x(bufs(h)[0].at[(xr, xl)[side], ks], bufs(h)[3 + side].at[ks], near_r.at[h], h, side)

    def summed(h, side):
        ks = some(h, side)
        return to_x(bufs(h)[2].at[ks], bufs(h)[3 + side].at[ks], near_r.at[h], h, side)

    def start_both(f, h):
        for side in range(2):
            f(h, side).start()

    def add_far(h):
        own_, got, out = bufs(h)[:3]
        for side in range(2):
            far(h, side).wait_recv()
            for k in range(first_k(h, side), first_k(h, side) + (4 if h == OGRP else 1)):
                out[k] = (own_[(xr, xl)[side], k].astype(F32) + got[k].astype(F32)).astype(BF)
            summed(h, side).start()

    kown = zh * 2 + c

    def r2(h, k):
        src, dst, o = (O2S, OZ, 1) if h == OGRP else (R2S, RZ, 0)
        return rcopy(src.at[k], dst.at[z], sent.at[11 + o], z_r.at[o], (k // 2, x, k % 2, y, c))

    def k_not_self(k):
        return jnp.logical_not((k == kown) & selfcore)

    def send_z(h):
        arrived(DWO.at[pl.ds(0, 2)] if h == OGRP else RL.at[pl.ds(0, 4)], near_r, h)
        own_, _, _, fl, fr, out = bufs(h)
        for side in range(2):
            for k in range(first_k(h, side), first_k(h, side) + (4 if h == OGRP else 1)):
                t = own_[x, k].astype(F32) + fl[k].astype(F32) + fr[k].astype(F32)
                out[k] = t.astype(BF)

                @pl.when(k_not_self(k))
                def _():
                    r2(h, k).start()

    def z_sum(h, buf, src):
        @pl.when(selfcore)
        def _():
            buf[z] = src[kown]

        @pl.when(selfcore)
        def _():
            arrived(buf.at[pl.ds(0, 7)], z_r, h // 4)

        @pl.when(jnp.logical_not(selfcore))
        def _():
            arrived(buf, z_r, h // 4)

        t = buf[0].astype(F32)
        for i in range(1, NZ):
            t = t + buf[i].astype(F32)
        return t.astype(BF)

    DWOB[...] = dot_tn(AS[...].reshape(NY * 256, 256), DA[...].reshape(NY * 256, D)).astype(BF)
    for q in range(4):
        tt = [DWOB[RP * q + 12 * t : RP * q + 12 * t + 12, 1024:1152].astype(F32) for t in range(3)]
        for r in range(NREP):
            zs, x2, cs = oslot(q, r)
            k = zs * 2 + cs
            DWO[x2, k, :RP, :] = DWOB[RP * q : RP * q + RP, 128 * r : 128 * r + 128]
            tail = None
            for t in range(3):
                v = roll(jnp.where(lane12 // 16 == r, tt[t], 0.0), 16 * (t - r))
                tail = v if tail is None else tail + v
            DWO[x2, k, RP:RO, :] = tail.astype(BF)
    start_both(far, OGRP)
    start_both(near, OGRP)

    dq_all = DQKV[...].reshape(NY * 256, 768)

    def dw_tile(i):
        lhs = XA[:, :, 128 * i : 128 * i + 128].reshape(NY * 256, 128)
        DWB[128 * i : 128 * i + 128, :] = dot_tn(lhs, dq_all).astype(BF)

    def pack(g):
        for q in range(4):
            p = g * 4 + q
            x2, k = (p // 2) % NX, (p // 8) * 2 + p % 2
            base = RP * p
            tail = None
            for s in range(3):
                DWS[x2, k, RP * s : RP * s + RP, :] = DWB[base : base + RP, 256 * s : 256 * s + 128]
                t = DWB[base : base + RP, 256 * s + 128 : 256 * s + 256].astype(F32)
                t = roll(t[: RP // 2], 32 * s) + roll(t[RP // 2 :], 32 * s + 16)
                tail = t if tail is None else tail + t
            DWS[x2, k, 3 * RP : 3 * RP + RP // 2, :] = tail.astype(BF)

    def own_sum(i):
        half = pl.ds(pl.multiple_of(c * ROWS, ROWS), ROWS)
        return DXP[i, half, :].astype(F32) + DXS[i].astype(F32)

    def dx_far(side):
        rows = pl.ds(64 * side, 64)
        return rcopy(
            DXC.at[0, rows], DXH.at[side], sent.at[13], xh_r.at[side],
            (zh, x, c, (right, left)[side], zl),
        )

    def dx_near(side, late):
        at = 64 * side if late else 64 - 64 * side
        i = (right, left)[side]
        t = own_sum(i)[at : at + 64]
        if late:
            t = t + DXH[side].astype(F32)
        DXC[1 + side, at : at + 64, :] = t.astype(BF)
        rows = pl.ds(at, 64)
        rcopy(
            DXC.at[1 + side, rows], DXR.at[side, rows], sent.at[14], dx_r.at[4], (zh, x, c, i, zl)
        ).start()

    def dx_mat(i):
        DXP[i] = dot_nt(DQKV[i], WCAT[...]).astype(BF)
        dx_sib(i).start()

    for i in range(5):
        dw_tile(i)
    for g in range(4):
        pack(g)
    start_both(far, 0)
    start_both(near, 0)
    start_both(far, 1)
    dx_mat(opp)
    for i in range(5, 9):
        dw_tile(i)
    for g in range(4, 8):
        pack(g)
    start_both(far, 2)
    add_far(OGRP)
    dx_mat(right)
    add_far(0)
    start_both(near, 1)
    dx_mat(left)
    arrived(DXS.at[opp], dx_r, opp)
    DXC[0] = own_sum(opp).astype(BF)
    for side in range(2):
        dx_far(side).start()
    arrived(DXS.at[right], dx_r, right)
    dx_near(0, False)
    add_far(1)
    start_both(far, 3)
    start_both(near, 2)
    arrived(DXS.at[left], dx_r, left)
    dx_near(1, False)
    send_z(OGRP)
    dx_mat(y)
    add_far(2)
    start_both(near, 3)
    send_z(0)
    add_far(3)
    send_z(1)

    head, foot = pl.ds(0, RA), pl.ds(RA, RO)

    def home_copy():
        r = home[3] * ZL + home[4]
        return rcopy(FO, FL.at[r, foot], sent.at[15], t_r.at[0], home)

    def home_arrival():
        return rcopy(FO, FL.at[rep, foot], sent.at[15], t_r.at[0], me)

    def fin(dr, part, o):
        r = (rep + dr) % NREP
        b = FL.at[rep, part]
        return rcopy(b, b, sent.at[16 + o], f_r.at[o], (zh, x, c, r // ZL, r % ZL))

    send_z(2)
    send_z(3)
    FO[...] = z_sum(OGRP, OZ, O2S)
    home_copy().start()
    for side in range(2):
        dx_far(side).wait_recv()
        dx_near(side, True)
    FL[rep, :RA, :] = z_sum(0, RZ, R2S)

    @pl.loop(1, NREP)
    def _(dr):
        fin(dr, head, 0).start()

    home_arrival().wait_recv()

    @pl.loop(1, NREP)
    def _(dr):
        fin(dr, foot, 1).start()

    arrived(DXS.at[y], dx_r, y)
    arrived(DXR, dx_r, 4)
    GI[...] = (own_sum(y) + DXR[0].astype(F32) + DXR[1].astype(F32)).astype(BF)
    gi_out = pltpu.make_async_copy(GI, gi_ref, lsem.at[6])
    gi_out.start()

    def left_from(ref, idx):
        rcopy(ref, ref, sent.at[idx], t_r.at[0], me).wait_send()

    left_from(XA.at[pl.ds(0, 3)], 0)
    left_from(XA.at[pl.ds(0, 3)], 1)
    left_from(XA.at[0], 2)
    hub_copy().wait_send()

    @pl.when(selfcore)
    def _():
        for b, idx in ((WL, 4), (OL, 6), (RZ, 11), (OZ, 12)):
            left_from(b.at[pl.ds(0, 7)], idx)

    @pl.when(jnp.logical_not(selfcore))
    def _():
        for b, idx in ((WL, 4), (OL, 6), (RZ, 11), (OZ, 12)):
            left_from(b.at[pl.ds(0, 8)], idx)

    left_from(WL.at[pl.ds(0, 24)], 5)
    left_from(OL.at[pl.ds(0, 24)], 7)
    left_from(DXS, 8)
    left_from(DWS.at[pl.ds(0, 3)], 9)
    left_from(DWO.at[pl.ds(0, 3)], 10)
    left_from(DXH, 13)
    left_from(DXR, 14)
    home_copy().wait_send()

    for o, part in enumerate((head, foot)):
        b = FL.at[pl.ds(0, 7), part]
        arrived(b, f_r, o)
        left_from(b, 16 + o)

    lane36 = lanes(RP)
    for s in range(3):
        last, lastt = None, None
        for t in range(9):
            if t < 8:
                main = roll(FL[t, RP * s : RP * s + RP, :].astype(F32), 16 * t)
            out = main
            if t > 0:
                prev = jnp.where(lane36 < 16 * (t - 1), last, lastt)
                out = prev if t == 8 else jnp.where(lane36 >= 16 * t, main, prev)
            GW[:, s * D + 128 * t : s * D + 128 * t + 128] = out.astype(GW.dtype)
            if t < 8:
                last = main
                tl = FL[t, 3 * RP : 3 * RP + RP // 2, :].astype(F32)
                halves = [roll(tl, 16 * t - 32 * s - 16 * h) for h in range(2)]
                lastt = jnp.concatenate(halves, axis=0)
    parts = [None] * 3
    for r in range(NREP):
        at = 3 * D + 128 * r
        GW[:, at : at + 128] = FL[r, RA : RA + RP, :].astype(GW.dtype)
        tl = FL[r, RA + RP : RA + RP + 12, :].astype(F32)
        for t in range(3):
            v = roll(jnp.where(lane12 // 16 == t, tl, 0.0), 16 * (r - t))
            parts[t] = v if parts[t] is None else parts[t] + v
    GW[:, 3 * D + 1024 :] = jnp.concatenate(parts, axis=0).astype(GW.dtype)
    gw_out = pltpu.make_async_copy(GW, gw_ref, lsem.at[7])
    gw_out.start()
    gi_out.wait()
    gw_out.wait()


def finish(gi_ref, gw_ref, gi_out, gw_out, GI, GW, GF, sem):
    ins = [pltpu.make_async_copy(gw_ref, GW, sem.at[0]), pltpu.make_async_copy(gi_ref, GI, sem.at[1])]
    outs = [pltpu.make_async_copy(GF, gw_out, sem.at[2]), pltpu.make_async_copy(GI, gi_out, sem.at[3])]
    for i in ins:
        i.start()
    ins[0].wait()
    GF[...] = GW[...].astype(F32)
    outs[0].start()
    ins[1].wait()
    outs[1].start()
    for o in outs:
        o.wait()


def vm(*shape, dtype=BF):
    return pltpu.VMEM(shape, dtype)


def local(tokens, out_grad, wq, wk, wv, wo):
    rows = tokens.reshape(-1, D)
    drows = out_grad.reshape(-1, D)
    dma = lambda n: pltpu.SemaphoreType.DMA((n,))
    hbm = pl.BlockSpec(memory_space=pl.ANY)
    gi, gw = pl.pallas_call(
        kernel,
        out_shape=(
            jax.ShapeDtypeStruct((ROWS, D), BF),
            jax.ShapeDtypeStruct((RP, 4 * D), BF),
        ),
        in_specs=[hbm] * 6,
        out_specs=(hbm, hbm),
        scratch_shapes=[
            vm(NY, 256, D), vm(NY, 256, D), vm(4, RP, D),
            vm(RA, 128), vm(RO, 128), vm(RO, 128), vm(NPIX, RA, 128), vm(NPIX, RO, 128),
            vm(D, 768), vm(256, D), vm(NY, 256, 768), vm(NY, 256, 256),
            vm(NY, 256, D), vm(NY, ROWS, D), vm(3, ROWS, D), vm(2, 64, D), vm(2, ROWS, D),
            vm(D, 768), vm(256, D), vm(NX, 8, RA, 128), *[vm(8, RA, 128)] * 5, vm(NZ, RA, 128),
            vm(NX, 8, RO, 128), *[vm(8, RO, 128)] * 5, vm(NZ, RO, 128),
            vm(RO, 128), vm(NREP, RF, 128), vm(ROWS, D), vm(RP, 4 * D),
            dma(8), dma(20), dma(8), dma(4), dma(1), dma(18), dma(18), dma(5), dma(2), dma(10),
            dma(5), dma(2), dma(1), dma(4),
        ],
        compiler_params=pltpu.CompilerParams(
            collective_id=0, has_side_effects=True, vmem_limit_bytes=60 * 2**20
        ),
    )(rows, drows, wq, wk, wv, wo)
    gi, gw = pl.pallas_call(
        finish,
        out_shape=(
            jax.ShapeDtypeStruct((ROWS, D), BF),
            jax.ShapeDtypeStruct((RP, 4 * D), F32),
        ),
        in_specs=[hbm] * 2,
        out_specs=(hbm, hbm),
        scratch_shapes=[vm(ROWS, D), vm(RP, 4 * D), vm(RP, 4 * D, dtype=F32), dma(4)],
        compiler_params=pltpu.CompilerParams(vmem_limit_bytes=63 * 2**20),
    )(gi, gw)
    return gi.reshape(tokens.shape), gw


def solution(mesh):
    torus = Mesh(mesh.devices.reshape(ZH, NX, NC, NY, ZL), AXES)
    act = P(AXES, None, None)
    w = P(("zh", "x", "c"), None)
    return jax.shard_map(
        local,
        mesh=torus,
        in_specs=(act, act, w, w, w, w),
        out_specs=(act, w),
        check_vma=False,
    )
```

```python
import jax
import jax.numpy as jnp
from jax import lax
from jax.experimental import pallas as pl
from jax.experimental.pallas import tpu as pltpu
from jax.sharding import Mesh
from jax.sharding import PartitionSpec as P

D = 1152
FRAMES = 16
HEAD_DIM = 72
ZH, NX, NC, NY, ZL = 4, 4, 2, 4, 2
NZ = ZH * ZL
NPIX = ZH * NX * NC
NREP = NY * ZL
ROWS = 128
RP = D // NPIX
COLS = 2 * HEAD_DIM
RA = 128
RO = 48
RF = RA + RO
BF = jnp.bfloat16
F32 = jnp.float32
AXES = ("zh", "x", "c", "y", "zl")


def dot_nn(a, b):
    return lax.dot_general(a, b, (((1,), (0,)), ((), ())), preferred_element_type=F32)


def dot_nt(a, b):
    return lax.dot_general(a, b, (((1,), (1,)), ((), ())), preferred_element_type=F32)


def dot_tn(a, b):
    return lax.dot_general(a, b, (((0,), (0,)), ((), ())), preferred_element_type=F32)


def roll(v, shift):
    shift = shift % 128
    return v if shift == 0 else pltpu.roll(v, shift, 1)


def lanes(rows):
    return lax.broadcasted_iota(jnp.int32, (rows, 128), 1)


def kernel(
    x_ref, d_ref, wq_ref, wk_ref, wv_ref, wo_ref, gi_ref, gw_ref,
    XA, DA, WIN, WS, OSRC, OH, WL, OL, WCAT, WOC, DQKV, AS, DXP, DXS, DXC, DXH, DXR,
    DWB, DWOB, DWS, RXA, SMB, RL, RR, R2S, RZ, DWO, OXA, OSM, ORL, ORR, O2S, OZ, FO, FL, GI, GW,
    lsem, sent, a_r, s_r, h_r, w_r, o_r, dx_r, xh_r, far_r, near_r, z_r, t_r, f_r,
):
    zh, x, c, y, zl = [lax.axis_index(a) for a in AXES]
    pix = (zh * NX + x) * NC + c
    rep = y * ZL + zl
    z = zh * ZL + zl
    sib = 1 - c
    me = (zh, x, c, y, zl)
    selfcore = zl == c
    right, left, opp = (y + 1) % NY, (y + 3) % NY, (y + 2) % NY
    xr, xl, xo = (x + 1) % NX, (x + 3) % NX, (x + 2) % NX
    pair = jnp.where(x % 2 == 0, (x + 3) % NX, xr)
    hub = ((2 * zh + 2 - y + 4) % ZH, jnp.where(zl == x // 2, x, pair), c, zh, x // 2)
    back = jnp.where(x % 2 == 0, (x + 3) % NX, xr)
    there = x // 2 == zl
    home = (y, jnp.where(there, x, back), c, (2 * y + 2 - zh + 4) % NY, jnp.where(there, zl, 1 - zl))

    def rcopy(src, dst, ss, rs, dev):
        return pltpu.make_async_remote_copy(
            src_ref=src, dst_ref=dst, send_sem=ss, recv_sem=rs,
            device_id=dev, device_id_type=pl.DeviceIdType.MESH,
        )

    def blk(kind, yb, cb):
        return (XA, DA)[kind].at[yb, pl.ds(pl.multiple_of(cb * ROWS, ROWS), ROWS)]

    wins = [
        pltpu.make_async_copy(r, WIN.at[k], lsem.at[2 + k])
        for k, r in enumerate((wq_ref, wk_ref, wv_ref, wo_ref))
    ]
    own = [pltpu.make_async_copy(r, blk(k, y, c), lsem.at[k]) for k, r in enumerate((x_ref, d_ref))]
    for o in own + wins:
        o.start()
    bar = pltpu.get_barrier_semaphore()

    def greet(dev):
        pl.semaphore_signal(bar, inc=1, device_id=dev, device_id_type=pl.DeviceIdType.MESH)

    @pl.loop(0, 16)
    def _(i):
        @pl.when(i != z * 2 + c)
        def _():
            greet((i // 4, x, i % 2, y, (i // 2) % 2))

    for dy in range(1, NY):
        greet((zh, x, c, (y + dy) % NY, zl))
        greet((zh, x, c, (y + dy) % NY, 1 - zl))
    greet((zh, xr, c, y, zl))
    greet((zh, xl, c, y, zl))

    greet(hub)
    greet(home)

    ii = lax.broadcasted_iota(jnp.int32, (256, 256), 0)
    nn = lax.broadcasted_iota(jnp.int32, (256, 256), 1)
    sel = jnp.where((ii == nn + 16 * rep) & (nn < COLS), 1.0, 0.0).astype(BF)
    osel = jnp.where((ii == nn + 16 * rep) & (nn < 16), 1.0, 0.0).astype(BF)[:128, :128]
    win = pl.multiple_of(128 * rep, 128)
    for w in wins:
        w.wait()
    tail = None
    for s in range(3):
        b = dot_nn(WIN[s, :, pl.ds(win, 256)], sel)
        WS[RP * s : RP * s + RP, :] = b[:, :128].astype(BF)
        t = b[:, 128:256]
        t = roll(t[: RP // 2], 32 * s) + roll(t[RP // 2 :], 32 * s + 16)
        tail = t if tail is None else tail + t
    WS[3 * RP : 3 * RP + RP // 2, :] = tail.astype(BF)
    OSRC[:RP, :] = WIN[3, :, pl.ds(win, 128)]
    t = dot_nn(WIN[3, :, 1024:], osel)
    tail = t[:12] + roll(t[12:24], 16) + roll(t[24:36], 32)
    OSRC[RP : RP + 12, :] = tail.astype(BF)
    for o in own:
        o.wait()

    pl.semaphore_wait(bar, 15 + 6 + 2 + 2)

    def act(kind, yb, cb, to_y, to_c, idx):
        rs = s_r.at[yb] if to_c is sib else a_r.at[kind * 4 + yb]
        return rcopy(blk(kind, yb, cb), blk(kind, yb, cb), sent.at[idx // 6], rs, (zh, x, to_c, to_y, zl))

    def hub_copy():
        return rcopy(OSRC, OH, sent.at[3], h_r.at[0], hub)

    sends = [
        act(0, y, c, right, c, 0), act(1, y, c, left, c, 1),
        act(1, y, c, right, c, 2), act(0, y, c, left, c, 3),
        act(0, y, c, y, sib, 4), act(1, y, c, y, sib, 5),
    ]

    hub_copy().start()
    for s in sends[:4]:
        s.start()

    def col(k, xs):
        return ((k // 2) * NX + xs) * NC + k % 2

    def along_z(src, buf, ss, rs, i):
        return rcopy(src, buf.at[pix], sent.at[ss], rs.at[zh * 2 + c], (i // 2, x, zl, y, i % 2))

    def not_self(i):
        return jnp.logical_not((i == z) & selfcore)

    def spread(src, buf, ss, rs):
        @pl.when(selfcore)
        def _():
            buf[pix] = src[...]

        for dz in (1, 7, 2, 6, 3, 5, 4):
            along_z(src, buf, ss, rs, (z + dz) % NZ).start()

        @pl.when(jnp.logical_not(selfcore))
        def _():
            along_z(src, buf, ss, rs, z).start()

    def around_x(buf, ss, rs, p, to, idx):
        return rcopy(buf.at[p], buf.at[p], sent.at[ss + 1], rs.at[idx], (zh, to, c, y, zl))

    def arrived(ref, rs, idx):
        rcopy(ref, ref, sent.at[0], rs.at[idx], me).wait_recv()

    def both_ways(buf, ss, rs, lo, hi):
        @pl.loop(lo, hi)
        def _(n):
            n = jnp.where(n < 4, n, jnp.where(n < 6, n + 2, n - 2))
            k = (2 * zh + n) % 8
            p = col(k, x)

            @pl.when(jnp.logical_not((p == pix) & selfcore))
            def _():
                arrived(buf.at[p], rs, k)

            around_x(buf, ss, rs, p, xr, jnp.where(k % 2 == 0, 8 + k, 16)).start()
            around_x(buf, ss, rs, p, xl, jnp.where(k % 2 == 0, 16, 8 + k)).start()

    def onward(buf, ss, rs, lo, hi):
        @pl.loop(lo, hi)
        def _(n):
            k = 2 * ((zh + jnp.where(n < 2, n, 5 - n)) % ZH)
            p, q = col(k, xl), col(k + 1, xr)
            arrived(buf.at[p], rs, 8 + k)
            around_x(buf, ss, rs, p, xr, 17).start()
            arrived(buf.at[q], rs, 9 + k)
            around_x(buf, ss, rs, q, xl, 17).start()

    def rest(buf, rs):
        arrived(buf.at[pl.ds(0, 8)], rs, 16)
        arrived(buf.at[pl.ds(0, 8)], rs, 17)

    spread(WS, WL, 4, w_r)
    for s in sends[4:]:
        s.start()
    both_ways(WL, 4, w_r, 0, 2)
    hub_copy().wait_recv()
    spread(OH, OL, 6, o_r)
    both_ways(WL, 4, w_r, 2, 6)
    onward(WL, 4, w_r, 0, 1)
    both_ways(WL, 4, w_r, 6, 8)

    low16 = lanes(RP // 2) < 16

    def unpack(xs):
        for x2 in range(NX):
            @pl.when(xs == x2)
            def _():
                @pl.loop(0, ZH)
                def _(zs):
                    out = WCAT.at[pl.ds(pl.multiple_of(zs * 288, 16), 288)]
                    for cs in range(NC):
                        p, base = (zs * NX + x2) * NC + cs, RP * (x2 * NC + cs)
                        tl = WL[p, 3 * RP : 3 * RP + RP // 2, :].astype(F32)
                        for s in range(3):
                            out[base : base + RP, 256 * s : 256 * s + 128] = WL[p, RP * s : RP * s + RP, :]
                            for half in range(2):
                                v = jnp.where(low16, roll(tl, -(32 * s + 16 * half)), 0.0).astype(BF)
                                at = base + half * (RP // 2)
                                out[at : at + RP // 2, 256 * s + 128 : 256 * s + 256] = v

    def await_act(kind, yb):
        rcopy(blk(kind, yb, c), blk(kind, yb, c), sent.at[0], a_r.at[kind * 4 + yb], me).wait_recv()

    def await_sib(yb):
        rcopy(XA.at[yb], XA.at[yb], sent.at[0], s_r.at[yb], me).wait_recv()

    fwd = [
        act(0, left, c, right, c, 6), act(1, right, c, left, c, 7),
        act(0, left, c, y, sib, 8), act(1, right, c, y, sib, 9),
        act(1, left, c, y, sib, 10), act(0, right, c, y, sib, 11),
        act(0, opp, c, y, sib, 12), act(1, opp, c, y, sib, 13),
    ]
    await_act(0, left)
    fwd[0].start()
    fwd[2].start()
    await_act(1, right)
    fwd[1].start()
    fwd[3].start()
    both_ways(OL, 6, o_r, 0, 8)
    unpack(x)
    onward(WL, 4, w_r, 1, 4)
    onward(OL, 6, o_r, 0, 4)
    arrived(WL.at[pl.ds(0, 8)], w_r, 16)
    unpack(xl)
    unpack(xr)
    arrived(WL.at[pl.ds(0, 8)], w_r, 17)
    unpack(xo)

    scale = 1.0 / HEAD_DIM**0.5
    row = lax.broadcasted_iota(jnp.int32, (ROWS, 128), 0)
    col_ = lax.broadcasted_iota(jnp.int32, (ROWS, 128), 1)
    inside = row // FRAMES == col_ // FRAMES
    lane256 = lax.broadcasted_iota(jnp.int32, (ROWS, 256), 1)
    first = lane256 < HEAD_DIM
    zero = jnp.zeros((ROWS, 256), BF)

    def two_heads(v):
        return jnp.concatenate([jnp.where(first, v, zero), jnp.where(first, zero, v)], axis=0)

    def chunk(ids):
        qkv = dot_nn(jnp.concatenate([XA[i] for i in ids], axis=0), WCAT[...]).astype(BF)
        da = dot_nt(jnp.concatenate([DA[i] for i in ids], axis=0), WOC[...]).astype(BF)
        for h in range(2 * len(ids)):
            i, rs, at = ids[h // 2], pl.ds(h % 2 * ROWS, ROWS), slice(h * ROWS, h * ROWS + ROWS)
            q, k, v, g = qkv[at, :256], qkv[at, 256:512], qkv[at, 512:], da[at]
            kk, vv = two_heads(k), two_heads(v)
            sc = dot_nt(kk, q) * scale
            dp = dot_nt(vv, g)
            probs, dscore = [], []
            for n2 in range(2):
                cs = slice(n2 * 128, n2 * 128 + 128)
                s1 = jnp.where(inside, sc[cs], -jnp.inf)
                e = jnp.exp(s1 - jnp.max(s1, axis=0, keepdims=True))
                p1 = e * (1.0 / jnp.sum(e, axis=0, keepdims=True))
                d1 = dp[cs]
                t1 = jnp.sum(d1 * p1, axis=0, keepdims=True)
                probs.append(p1.astype(BF))
                dscore.append((p1 * (d1 - t1) * scale).astype(BF))
            pb = jnp.concatenate(probs, axis=0)
            ds = jnp.concatenate(dscore, axis=0)
            AS[i, rs, :] = dot_tn(pb, vv).astype(BF)
            DQKV[i, rs, :256] = dot_tn(ds, kk).astype(BF)
            dk = dot_nn(ds, q)
            DQKV[i, rs, 256:512] = jnp.where(first, dk[:128], dk[128:]).astype(BF)
            dv = dot_nn(pb, g)
            DQKV[i, rs, 512:] = jnp.where(first, dv[:128], dv[128:]).astype(BF)

    await_act(1, left)
    fwd[4].start()
    await_act(0, right)
    fwd[5].start()
    rest(OL, o_r)

    def oslot(q, r):
        xs = 2 * c + q // 2
        other = (xs + 3) % NX if q // 2 == 0 else (xs + 1) % NX
        xh = jnp.where(c == r % 2, xs, other)
        return (2 * y + 2 - r // 2 + 4) % ZH, xh, q % 2

    def opix(q, r):
        zs, xh, cs = oslot(q, r)
        return (zs * NX + xh) * NC + cs

    WOC[COLS:, :] = jnp.zeros((256 - COLS, D), BF)
    lane12 = lanes(12)
    for q in range(4):
        parts = [None] * 3
        for r in range(NREP):
            WOC[RP * q : RP * q + RP, 128 * r : 128 * r + 128] = OL[opix(q, r), :RP, :]
            tl = OL[opix(q, r), RP : RP + 12, :].astype(F32)
            for t in range(3):
                v = jnp.where(lane12 // 16 == t, tl, 0.0)
                v = roll(v, 16 * (r - t))
                parts[t] = v if parts[t] is None else parts[t] + v
        for t in range(3):
            at = RP * q + 12 * t
            WOC[at : at + 12, 1024:1152] = parts[t].astype(BF)

    def dx_sib(i):
        return rcopy(
            DXP.at[i, pl.ds(pl.multiple_of(sib * ROWS, ROWS), ROWS)], DXS.at[i],
            sent.at[8], dx_r.at[i], (zh, x, sib, y, zl),
        )

    @pl.loop(0, NY)
    def _(n):
        off = jnp.where(n == 1, 3, jnp.where(n == 2, 1, jnp.where(n == 3, 2, 0)))
        i = (y + off) % NY

        @pl.when(n == 1)
        def _():
            await_act(0, opp)
            fwd[6].start()
            await_act(1, opp)
            fwd[7].start()

        await_sib(i)
        chunk((i,))

    OGRP, first_k = 4, (lambda h, side: 4 * side if h == 4 else 2 * h + side)
    bufs = lambda h: (DWO, OXA, OSM, ORL, ORR, O2S) if h == OGRP else (DWS, RXA, SMB, RL, RR, R2S)

    def some(h, side):
        return pl.ds(first_k(h, side), 4 if h == OGRP else 1)

    def to_x(src, dst, rs, h, side):
        return rcopy(src, dst, sent.at[9 + (h == OGRP)], rs, (zh, (xr, xl)[side], c, y, zl))

    def far(h, side):
        ks = some(h, side)
        return to_x(bufs(h)[0].at[xo, ks], bufs(h)[1].at[ks], far_r.at[h * 2 + side], h, side)

    def near(h, side):
        ks = some(h, 1 - side)
        return to_x(bufs(h)[0].at[(xr, xl)[side], ks], bufs(h)[3 + side].at[ks], near_r.at[h], h, side)

    def summed(h, side):
        ks = some(h, side)
        return to_x(bufs(h)[2].at[ks], bufs(h)[3 + side].at[ks], near_r.at[h], h, side)

    def start_both(f, h):
        for side in range(2):
            f(h, side).start()

    def add_far(h):
        own_, got, out = bufs(h)[:3]
        for side in range(2):
            far(h, side).wait_recv()
            for k in range(first_k(h, side), first_k(h, side) + (4 if h == OGRP else 1)):
                out[k] = (own_[(xr, xl)[side], k].astype(F32) + got[k].astype(F32)).astype(BF)
            summed(h, side).start()

    kown = zh * 2 + c

    def r2(h, k):
        src, dst, o = (O2S, OZ, 1) if h == OGRP else (R2S, RZ, 0)
        return rcopy(src.at[k], dst.at[z], sent.at[11 + o], z_r.at[o], (k // 2, x, k % 2, y, c))

    def k_not_self(k):
        return jnp.logical_not((k == kown) & selfcore)

    def send_z(h):
        arrived(DWO.at[pl.ds(0, 2)] if h == OGRP else RL.at[pl.ds(0, 4)], near_r, h)
        own_, _, _, fl, fr, out = bufs(h)
        for side in range(2):
            for k in range(first_k(h, side), first_k(h, side) + (4 if h == OGRP else 1)):
                t = own_[x, k].astype(F32) + fl[k].astype(F32) + fr[k].astype(F32)
                out[k] = t.astype(BF)

                @pl.when(k_not_self(k))
                def _():
                    r2(h, k).start()

    def z_sum(h, buf, src):
        @pl.when(selfcore)
        def _():
            buf[z] = src[kown]

        @pl.when(selfcore)
        def _():
            arrived(buf.at[pl.ds(0, 7)], z_r, h // 4)

        @pl.when(jnp.logical_not(selfcore))
        def _():
            arrived(buf, z_r, h // 4)

        t = buf[0].astype(F32)
        for i in range(1, NZ):
            t = t + buf[i].astype(F32)
        return t.astype(BF)

    attended = AS[...].reshape(NY * 256, 256)[:, :COLS]
    DWOB[...] = dot_tn(attended, DA[...].reshape(NY * 256, D)).astype(BF)
    for q in range(4):
        tt = [DWOB[RP * q + 12 * t : RP * q + 12 * t + 12, 1024:1152].astype(F32) for t in range(3)]
        for r in range(NREP):
            zs, x2, cs = oslot(q, r)
            k = zs * 2 + cs
            DWO[x2, k, :RP, :] = DWOB[RP * q : RP * q + RP, 128 * r : 128 * r + 128]
            tail = None
            for t in range(3):
                v = roll(jnp.where(lane12 // 16 == r, tt[t], 0.0), 16 * (t - r))
                tail = v if tail is None else tail + v
            DWO[x2, k, RP:RO, :] = tail.astype(BF)
    start_both(far, OGRP)
    start_both(near, OGRP)

    dq_all = DQKV[...].reshape(NY * 256, 768)

    def dw_tile(i):
        lhs = XA[:, :, 128 * i : 128 * i + 128].reshape(NY * 256, 128)
        DWB[128 * i : 128 * i + 128, :] = dot_tn(lhs, dq_all).astype(BF)

    def pack(g):
        for q in range(4):
            p = g * 4 + q
            x2, k = (p // 2) % NX, (p // 8) * 2 + p % 2
            base = RP * p
            tail = None
            for s in range(3):
                DWS[x2, k, RP * s : RP * s + RP, :] = DWB[base : base + RP, 256 * s : 256 * s + 128]
                t = DWB[base : base + RP, 256 * s + 128 : 256 * s + 256].astype(F32)
                t = roll(t[: RP // 2], 32 * s) + roll(t[RP // 2 :], 32 * s + 16)
                tail = t if tail is None else tail + t
            DWS[x2, k, 3 * RP : 3 * RP + RP // 2, :] = tail.astype(BF)

    def own_sum(i):
        half = pl.ds(pl.multiple_of(c * ROWS, ROWS), ROWS)
        return DXP[i, half, :].astype(F32) + DXS[i].astype(F32)

    def dx_far(side):
        rows = pl.ds(64 * side, 64)
        return rcopy(
            DXC.at[0, rows], DXH.at[side], sent.at[13], xh_r.at[side],
            (zh, x, c, (right, left)[side], zl),
        )

    def dx_near(side, late):
        at = 64 * side if late else 64 - 64 * side
        i = (right, left)[side]
        t = own_sum(i)[at : at + 64]
        if late:
            t = t + DXH[side].astype(F32)
        DXC[1 + side, at : at + 64, :] = t.astype(BF)
        rows = pl.ds(at, 64)
        rcopy(
            DXC.at[1 + side, rows], DXR.at[side, rows], sent.at[14], dx_r.at[4], (zh, x, c, i, zl)
        ).start()

    def dx_mat(i):
        DXP[i] = dot_nt(DQKV[i], WCAT[...]).astype(BF)
        dx_sib(i).start()

    for i in range(3):
        dw_tile(i)
    for g in range(2):
        pack(g)
    start_both(far, 0)
    start_both(near, 0)
    for i in range(3, 5):
        dw_tile(i)
    for g in range(2, 4):
        pack(g)
    start_both(far, 1)
    dx_mat(opp)
    for i in range(5, 9):
        dw_tile(i)
    for g in range(4, 8):
        pack(g)
    start_both(far, 2)
    add_far(OGRP)
    dx_mat(right)
    add_far(0)
    start_both(near, 1)
    dx_mat(left)
    arrived(DXS.at[opp], dx_r, opp)
    DXC[0] = own_sum(opp).astype(BF)
    for side in range(2):
        dx_far(side).start()
    arrived(DXS.at[right], dx_r, right)
    dx_near(0, False)
    add_far(1)
    start_both(far, 3)
    start_both(near, 2)
    send_z(OGRP)
    arrived(DXS.at[left], dx_r, left)
    dx_near(1, False)
    dx_mat(y)
    add_far(2)
    start_both(near, 3)
    send_z(0)
    add_far(3)
    send_z(1)

    head, foot = pl.ds(0, RA), pl.ds(RA, RO)

    def home_copy():
        r = home[3] * ZL + home[4]
        return rcopy(FO, FL.at[r, foot], sent.at[15], t_r.at[0], home)

    def home_arrival():
        return rcopy(FO, FL.at[rep, foot], sent.at[15], t_r.at[0], me)

    def fin(dr, part, o):
        r = (rep + dr) % NREP
        b = FL.at[rep, part]
        return rcopy(b, b, sent.at[16 + o], f_r.at[o], (zh, x, c, r // ZL, r % ZL))

    for side in range(2):
        dx_far(side).wait_recv()
        dx_near(side, True)
    send_z(2)
    send_z(3)
    FO[...] = z_sum(OGRP, OZ, O2S)
    home_copy().start()
    FL[rep, :RA, :] = z_sum(0, RZ, R2S)

    @pl.loop(1, NREP)
    def _(dr):
        fin(dr, head, 0).start()

    home_arrival().wait_recv()

    @pl.loop(1, NREP)
    def _(dr):
        fin(dr, foot, 1).start()

    arrived(DXS.at[y], dx_r, y)
    arrived(DXR, dx_r, 4)
    GI[...] = (own_sum(y) + DXR[0].astype(F32) + DXR[1].astype(F32)).astype(BF)
    gi_out = pltpu.make_async_copy(GI, gi_ref, lsem.at[6])
    gi_out.start()

    def left_from(ref, idx):
        rcopy(ref, ref, sent.at[idx], t_r.at[0], me).wait_send()

    left_from(XA.at[pl.ds(0, 3)], 0)
    left_from(XA.at[pl.ds(0, 3)], 1)
    left_from(XA.at[0], 2)
    hub_copy().wait_send()

    @pl.when(selfcore)
    def _():
        for b, idx in ((WL, 4), (OL, 6), (RZ, 11), (OZ, 12)):
            left_from(b.at[pl.ds(0, 7)], idx)

    @pl.when(jnp.logical_not(selfcore))
    def _():
        for b, idx in ((WL, 4), (OL, 6), (RZ, 11), (OZ, 12)):
            left_from(b.at[pl.ds(0, 8)], idx)

    left_from(WL.at[pl.ds(0, 24)], 5)
    left_from(OL.at[pl.ds(0, 24)], 7)
    left_from(DXS, 8)
    left_from(DWS.at[pl.ds(0, 3)], 9)
    left_from(DWO.at[pl.ds(0, 3)], 10)
    left_from(DXH, 13)
    left_from(DXR, 14)
    home_copy().wait_send()

    for o, part in enumerate((head, foot)):
        b = FL.at[pl.ds(0, 7), part]
        arrived(b, f_r, o)
        left_from(b, 16 + o)

    lane36 = lanes(RP)
    for s in range(3):
        last, lastt = None, None
        for t in range(9):
            if t < 8:
                main = roll(FL[t, RP * s : RP * s + RP, :].astype(F32), 16 * t)
            out = main
            if t > 0:
                prev = jnp.where(lane36 < 16 * (t - 1), last, lastt)
                out = prev if t == 8 else jnp.where(lane36 >= 16 * t, main, prev)
            GW[:, s * D + 128 * t : s * D + 128 * t + 128] = out.astype(GW.dtype)
            if t < 8:
                last = main
                tl = FL[t, 3 * RP : 3 * RP + RP // 2, :].astype(F32)
                halves = [roll(tl, 16 * t - 32 * s - 16 * h) for h in range(2)]
                lastt = jnp.concatenate(halves, axis=0)
    parts = [None] * 3
    for r in range(NREP):
        at = 3 * D + 128 * r
        GW[:, at : at + 128] = FL[r, RA : RA + RP, :].astype(GW.dtype)
        tl = FL[r, RA + RP : RA + RP + 12, :].astype(F32)
        for t in range(3):
            v = roll(jnp.where(lane12 // 16 == t, tl, 0.0), 16 * (r - t))
            parts[t] = v if parts[t] is None else parts[t] + v
    GW[:, 3 * D + 1024 :] = jnp.concatenate(parts, axis=0).astype(GW.dtype)
    gw_out = pltpu.make_async_copy(GW, gw_ref, lsem.at[7])
    gw_out.start()
    gi_out.wait()
    gw_out.wait()


def finish(gi_ref, gw_ref, gi_out, gw_out, GI, GW, GF, sem):
    ins = [pltpu.make_async_copy(gw_ref, GW, sem.at[0]), pltpu.make_async_copy(gi_ref, GI, sem.at[1])]
    outs = [pltpu.make_async_copy(GF, gw_out, sem.at[2]), pltpu.make_async_copy(GI, gi_out, sem.at[3])]
    for i in ins:
        i.start()
    ins[0].wait()
    GF[...] = GW[...].astype(F32)
    outs[0].start()
    ins[1].wait()
    outs[1].start()
    for o in outs:
        o.wait()


def vm(*shape, dtype=BF):
    return pltpu.VMEM(shape, dtype)


def local(tokens, out_grad, wq, wk, wv, wo):
    rows = tokens.reshape(-1, D)
    drows = out_grad.reshape(-1, D)
    dma = lambda n: pltpu.SemaphoreType.DMA((n,))
    hbm = pl.BlockSpec(memory_space=pl.ANY)
    gi, gw = pl.pallas_call(
        kernel,
        out_shape=(
            jax.ShapeDtypeStruct((ROWS, D), BF),
            jax.ShapeDtypeStruct((RP, 4 * D), BF),
        ),
        in_specs=[hbm] * 6,
        out_specs=(hbm, hbm),
        scratch_shapes=[
            vm(NY, 256, D), vm(NY, 256, D), vm(4, RP, D),
            vm(RA, 128), vm(RO, 128), vm(RO, 128), vm(NPIX, RA, 128), vm(NPIX, RO, 128),
            vm(D, 768), vm(256, D), vm(NY, 256, 768), vm(NY, 256, 256),
            vm(NY, 256, D), vm(NY, ROWS, D), vm(3, ROWS, D), vm(2, 64, D), vm(2, ROWS, D),
            vm(D, 768), vm(COLS, D), vm(NX, 8, RA, 128), *[vm(8, RA, 128)] * 5, vm(NZ, RA, 128),
            vm(NX, 8, RO, 128), *[vm(8, RO, 128)] * 5, vm(NZ, RO, 128),
            vm(RO, 128), vm(NREP, RF, 128), vm(ROWS, D), vm(RP, 4 * D),
            dma(8), dma(20), dma(8), dma(4), dma(1), dma(18), dma(18), dma(5), dma(2), dma(10),
            dma(5), dma(2), dma(1), dma(4),
        ],
        compiler_params=pltpu.CompilerParams(
            collective_id=0, has_side_effects=True, vmem_limit_bytes=60 * 2**20
        ),
    )(rows, drows, wq, wk, wv, wo)
    gi, gw = pl.pallas_call(
        finish,
        out_shape=(
            jax.ShapeDtypeStruct((ROWS, D), BF),
            jax.ShapeDtypeStruct((RP, 4 * D), F32),
        ),
        in_specs=[hbm] * 2,
        out_specs=(hbm, hbm),
        scratch_shapes=[vm(ROWS, D), vm(RP, 4 * D), vm(RP, 4 * D, dtype=F32), dma(4)],
        compiler_params=pltpu.CompilerParams(vmem_limit_bytes=63 * 2**20),
    )(gi, gw)
    return gi.reshape(tokens.shape), gw


def solution(mesh):
    torus = Mesh(mesh.devices.reshape(ZH, NX, NC, NY, ZL), AXES)
    act = P(AXES, None, None)
    w = P(("zh", "x", "c"), None)
    return jax.shard_map(
        local,
        mesh=torus,
        in_specs=(act, act, w, w, w, w),
        out_specs=(act, w),
        check_vma=False,
    )
```

```python
import jax
import jax.numpy as jnp
from jax import lax
from jax.experimental import pallas as pl
from jax.experimental.pallas import tpu as pltpu
from jax.sharding import Mesh
from jax.sharding import PartitionSpec as P

D = 1152
FRAMES = 16
HEAD_DIM = 72
ZH, NX, NC, NY, ZL = 4, 4, 2, 4, 2
NZ = ZH * ZL
NPIX = ZH * NX * NC
NREP = NY * ZL
ROWS = 128
RP = D // NPIX
COLS = 2 * HEAD_DIM
RA = 128
RO = 48
RF = RA + RO
BF = jnp.bfloat16
F32 = jnp.float32
AXES = ("zh", "x", "c", "y", "zl")


def dot_nn(a, b):
    return lax.dot_general(a, b, (((1,), (0,)), ((), ())), preferred_element_type=F32)


def dot_nt(a, b):
    return lax.dot_general(a, b, (((1,), (1,)), ((), ())), preferred_element_type=F32)


def dot_tn(a, b):
    return lax.dot_general(a, b, (((0,), (0,)), ((), ())), preferred_element_type=F32)


def roll(v, shift):
    shift = shift % 128
    return v if shift == 0 else pltpu.roll(v, shift, 1)


def lanes(rows):
    return lax.broadcasted_iota(jnp.int32, (rows, 128), 1)


def kernel(
    x_ref, d_ref, wq_ref, wk_ref, wv_ref, wo_ref, gi_ref, gw_ref,
    XA, DA, WIN, WS, OSRC, OH, WL, OL, WCAT, WOC, DQKV, AS, DXP, DXS, DXC, DXH, DXR,
    DWB, DWOB, DWS, RXA, SMB, RL, RR, R2S, RZ, DWO, OXA, OSM, ORL, ORR, O2S, OZ, FO, FL, GI, GW,
    lsem, sent, a_r, s_r, h_r, w_r, o_r, dx_r, xh_r, far_r, near_r, z_r, t_r, f_r,
):
    zh, x, c, y, zl = [lax.axis_index(a) for a in AXES]
    pix = (zh * NX + x) * NC + c
    rep = y * ZL + zl
    z = zh * ZL + zl
    sib = 1 - c
    me = (zh, x, c, y, zl)
    selfcore = zl == c
    right, left, opp = (y + 1) % NY, (y + 3) % NY, (y + 2) % NY
    xr, xl, xo = (x + 1) % NX, (x + 3) % NX, (x + 2) % NX
    pair = jnp.where(x % 2 == 0, (x + 3) % NX, xr)
    hub = ((2 * zh + 2 - y + 4) % ZH, jnp.where(zl == x // 2, x, pair), c, zh, x // 2)
    back = jnp.where(x % 2 == 0, (x + 3) % NX, xr)
    there = x // 2 == zl
    home = (y, jnp.where(there, x, back), c, (2 * y + 2 - zh + 4) % NY, jnp.where(there, zl, 1 - zl))

    def rcopy(src, dst, ss, rs, dev):
        return pltpu.make_async_remote_copy(
            src_ref=src, dst_ref=dst, send_sem=ss, recv_sem=rs,
            device_id=dev, device_id_type=pl.DeviceIdType.MESH,
        )

    def blk(kind, yb, cb):
        return (XA, DA)[kind].at[yb, pl.ds(pl.multiple_of(cb * ROWS, ROWS), ROWS)]

    wins = [
        pltpu.make_async_copy(r, WIN.at[k], lsem.at[2 + k])
        for k, r in enumerate((wq_ref, wk_ref, wv_ref, wo_ref))
    ]
    own = [pltpu.make_async_copy(r, blk(k, y, c), lsem.at[k]) for k, r in enumerate((x_ref, d_ref))]
    for o in own + wins:
        o.start()
    bar = pltpu.get_barrier_semaphore()

    def greet(dev):
        pl.semaphore_signal(bar, inc=1, device_id=dev, device_id_type=pl.DeviceIdType.MESH)

    @pl.loop(0, 16)
    def _(i):
        @pl.when(i != z * 2 + c)
        def _():
            greet((i // 4, x, i % 2, y, (i // 2) % 2))

    for dy in range(1, NY):
        greet((zh, x, c, (y + dy) % NY, zl))
        greet((zh, x, c, (y + dy) % NY, 1 - zl))
    greet((zh, xr, c, y, zl))
    greet((zh, xl, c, y, zl))

    greet(hub)
    greet(home)

    ii = lax.broadcasted_iota(jnp.int32, (256, 256), 0)
    nn = lax.broadcasted_iota(jnp.int32, (256, 256), 1)
    sel = jnp.where((ii == nn + 16 * rep) & (nn < COLS), 1.0, 0.0).astype(BF)
    osel = jnp.where((ii == nn + 16 * rep) & (nn < 16), 1.0, 0.0).astype(BF)[:128, :128]
    win = pl.multiple_of(128 * rep, 128)
    for w in wins:
        w.wait()
    tail = None
    for s in range(3):
        b = dot_nn(WIN[s, :, pl.ds(win, 256)], sel)
        WS[RP * s : RP * s + RP, :] = b[:, :128].astype(BF)
        t = b[:, 128:256]
        t = roll(t[: RP // 2], 32 * s) + roll(t[RP // 2 :], 32 * s + 16)
        tail = t if tail is None else tail + t
    WS[3 * RP : 3 * RP + RP // 2, :] = tail.astype(BF)
    OSRC[:RP, :] = WIN[3, :, pl.ds(win, 128)]
    t = dot_nn(WIN[3, :, 1024:], osel)
    tail = t[:12] + roll(t[12:24], 16) + roll(t[24:36], 32)
    OSRC[RP : RP + 12, :] = tail.astype(BF)
    for o in own:
        o.wait()

    pl.semaphore_wait(bar, 15 + 6 + 2 + 2)

    def act(kind, yb, cb, to_y, to_c, idx):
        rs = s_r.at[yb] if to_c is sib else a_r.at[kind * 4 + yb]
        return rcopy(blk(kind, yb, cb), blk(kind, yb, cb), sent.at[idx // 6], rs, (zh, x, to_c, to_y, zl))

    def hub_copy():
        return rcopy(OSRC, OH, sent.at[3], h_r.at[0], hub)

    sends = [
        act(0, y, c, right, c, 0), act(1, y, c, left, c, 1),
        act(1, y, c, right, c, 2), act(0, y, c, left, c, 3),
        act(0, y, c, y, sib, 4), act(1, y, c, y, sib, 5),
    ]

    hub_copy().start()
    for s in sends[:4]:
        s.start()

    def col(k, xs):
        return ((k // 2) * NX + xs) * NC + k % 2

    def along_z(src, buf, ss, rs, i):
        return rcopy(src, buf.at[pix], sent.at[ss], rs.at[zh * 2 + c], (i // 2, x, zl, y, i % 2))

    def not_self(i):
        return jnp.logical_not((i == z) & selfcore)

    def spread(src, buf, ss, rs):
        @pl.when(selfcore)
        def _():
            buf[pix] = src[...]

        for dz in (1, 7, 2, 6, 3, 5, 4):
            along_z(src, buf, ss, rs, (z + dz) % NZ).start()

        @pl.when(jnp.logical_not(selfcore))
        def _():
            along_z(src, buf, ss, rs, z).start()

    def around_x(buf, ss, rs, p, to, idx):
        return rcopy(buf.at[p], buf.at[p], sent.at[ss + 1], rs.at[idx], (zh, to, c, y, zl))

    def arrived(ref, rs, idx):
        rcopy(ref, ref, sent.at[0], rs.at[idx], me).wait_recv()

    def both_ways(buf, ss, rs, lo, hi):
        @pl.loop(lo, hi)
        def _(n):
            n = jnp.where(n < 4, n, jnp.where(n < 6, n + 2, n - 2))
            k = (2 * zh + n) % 8
            p = col(k, x)

            @pl.when(jnp.logical_not((p == pix) & selfcore))
            def _():
                arrived(buf.at[p], rs, k)

            around_x(buf, ss, rs, p, xr, jnp.where(k % 2 == 0, 8 + k, 16)).start()
            around_x(buf, ss, rs, p, xl, jnp.where(k % 2 == 0, 16, 8 + k)).start()

    def onward(buf, ss, rs, lo, hi):
        @pl.loop(lo, hi)
        def _(n):
            k = 2 * ((zh + jnp.where(n < 2, n, 5 - n)) % ZH)
            p, q = col(k, xl), col(k + 1, xr)
            arrived(buf.at[p], rs, 8 + k)
            around_x(buf, ss, rs, p, xr, 17).start()
            arrived(buf.at[q], rs, 9 + k)
            around_x(buf, ss, rs, q, xl, 17).start()

    def rest(buf, rs):
        arrived(buf.at[pl.ds(0, 8)], rs, 16)
        arrived(buf.at[pl.ds(0, 8)], rs, 17)

    spread(WS, WL, 4, w_r)
    for s in sends[4:]:
        s.start()
    both_ways(WL, 4, w_r, 0, 2)
    hub_copy().wait_recv()
    spread(OH, OL, 6, o_r)
    both_ways(WL, 4, w_r, 2, 6)
    onward(WL, 4, w_r, 0, 1)
    both_ways(WL, 4, w_r, 6, 8)

    low16 = lanes(RP // 2) < 16

    def unpack(xs):
        for x2 in range(NX):
            @pl.when(xs == x2)
            def _():
                @pl.loop(0, ZH)
                def _(zs):
                    out = WCAT.at[pl.ds(pl.multiple_of(zs * 288, 16), 288)]
                    for cs in range(NC):
                        p, base = (zs * NX + x2) * NC + cs, RP * (x2 * NC + cs)
                        tl = WL[p, 3 * RP : 3 * RP + RP // 2, :].astype(F32)
                        for s in range(3):
                            out[base : base + RP, 256 * s : 256 * s + 128] = WL[p, RP * s : RP * s + RP, :]
                            for half in range(2):
                                v = jnp.where(low16, roll(tl, -(32 * s + 16 * half)), 0.0).astype(BF)
                                at = base + half * (RP // 2)
                                out[at : at + RP // 2, 256 * s + 128 : 256 * s + 256] = v

    def await_act(kind, yb):
        rcopy(blk(kind, yb, c), blk(kind, yb, c), sent.at[0], a_r.at[kind * 4 + yb], me).wait_recv()

    def await_sib(yb):
        rcopy(XA.at[yb], XA.at[yb], sent.at[0], s_r.at[yb], me).wait_recv()

    fwd = [
        act(0, left, c, right, c, 6), act(1, right, c, left, c, 7),
        act(0, left, c, y, sib, 8), act(1, right, c, y, sib, 9),
        act(1, left, c, y, sib, 10), act(0, right, c, y, sib, 11),
        act(0, opp, c, y, sib, 12), act(1, opp, c, y, sib, 13),
    ]
    await_act(0, left)
    fwd[0].start()
    fwd[2].start()
    await_act(1, right)
    fwd[1].start()
    fwd[3].start()
    both_ways(OL, 6, o_r, 0, 8)
    unpack(x)
    onward(WL, 4, w_r, 1, 4)
    onward(OL, 6, o_r, 0, 4)
    arrived(WL.at[pl.ds(0, 8)], w_r, 16)
    unpack(xl)
    unpack(xr)
    arrived(WL.at[pl.ds(0, 8)], w_r, 17)
    unpack(xo)

    scale = 1.0 / HEAD_DIM**0.5
    row = lax.broadcasted_iota(jnp.int32, (ROWS, 128), 0)
    col_ = lax.broadcasted_iota(jnp.int32, (ROWS, 128), 1)
    inside = row // FRAMES == col_ // FRAMES
    lane256 = lax.broadcasted_iota(jnp.int32, (ROWS, 256), 1)
    first = lane256 < HEAD_DIM
    zero = jnp.zeros((ROWS, 256), BF)

    def two_heads(v):
        return jnp.concatenate([jnp.where(first, v, zero), jnp.where(first, zero, v)], axis=0)

    def chunk(ids):
        qkv = dot_nn(jnp.concatenate([XA[i] for i in ids], axis=0), WCAT[...]).astype(BF)
        da = dot_nt(jnp.concatenate([DA[i] for i in ids], axis=0), WOC[...]).astype(BF)
        for h in range(2 * len(ids)):
            i, rs, at = ids[h // 2], pl.ds(h % 2 * ROWS, ROWS), slice(h * ROWS, h * ROWS + ROWS)
            q, k, v, g = qkv[at, :256], qkv[at, 256:512], qkv[at, 512:], da[at]
            kk, vv = two_heads(k), two_heads(v)
            sc = dot_nt(kk, q) * scale
            dp = dot_nt(vv, g)
            probs, dscore = [], []
            for n2 in range(2):
                cs = slice(n2 * 128, n2 * 128 + 128)
                s1 = jnp.where(inside, sc[cs], -jnp.inf)
                e = jnp.exp(s1 - jnp.max(s1, axis=0, keepdims=True))
                p1 = e * (1.0 / jnp.sum(e, axis=0, keepdims=True))
                d1 = dp[cs]
                t1 = jnp.sum(d1 * p1, axis=0, keepdims=True)
                probs.append(p1.astype(BF))
                dscore.append((p1 * (d1 - t1) * scale).astype(BF))
            pb = jnp.concatenate(probs, axis=0)
            ds = jnp.concatenate(dscore, axis=0)
            AS[i, rs, :] = dot_tn(pb, vv).astype(BF)
            DQKV[i, rs, :256] = dot_tn(ds, kk).astype(BF)
            dk = dot_nn(ds, q)
            DQKV[i, rs, 256:512] = jnp.where(first, dk[:128], dk[128:]).astype(BF)
            dv = dot_nn(pb, g)
            DQKV[i, rs, 512:] = jnp.where(first, dv[:128], dv[128:]).astype(BF)

    await_act(1, left)
    fwd[4].start()
    await_act(0, right)
    fwd[5].start()
    rest(OL, o_r)

    def oslot(q, r):
        xs = 2 * c + q // 2
        other = (xs + 3) % NX if q // 2 == 0 else (xs + 1) % NX
        xh = jnp.where(c == r % 2, xs, other)
        return (2 * y + 2 - r // 2 + 4) % ZH, xh, q % 2

    def opix(q, r):
        zs, xh, cs = oslot(q, r)
        return (zs * NX + xh) * NC + cs

    WOC[COLS:, :] = jnp.zeros((256 - COLS, D), BF)
    lane12 = lanes(12)
    for q in range(4):
        parts = [None] * 3
        for r in range(NREP):
            WOC[RP * q : RP * q + RP, 128 * r : 128 * r + 128] = OL[opix(q, r), :RP, :]
            tl = OL[opix(q, r), RP : RP + 12, :].astype(F32)
            for t in range(3):
                v = jnp.where(lane12 // 16 == t, tl, 0.0)
                v = roll(v, 16 * (r - t))
                parts[t] = v if parts[t] is None else parts[t] + v
        for t in range(3):
            at = RP * q + 12 * t
            WOC[at : at + 12, 1024:1152] = parts[t].astype(BF)

    def dx_sib(i):
        return rcopy(
            DXP.at[i, pl.ds(pl.multiple_of(sib * ROWS, ROWS), ROWS)], DXS.at[i],
            sent.at[8], dx_r.at[i], (zh, x, sib, y, zl),
        )

    @pl.loop(0, NY)
    def _(n):
        off = jnp.where(n == 1, 3, jnp.where(n == 2, 1, jnp.where(n == 3, 2, 0)))
        i = (y + off) % NY

        @pl.when(n == 1)
        def _():
            await_act(0, opp)
            fwd[6].start()
            await_act(1, opp)
            fwd[7].start()

        await_sib(i)
        chunk((i,))

    OGRP, first_k = 4, (lambda h, side: 4 * side if h == 4 else (0, 1, 4, 5)[h] + 2 * side)
    bufs = lambda h: (DWO, OXA, OSM, ORL, ORR, O2S) if h == OGRP else (DWS, RXA, SMB, RL, RR, R2S)

    def some(h, side):
        return pl.ds(first_k(h, side), 4 if h == OGRP else 1)

    def to_x(src, dst, rs, h, side):
        return rcopy(src, dst, sent.at[9 + (h == OGRP)], rs, (zh, (xr, xl)[side], c, y, zl))

    def far(h, side):
        ks = some(h, side)
        return to_x(bufs(h)[0].at[xo, ks], bufs(h)[1].at[ks], far_r.at[h * 2 + side], h, side)

    def near(h, side):
        ks = some(h, 1 - side)
        return to_x(bufs(h)[0].at[(xr, xl)[side], ks], bufs(h)[3 + side].at[ks], near_r.at[h], h, side)

    def summed(h, side):
        ks = some(h, side)
        return to_x(bufs(h)[2].at[ks], bufs(h)[3 + side].at[ks], near_r.at[h], h, side)

    def start_both(f, h):
        for side in range(2):
            f(h, side).start()

    def add_far(h):
        own_, got, out = bufs(h)[:3]
        for side in range(2):
            far(h, side).wait_recv()
            for k in range(first_k(h, side), first_k(h, side) + (4 if h == OGRP else 1)):
                out[k] = (own_[(xr, xl)[side], k].astype(F32) + got[k].astype(F32)).astype(BF)
            summed(h, side).start()

    kown = zh * 2 + c

    def r2(h, k):
        src, dst, o = (O2S, OZ, 1) if h == OGRP else (R2S, RZ, 0)
        return rcopy(src.at[k], dst.at[z], sent.at[11 + o], z_r.at[o], (k // 2, x, k % 2, y, c))

    def k_not_self(k):
        return jnp.logical_not((k == kown) & selfcore)

    def send_z(h):
        arrived(DWO.at[pl.ds(0, 2)] if h == OGRP else RL.at[pl.ds(0, 4)], near_r, h)
        own_, _, _, fl, fr, out = bufs(h)
        for side in range(2):
            for k in range(first_k(h, side), first_k(h, side) + (4 if h == OGRP else 1)):
                t = own_[x, k].astype(F32) + fl[k].astype(F32) + fr[k].astype(F32)
                out[k] = t.astype(BF)

                @pl.when(k_not_self(k))
                def _():
                    r2(h, k).start()

    def z_sum(h, buf, src):
        @pl.when(selfcore)
        def _():
            buf[z] = src[kown]

        @pl.when(selfcore)
        def _():
            arrived(buf.at[pl.ds(0, 7)], z_r, h // 4)

        @pl.when(jnp.logical_not(selfcore))
        def _():
            arrived(buf, z_r, h // 4)

        t = buf[0].astype(F32)
        for i in range(1, NZ):
            t = t + buf[i].astype(F32)
        return t.astype(BF)

    attended = AS[...].reshape(NY * 256, 256)[:, :COLS]
    DWOB[...] = dot_tn(attended, DA[...].reshape(NY * 256, D)).astype(BF)
    for q in range(4):
        tt = [DWOB[RP * q + 12 * t : RP * q + 12 * t + 12, 1024:1152].astype(F32) for t in range(3)]
        for r in range(NREP):
            zs, x2, cs = oslot(q, r)
            k = zs * 2 + cs
            DWO[x2, k, :RP, :] = DWOB[RP * q : RP * q + RP, 128 * r : 128 * r + 128]
            tail = None
            for t in range(3):
                v = roll(jnp.where(lane12 // 16 == r, tt[t], 0.0), 16 * (t - r))
                tail = v if tail is None else tail + v
            DWO[x2, k, RP:RO, :] = tail.astype(BF)
    start_both(far, OGRP)
    start_both(near, OGRP)

    dq_all = DQKV[...].reshape(NY * 256, 768)

    def dw_tile(i):
        lhs = XA[:, :, 128 * i : 128 * i + 128].reshape(NY * 256, 128)
        DWB[128 * i : 128 * i + 128, :] = dot_tn(lhs, dq_all).astype(BF)

    def pack(g):
        for q in range(4):
            p = g * 4 + q
            x2, k = (p // 2) % NX, (p // 8) * 2 + p % 2
            base = RP * p
            tail = None
            for s in range(3):
                DWS[x2, k, RP * s : RP * s + RP, :] = DWB[base : base + RP, 256 * s : 256 * s + 128]
                t = DWB[base : base + RP, 256 * s + 128 : 256 * s + 256].astype(F32)
                t = roll(t[: RP // 2], 32 * s) + roll(t[RP // 2 :], 32 * s + 16)
                tail = t if tail is None else tail + t
            DWS[x2, k, 3 * RP : 3 * RP + RP // 2, :] = tail.astype(BF)

    def own_sum(i):
        half = pl.ds(pl.multiple_of(c * ROWS, ROWS), ROWS)
        return DXP[i, half, :].astype(F32) + DXS[i].astype(F32)

    def dx_far(side):
        rows = pl.ds(64 * side, 64)
        return rcopy(
            DXC.at[0, rows], DXH.at[side], sent.at[13], xh_r.at[side],
            (zh, x, c, (right, left)[side], zl),
        )

    def dx_near(side, late):
        at = 64 * side if late else 64 - 64 * side
        i = (right, left)[side]
        t = own_sum(i)[at : at + 64]
        if late:
            t = t + DXH[side].astype(F32)
        DXC[1 + side, at : at + 64, :] = t.astype(BF)
        rows = pl.ds(at, 64)
        rcopy(
            DXC.at[1 + side, rows], DXR.at[side, rows], sent.at[14], dx_r.at[4], (zh, x, c, i, zl)
        ).start()

    def dx_mat(i):
        DXP[i] = dot_nt(DQKV[i], WCAT[...]).astype(BF)
        dx_sib(i).start()

    for i in range(5):
        dw_tile(i)
    for g in range(4):
        pack(g)
    start_both(far, 0)
    start_both(near, 0)
    start_both(far, 1)
    dx_mat(opp)
    for i in range(5, 9):
        dw_tile(i)
    for g in range(4, 8):
        pack(g)
    start_both(far, 2)
    add_far(OGRP)
    dx_mat(right)
    add_far(0)
    start_both(near, 1)
    dx_mat(left)
    arrived(DXS.at[opp], dx_r, opp)
    DXC[0] = own_sum(opp).astype(BF)
    for side in range(2):
        dx_far(side).start()
    arrived(DXS.at[right], dx_r, right)
    dx_near(0, False)
    add_far(1)
    start_both(far, 3)
    start_both(near, 2)
    arrived(DXS.at[left], dx_r, left)
    dx_near(1, False)
    send_z(OGRP)
    dx_mat(y)
    add_far(2)
    start_both(near, 3)
    send_z(0)
    add_far(3)
    send_z(1)

    head, foot = pl.ds(0, RA), pl.ds(RA, RO)

    def home_copy():
        r = home[3] * ZL + home[4]
        return rcopy(FO, FL.at[r, foot], sent.at[15], t_r.at[0], home)

    def home_arrival():
        return rcopy(FO, FL.at[rep, foot], sent.at[15], t_r.at[0], me)

    def fin(dr, part, o):
        r = (rep + dr) % NREP
        b = FL.at[rep, part]
        return rcopy(b, b, sent.at[16 + o], f_r.at[o], (zh, x, c, r // ZL, r % ZL))

    send_z(2)
    send_z(3)
    FO[...] = z_sum(OGRP, OZ, O2S)
    home_copy().start()
    for side in range(2):
        dx_far(side).wait_recv()
        dx_near(side, True)
    FL[rep, :RA, :] = z_sum(0, RZ, R2S)

    @pl.loop(1, NREP)
    def _(dr):
        fin(dr, head, 0).start()

    home_arrival().wait_recv()

    @pl.loop(1, NREP)
    def _(dr):
        fin(dr, foot, 1).start()

    arrived(DXS.at[y], dx_r, y)
    arrived(DXR, dx_r, 4)
    GI[...] = (own_sum(y) + DXR[0].astype(F32) + DXR[1].astype(F32)).astype(BF)
    gi_out = pltpu.make_async_copy(GI, gi_ref, lsem.at[6])
    gi_out.start()

    def left_from(ref, idx):
        rcopy(ref, ref, sent.at[idx], t_r.at[0], me).wait_send()

    left_from(XA.at[pl.ds(0, 3)], 0)
    left_from(XA.at[pl.ds(0, 3)], 1)
    left_from(XA.at[0], 2)
    hub_copy().wait_send()

    @pl.when(selfcore)
    def _():
        for b, idx in ((WL, 4), (OL, 6), (RZ, 11), (OZ, 12)):
            left_from(b.at[pl.ds(0, 7)], idx)

    @pl.when(jnp.logical_not(selfcore))
    def _():
        for b, idx in ((WL, 4), (OL, 6), (RZ, 11), (OZ, 12)):
            left_from(b.at[pl.ds(0, 8)], idx)

    left_from(WL.at[pl.ds(0, 24)], 5)
    left_from(OL.at[pl.ds(0, 24)], 7)
    left_from(DXS, 8)
    left_from(DWS.at[pl.ds(0, 3)], 9)
    left_from(DWO.at[pl.ds(0, 3)], 10)
    left_from(DXH, 13)
    left_from(DXR, 14)
    home_copy().wait_send()

    for o, part in enumerate((head, foot)):
        b = FL.at[pl.ds(0, 7), part]
        arrived(b, f_r, o)
        left_from(b, 16 + o)

    lane36 = lanes(RP)
    for s in range(3):
        last, lastt = None, None
        for t in range(9):
            if t < 8:
                main = roll(FL[t, RP * s : RP * s + RP, :].astype(F32), 16 * t)
            out = main
            if t > 0:
                prev = jnp.where(lane36 < 16 * (t - 1), last, lastt)
                out = prev if t == 8 else jnp.where(lane36 >= 16 * t, main, prev)
            GW[:, s * D + 128 * t : s * D + 128 * t + 128] = out.astype(GW.dtype)
            if t < 8:
                last = main
                tl = FL[t, 3 * RP : 3 * RP + RP // 2, :].astype(F32)
                halves = [roll(tl, 16 * t - 32 * s - 16 * h) for h in range(2)]
                lastt = jnp.concatenate(halves, axis=0)
    parts = [None] * 3
    for r in range(NREP):
        at = 3 * D + 128 * r
        GW[:, at : at + 128] = FL[r, RA : RA + RP, :].astype(GW.dtype)
        tl = FL[r, RA + RP : RA + RP + 12, :].astype(F32)
        for t in range(3):
            v = roll(jnp.where(lane12 // 16 == t, tl, 0.0), 16 * (r - t))
            parts[t] = v if parts[t] is None else parts[t] + v
    GW[:, 3 * D + 1024 :] = jnp.concatenate(parts, axis=0).astype(GW.dtype)
    gw_out = pltpu.make_async_copy(GW, gw_ref, lsem.at[7])
    gw_out.start()
    gi_out.wait()
    gw_out.wait()


def finish(gi_ref, gw_ref, gi_out, gw_out, GI, GW, GF, sem):
    ins = [pltpu.make_async_copy(gw_ref, GW, sem.at[0]), pltpu.make_async_copy(gi_ref, GI, sem.at[1])]
    outs = [pltpu.make_async_copy(GF, gw_out, sem.at[2]), pltpu.make_async_copy(GI, gi_out, sem.at[3])]
    for i in ins:
        i.start()
    ins[0].wait()
    GF[...] = GW[...].astype(F32)
    outs[0].start()
    ins[1].wait()
    outs[1].start()
    for o in outs:
        o.wait()


def vm(*shape, dtype=BF):
    return pltpu.VMEM(shape, dtype)


def local(tokens, out_grad, wq, wk, wv, wo):
    rows = tokens.reshape(-1, D)
    drows = out_grad.reshape(-1, D)
    dma = lambda n: pltpu.SemaphoreType.DMA((n,))
    hbm = pl.BlockSpec(memory_space=pl.ANY)
    gi, gw = pl.pallas_call(
        kernel,
        out_shape=(
            jax.ShapeDtypeStruct((ROWS, D), BF),
            jax.ShapeDtypeStruct((RP, 4 * D), BF),
        ),
        in_specs=[hbm] * 6,
        out_specs=(hbm, hbm),
        scratch_shapes=[
            vm(NY, 256, D), vm(NY, 256, D), vm(4, RP, D),
            vm(RA, 128), vm(RO, 128), vm(RO, 128), vm(NPIX, RA, 128), vm(NPIX, RO, 128),
            vm(D, 768), vm(256, D), vm(NY, 256, 768), vm(NY, 256, 256),
            vm(NY, 256, D), vm(NY, ROWS, D), vm(3, ROWS, D), vm(2, 64, D), vm(2, ROWS, D),
            vm(D, 768), vm(COLS, D), vm(NX, 8, RA, 128), *[vm(8, RA, 128)] * 5, vm(NZ, RA, 128),
            vm(NX, 8, RO, 128), *[vm(8, RO, 128)] * 5, vm(NZ, RO, 128),
            vm(RO, 128), vm(NREP, RF, 128), vm(ROWS, D), vm(RP, 4 * D),
            dma(8), dma(20), dma(8), dma(4), dma(1), dma(18), dma(18), dma(5), dma(2), dma(10),
            dma(5), dma(2), dma(1), dma(4),
        ],
        compiler_params=pltpu.CompilerParams(
            collective_id=0, has_side_effects=True, vmem_limit_bytes=60 * 2**20
        ),
    )(rows, drows, wq, wk, wv, wo)
    gi, gw = pl.pallas_call(
        finish,
        out_shape=(
            jax.ShapeDtypeStruct((ROWS, D), BF),
            jax.ShapeDtypeStruct((RP, 4 * D), F32),
        ),
        in_specs=[hbm] * 2,
        out_specs=(hbm, hbm),
        scratch_shapes=[vm(ROWS, D), vm(RP, 4 * D), vm(RP, 4 * D, dtype=F32), dma(4)],
        compiler_params=pltpu.CompilerParams(vmem_limit_bytes=63 * 2**20),
    )(gi, gw)
    return gi.reshape(tokens.shape), gw


def solution(mesh):
    torus = Mesh(mesh.devices.reshape(ZH, NX, NC, NY, ZL), AXES)
    act = P(AXES, None, None)
    w = P(("zh", "x", "c"), None)
    return jax.shard_map(
        local,
        mesh=torus,
        in_specs=(act, act, w, w, w, w),
        out_specs=(act, w),
        check_vma=False,
    )
```

```python
import jax
import jax.numpy as jnp
from jax import lax
from jax.experimental import pallas as pl
from jax.experimental.pallas import tpu as pltpu
from jax.sharding import Mesh
from jax.sharding import PartitionSpec as P

D = 1152
FRAMES = 16
HEAD_DIM = 72
ZH, NX, NC, NY, ZL = 4, 4, 2, 4, 2
NZ = ZH * ZL
NPIX = ZH * NX * NC
NREP = NY * ZL
ROWS = 128
RP = D // NPIX
COLS = 2 * HEAD_DIM
RA = 128
RO = 48
RF = RA + RO
BF = jnp.bfloat16
F32 = jnp.float32
AXES = ("zh", "x", "c", "y", "zl")


def dot_nn(a, b):
    return lax.dot_general(a, b, (((1,), (0,)), ((), ())), preferred_element_type=F32)


def dot_nt(a, b):
    return lax.dot_general(a, b, (((1,), (1,)), ((), ())), preferred_element_type=F32)


def dot_tn(a, b):
    return lax.dot_general(a, b, (((0,), (0,)), ((), ())), preferred_element_type=F32)


def roll(v, shift):
    shift = shift % 128
    return v if shift == 0 else pltpu.roll(v, shift, 1)


def lanes(rows):
    return lax.broadcasted_iota(jnp.int32, (rows, 128), 1)


def kernel(
    x_ref, d_ref, wq_ref, wk_ref, wv_ref, wo_ref, gi_ref, gw_ref,
    XA, DA, WIN, WS, OSRC, OH, WL, OL, WCAT, WOC, DQKV, AS, DXP, DXS, DXC, DXH, DXR,
    DWB, DWOB, DWS, RXA, SMB, RL, RR, R2S, RZ, DWO, OXA, OSM, ORL, ORR, O2S, OZ, FO, FL, GI, GW,
    lsem, sent, a_r, s_r, h_r, w_r, o_r, dx_r, xh_r, far_r, near_r, z_r, t_r, f_r,
):
    zh, x, c, y, zl = [lax.axis_index(a) for a in AXES]
    pix = (zh * NX + x) * NC + c
    rep = y * ZL + zl
    z = zh * ZL + zl
    sib = 1 - c
    me = (zh, x, c, y, zl)
    selfcore = zl == c
    right, left, opp = (y + 1) % NY, (y + 3) % NY, (y + 2) % NY
    xr, xl, xo = (x + 1) % NX, (x + 3) % NX, (x + 2) % NX
    pair = jnp.where(x % 2 == 0, (x + 3) % NX, xr)
    hub = ((2 * zh + 2 - y + 4) % ZH, jnp.where(zl == x // 2, x, pair), c, zh, x // 2)
    back = jnp.where(x % 2 == 0, (x + 3) % NX, xr)
    there = x // 2 == zl
    home = (y, jnp.where(there, x, back), c, (2 * y + 2 - zh + 4) % NY, jnp.where(there, zl, 1 - zl))

    def rcopy(src, dst, ss, rs, dev):
        return pltpu.make_async_remote_copy(
            src_ref=src, dst_ref=dst, send_sem=ss, recv_sem=rs,
            device_id=dev, device_id_type=pl.DeviceIdType.MESH,
        )

    def blk(kind, yb, cb):
        return (XA, DA)[kind].at[yb, pl.ds(pl.multiple_of(cb * ROWS, ROWS), ROWS)]

    wins = [
        pltpu.make_async_copy(r, WIN.at[k], lsem.at[2 + k])
        for k, r in enumerate((wq_ref, wk_ref, wv_ref, wo_ref))
    ]
    own = [pltpu.make_async_copy(r, blk(k, y, c), lsem.at[k]) for k, r in enumerate((x_ref, d_ref))]
    for o in own + wins:
        o.start()
    bar = pltpu.get_barrier_semaphore()

    def greet(dev):
        pl.semaphore_signal(bar, inc=1, device_id=dev, device_id_type=pl.DeviceIdType.MESH)

    @pl.loop(0, 16)
    def _(i):
        @pl.when(i != z * 2 + c)
        def _():
            greet((i // 4, x, i % 2, y, (i // 2) % 2))

    for dy in range(1, NY):
        greet((zh, x, c, (y + dy) % NY, zl))
        greet((zh, x, c, (y + dy) % NY, 1 - zl))
    greet((zh, xr, c, y, zl))
    greet((zh, xl, c, y, zl))

    greet(hub)
    greet(home)

    ii = lax.broadcasted_iota(jnp.int32, (256, 256), 0)
    nn = lax.broadcasted_iota(jnp.int32, (256, 256), 1)
    sel = jnp.where((ii == nn + 16 * rep) & (nn < COLS), 1.0, 0.0).astype(BF)
    osel = jnp.where((ii == nn + 16 * rep) & (nn < 16), 1.0, 0.0).astype(BF)[:128, :128]
    win = pl.multiple_of(128 * rep, 128)
    for w in wins:
        w.wait()
    tail = None
    for s in range(3):
        b = dot_nn(WIN[s, :, pl.ds(win, 256)], sel)
        WS[RP * s : RP * s + RP, :] = b[:, :128].astype(BF)
        t = b[:, 128:256]
        t = roll(t[: RP // 2], 32 * s) + roll(t[RP // 2 :], 32 * s + 16)
        tail = t if tail is None else tail + t
    WS[3 * RP : 3 * RP + RP // 2, :] = tail.astype(BF)
    OSRC[:RP, :] = WIN[3, :, pl.ds(win, 128)]
    t = dot_nn(WIN[3, :, 1024:], osel)
    tail = t[:12] + roll(t[12:24], 16) + roll(t[24:36], 32)
    OSRC[RP : RP + 12, :] = tail.astype(BF)
    for o in own:
        o.wait()

    pl.semaphore_wait(bar, 15 + 6 + 2 + 2)

    def act(kind, yb, cb, to_y, to_c, idx):
        rs = s_r.at[yb] if to_c is sib else a_r.at[kind * 4 + yb]
        return rcopy(blk(kind, yb, cb), blk(kind, yb, cb), sent.at[idx // 6], rs, (zh, x, to_c, to_y, zl))

    def hub_copy():
        return rcopy(OSRC, OH, sent.at[3], h_r.at[0], hub)

    sends = [
        act(0, y, c, right, c, 0), act(1, y, c, left, c, 1),
        act(1, y, c, right, c, 2), act(0, y, c, left, c, 3),
        act(0, y, c, y, sib, 4), act(1, y, c, y, sib, 5),
    ]

    hub_copy().start()
    for s in sends[:4]:
        s.start()

    def col(k, xs):
        return ((k // 2) * NX + xs) * NC + k % 2

    def along_z(src, buf, ss, rs, i):
        return rcopy(src, buf.at[pix], sent.at[ss], rs.at[zh * 2 + c], (i // 2, x, zl, y, i % 2))

    def not_self(i):
        return jnp.logical_not((i == z) & selfcore)

    def spread(src, buf, ss, rs):
        @pl.when(selfcore)
        def _():
            buf[pix] = src[...]

        for dz in (1, 7, 2, 6, 3, 5, 4):
            along_z(src, buf, ss, rs, (z + dz) % NZ).start()

        @pl.when(jnp.logical_not(selfcore))
        def _():
            along_z(src, buf, ss, rs, z).start()

    def around_x(buf, ss, rs, p, to, idx):
        return rcopy(buf.at[p], buf.at[p], sent.at[ss + 1], rs.at[idx], (zh, to, c, y, zl))

    def arrived(ref, rs, idx):
        rcopy(ref, ref, sent.at[0], rs.at[idx], me).wait_recv()

    def both_ways(buf, ss, rs, lo, hi):
        @pl.loop(lo, hi)
        def _(n):
            n = jnp.where(n < 4, n, jnp.where(n < 6, n + 2, n - 2))
            k = (2 * zh + n) % 8
            p = col(k, x)

            @pl.when(jnp.logical_not((p == pix) & selfcore))
            def _():
                arrived(buf.at[p], rs, k)

            around_x(buf, ss, rs, p, xr, jnp.where(k % 2 == 0, 8 + k, 16)).start()
            around_x(buf, ss, rs, p, xl, jnp.where(k % 2 == 0, 16, 8 + k)).start()

    def onward(buf, ss, rs, lo, hi):
        @pl.loop(lo, hi)
        def _(n):
            k = 2 * ((zh + jnp.where(n < 2, n, 5 - n)) % ZH)
            p, q = col(k, xl), col(k + 1, xr)
            arrived(buf.at[p], rs, 8 + k)
            around_x(buf, ss, rs, p, xr, 17).start()
            arrived(buf.at[q], rs, 9 + k)
            around_x(buf, ss, rs, q, xl, 17).start()

    def rest(buf, rs):
        arrived(buf.at[pl.ds(0, 8)], rs, 16)
        arrived(buf.at[pl.ds(0, 8)], rs, 17)

    spread(WS, WL, 4, w_r)
    for s in sends[4:]:
        s.start()
    both_ways(WL, 4, w_r, 0, 2)
    hub_copy().wait_recv()
    spread(OH, OL, 6, o_r)
    both_ways(WL, 4, w_r, 2, 6)
    onward(WL, 4, w_r, 0, 1)
    both_ways(WL, 4, w_r, 6, 8)

    low16 = lanes(RP // 2) < 16

    def unpack(xs):
        for x2 in range(NX):
            @pl.when(xs == x2)
            def _():
                @pl.loop(0, ZH)
                def _(zs):
                    out = WCAT.at[pl.ds(pl.multiple_of(zs * 288, 16), 288)]
                    for cs in range(NC):
                        p, base = (zs * NX + x2) * NC + cs, RP * (x2 * NC + cs)
                        tl = WL[p, 3 * RP : 3 * RP + RP // 2, :].astype(F32)
                        for s in range(3):
                            out[base : base + RP, 256 * s : 256 * s + 128] = WL[p, RP * s : RP * s + RP, :]
                            for half in range(2):
                                v = jnp.where(low16, roll(tl, -(32 * s + 16 * half)), 0.0).astype(BF)
                                at = base + half * (RP // 2)
                                out[at : at + RP // 2, 256 * s + 128 : 256 * s + 256] = v

    def await_act(kind, yb):
        rcopy(blk(kind, yb, c), blk(kind, yb, c), sent.at[0], a_r.at[kind * 4 + yb], me).wait_recv()

    def await_sib(yb):
        rcopy(XA.at[yb], XA.at[yb], sent.at[0], s_r.at[yb], me).wait_recv()

    fwd = [
        act(0, left, c, right, c, 6), act(1, right, c, left, c, 7),
        act(0, left, c, y, sib, 8), act(1, right, c, y, sib, 9),
        act(1, left, c, y, sib, 10), act(0, right, c, y, sib, 11),
        act(0, opp, c, y, sib, 12), act(1, opp, c, y, sib, 13),
    ]
    await_act(0, left)
    fwd[0].start()
    fwd[2].start()
    await_act(1, right)
    fwd[1].start()
    fwd[3].start()
    both_ways(OL, 6, o_r, 0, 8)
    unpack(x)
    onward(WL, 4, w_r, 1, 4)
    onward(OL, 6, o_r, 0, 4)
    arrived(WL.at[pl.ds(0, 8)], w_r, 16)
    unpack(xl)
    unpack(xr)
    arrived(WL.at[pl.ds(0, 8)], w_r, 17)
    unpack(xo)

    scale = 1.0 / HEAD_DIM**0.5
    row = lax.broadcasted_iota(jnp.int32, (ROWS, 128), 0)
    col_ = lax.broadcasted_iota(jnp.int32, (ROWS, 128), 1)
    inside = row // FRAMES == col_ // FRAMES
    lane256 = lax.broadcasted_iota(jnp.int32, (ROWS, 256), 1)
    first = lane256 < HEAD_DIM
    zero = jnp.zeros((ROWS, 256), BF)

    def two_heads(v):
        return jnp.concatenate([jnp.where(first, v, zero), jnp.where(first, zero, v)], axis=0)

    def chunk(ids):
        qkv = dot_nn(jnp.concatenate([XA[i] for i in ids], axis=0), WCAT[...]).astype(BF)
        da = dot_nt(jnp.concatenate([DA[i] for i in ids], axis=0), WOC[...]).astype(BF)
        for h in range(2 * len(ids)):
            i, rs, at = ids[h // 2], pl.ds(h % 2 * ROWS, ROWS), slice(h * ROWS, h * ROWS + ROWS)
            q, k, v, g = qkv[at, :256], qkv[at, 256:512], qkv[at, 512:], da[at]
            kk, vv = two_heads(k), two_heads(v)
            sc = dot_nt(kk, q) * scale
            dp = dot_nt(vv, g)
            probs, dscore = [], []
            for n2 in range(2):
                cs = slice(n2 * 128, n2 * 128 + 128)
                s1 = jnp.where(inside, sc[cs], -jnp.inf)
                e = jnp.exp(s1 - jnp.max(s1, axis=0, keepdims=True))
                p1 = e * (1.0 / jnp.sum(e, axis=0, keepdims=True))
                d1 = dp[cs]
                t1 = jnp.sum(d1 * p1, axis=0, keepdims=True)
                probs.append(p1.astype(BF))
                dscore.append((p1 * (d1 - t1) * scale).astype(BF))
            pb = jnp.concatenate(probs, axis=0)
            ds = jnp.concatenate(dscore, axis=0)
            AS[i, rs, :] = dot_tn(pb, vv).astype(BF)
            DQKV[i, rs, :256] = dot_tn(ds, kk).astype(BF)
            dk = dot_nn(ds, q)
            DQKV[i, rs, 256:512] = jnp.where(first, dk[:128], dk[128:]).astype(BF)
            dv = dot_nn(pb, g)
            DQKV[i, rs, 512:] = jnp.where(first, dv[:128], dv[128:]).astype(BF)

    await_act(1, left)
    fwd[4].start()
    await_act(0, right)
    fwd[5].start()
    rest(OL, o_r)

    def oslot(q, r):
        xs = 2 * c + q // 2
        other = (xs + 3) % NX if q // 2 == 0 else (xs + 1) % NX
        xh = jnp.where(c == r % 2, xs, other)
        return (2 * y + 2 - r // 2 + 4) % ZH, xh, q % 2

    def opix(q, r):
        zs, xh, cs = oslot(q, r)
        return (zs * NX + xh) * NC + cs

    WOC[COLS:, :] = jnp.zeros((256 - COLS, D), BF)
    lane12 = lanes(12)
    for q in range(4):
        parts = [None] * 3
        for r in range(NREP):
            WOC[RP * q : RP * q + RP, 128 * r : 128 * r + 128] = OL[opix(q, r), :RP, :]
            tl = OL[opix(q, r), RP : RP + 12, :].astype(F32)
            for t in range(3):
                v = jnp.where(lane12 // 16 == t, tl, 0.0)
                v = roll(v, 16 * (r - t))
                parts[t] = v if parts[t] is None else parts[t] + v
        for t in range(3):
            at = RP * q + 12 * t
            WOC[at : at + 12, 1024:1152] = parts[t].astype(BF)

    def dx_sib(i):
        return rcopy(
            DXP.at[i, pl.ds(pl.multiple_of(sib * ROWS, ROWS), ROWS)], DXS.at[i],
            sent.at[8], dx_r.at[i], (zh, x, sib, y, zl),
        )

    @pl.loop(0, NY)
    def _(n):
        off = jnp.where(n == 1, 3, jnp.where(n == 2, 1, jnp.where(n == 3, 2, 0)))
        i = (y + off) % NY

        @pl.when(n == 1)
        def _():
            await_act(0, opp)
            fwd[6].start()
            await_act(1, opp)
            fwd[7].start()

        await_sib(i)
        chunk((i,))

    OGRP, first_k = 4, (lambda h, side: 4 * side if h == 4 else 2 * h + side)
    bufs = lambda h: (DWO, OXA, OSM, ORL, ORR, O2S) if h == OGRP else (DWS, RXA, SMB, RL, RR, R2S)

    def some(h, side):
        return pl.ds(first_k(h, side), 4 if h == OGRP else 1)

    def to_x(src, dst, rs, h, side):
        return rcopy(src, dst, sent.at[9 + (h == OGRP)], rs, (zh, (xr, xl)[side], c, y, zl))

    def far(h, side):
        ks = some(h, side)
        return to_x(bufs(h)[0].at[xo, ks], bufs(h)[1].at[ks], far_r.at[h * 2 + side], h, side)

    def near(h, side):
        ks = some(h, 1 - side)
        return to_x(bufs(h)[0].at[(xr, xl)[side], ks], bufs(h)[3 + side].at[ks], near_r.at[h], h, side)

    def summed(h, side):
        ks = some(h, side)
        return to_x(bufs(h)[2].at[ks], bufs(h)[3 + side].at[ks], near_r.at[h], h, side)

    def start_both(f, h):
        for side in range(2):
            f(h, side).start()

    def add_far(h):
        own_, got, out = bufs(h)[:3]
        for side in range(2):
            far(h, side).wait_recv()
            for k in range(first_k(h, side), first_k(h, side) + (4 if h == OGRP else 1)):
                out[k] = (own_[(xr, xl)[side], k].astype(F32) + got[k].astype(F32)).astype(BF)
            summed(h, side).start()

    kown = zh * 2 + c

    def r2(h, k):
        src, dst, o = (O2S, OZ, 1) if h == OGRP else (R2S, RZ, 0)
        return rcopy(src.at[k], dst.at[z], sent.at[11 + o], z_r.at[o], (k // 2, x, k % 2, y, c))

    def k_not_self(k):
        return jnp.logical_not((k == kown) & selfcore)

    def send_z(h):
        arrived(DWO.at[pl.ds(0, 2)] if h == OGRP else RL.at[pl.ds(0, 4)], near_r, h)
        own_, _, _, fl, fr, out = bufs(h)
        for side in range(2):
            for k in range(first_k(h, side), first_k(h, side) + (4 if h == OGRP else 1)):
                t = own_[x, k].astype(F32) + fl[k].astype(F32) + fr[k].astype(F32)
                out[k] = t.astype(BF)

                @pl.when(k_not_self(k))
                def _():
                    r2(h, k).start()

    def z_sum(h, buf, src):
        @pl.when(selfcore)
        def _():
            buf[z] = src[kown]

        @pl.when(selfcore)
        def _():
            arrived(buf.at[pl.ds(0, 7)], z_r, h // 4)

        @pl.when(jnp.logical_not(selfcore))
        def _():
            arrived(buf, z_r, h // 4)

        t = buf[0].astype(F32)
        for i in range(1, NZ):
            t = t + buf[i].astype(F32)
        return t.astype(BF)

    attended = AS[...].reshape(NY * 256, 256)[:, :COLS]
    DWOB[...] = dot_tn(attended, DA[...].reshape(NY * 256, D)).astype(BF)
    for q in range(4):
        tt = [DWOB[RP * q + 12 * t : RP * q + 12 * t + 12, 1024:1152].astype(F32) for t in range(3)]
        for r in range(NREP):
            zs, x2, cs = oslot(q, r)
            k = zs * 2 + cs
            DWO[x2, k, :RP, :] = DWOB[RP * q : RP * q + RP, 128 * r : 128 * r + 128]
            tail = None
            for t in range(3):
                v = roll(jnp.where(lane12 // 16 == r, tt[t], 0.0), 16 * (t - r))
                tail = v if tail is None else tail + v
            DWO[x2, k, RP:RO, :] = tail.astype(BF)
    start_both(far, OGRP)
    start_both(near, OGRP)

    dq_all = DQKV[...].reshape(NY * 256, 768)

    def dw_tile(i):
        lhs = XA[:, :, 128 * i : 128 * i + 128].reshape(NY * 256, 128)
        DWB[128 * i : 128 * i + 128, :] = dot_tn(lhs, dq_all).astype(BF)

    def pack(g):
        for q in range(4):
            p = g * 4 + q
            x2, k = (p // 2) % NX, (p // 8) * 2 + p % 2
            base = RP * p
            tail = None
            for s in range(3):
                DWS[x2, k, RP * s : RP * s + RP, :] = DWB[base : base + RP, 256 * s : 256 * s + 128]
                t = DWB[base : base + RP, 256 * s + 128 : 256 * s + 256].astype(F32)
                t = roll(t[: RP // 2], 32 * s) + roll(t[RP // 2 :], 32 * s + 16)
                tail = t if tail is None else tail + t
            DWS[x2, k, 3 * RP : 3 * RP + RP // 2, :] = tail.astype(BF)

    def own_sum(i):
        half = pl.ds(pl.multiple_of(c * ROWS, ROWS), ROWS)
        return DXP[i, half, :].astype(F32) + DXS[i].astype(F32)

    def dx_far(side):
        rows = pl.ds(64 * side, 64)
        return rcopy(
            DXC.at[0, rows], DXH.at[side], sent.at[13], xh_r.at[side],
            (zh, x, c, (right, left)[side], zl),
        )

    def dx_near(side, late):
        at = 64 * side if late else 64 - 64 * side
        i = (right, left)[side]
        t = own_sum(i)[at : at + 64]
        if late:
            t = t + DXH[side].astype(F32)
        DXC[1 + side, at : at + 64, :] = t.astype(BF)
        rows = pl.ds(at, 64)
        rcopy(
            DXC.at[1 + side, rows], DXR.at[side, rows], sent.at[14], dx_r.at[4], (zh, x, c, i, zl)
        ).start()

    def dx_mat(i):
        DXP[i] = dot_nt(DQKV[i], WCAT[...]).astype(BF)
        dx_sib(i).start()

    for i in range(3):
        dw_tile(i)
    for g in range(2):
        pack(g)
    start_both(far, 0)
    start_both(near, 0)
    for i in range(3, 5):
        dw_tile(i)
    for g in range(2, 4):
        pack(g)
    start_both(far, 1)
    dx_mat(opp)
    for i in range(5, 9):
        dw_tile(i)
    for g in range(4, 8):
        pack(g)
    start_both(far, 2)
    add_far(OGRP)
    dx_mat(right)
    add_far(0)
    start_both(near, 1)
    dx_mat(left)
    arrived(DXS.at[opp], dx_r, opp)
    DXC[0] = own_sum(opp).astype(BF)
    for side in range(2):
        dx_far(side).start()
    arrived(DXS.at[right], dx_r, right)
    dx_near(0, False)
    add_far(1)
    start_both(far, 3)
    start_both(near, 2)
    arrived(DXS.at[left], dx_r, left)
    dx_near(1, False)
    send_z(OGRP)
    dx_mat(y)
    add_far(2)
    start_both(near, 3)
    send_z(0)
    add_far(3)
    send_z(1)

    head, foot = pl.ds(0, RA), pl.ds(RA, RO)

    def home_copy():
        r = home[3] * ZL + home[4]
        return rcopy(FO, FL.at[r, foot], sent.at[15], t_r.at[0], home)

    def home_arrival():
        return rcopy(FO, FL.at[rep, foot], sent.at[15], t_r.at[0], me)

    def fin(dr, part, o):
        r = (rep + dr) % NREP
        b = FL.at[rep, part]
        return rcopy(b, b, sent.at[16 + o], f_r.at[o], (zh, x, c, r // ZL, r % ZL))

    send_z(2)
    send_z(3)
    FO[...] = z_sum(OGRP, OZ, O2S)
    home_copy().start()
    for side in range(2):
        dx_far(side).wait_recv()
        dx_near(side, True)
    FL[rep, :RA, :] = z_sum(0, RZ, R2S)

    @pl.loop(1, NREP)
    def _(dr):
        fin(dr, head, 0).start()

    home_arrival().wait_recv()

    @pl.loop(1, NREP)
    def _(dr):
        fin(dr, foot, 1).start()

    arrived(DXS.at[y], dx_r, y)
    arrived(DXR, dx_r, 4)
    GI[...] = (own_sum(y) + DXR[0].astype(F32) + DXR[1].astype(F32)).astype(BF)
    gi_out = pltpu.make_async_copy(GI, gi_ref, lsem.at[0])
    gi_out.start()

    def left_from(ref, idx):
        rcopy(ref, ref, sent.at[idx], t_r.at[0], me).wait_send()

    left_from(XA.at[pl.ds(0, 3)], 0)
    left_from(XA.at[pl.ds(0, 3)], 1)
    left_from(XA.at[0], 2)
    hub_copy().wait_send()

    @pl.when(selfcore)
    def _():
        for b, idx in ((WL, 4), (OL, 6), (RZ, 11), (OZ, 12)):
            left_from(b.at[pl.ds(0, 7)], idx)

    @pl.when(jnp.logical_not(selfcore))
    def _():
        for b, idx in ((WL, 4), (OL, 6), (RZ, 11), (OZ, 12)):
            left_from(b.at[pl.ds(0, 8)], idx)

    left_from(WL.at[pl.ds(0, 24)], 5)
    left_from(OL.at[pl.ds(0, 24)], 7)
    left_from(DXS, 8)
    left_from(DWS.at[pl.ds(0, 3)], 9)
    left_from(DWO.at[pl.ds(0, 3)], 10)
    left_from(DXH, 13)
    left_from(DXR, 14)
    home_copy().wait_send()

    for o, part in enumerate((head, foot)):
        b = FL.at[pl.ds(0, 7), part]
        arrived(b, f_r, o)
        left_from(b, 16 + o)

    lane36 = lanes(RP)
    for s in range(3):
        last, lastt = None, None
        for t in range(9):
            if t < 8:
                main = roll(FL[t, RP * s : RP * s + RP, :].astype(F32), 16 * t)
            out = main
            if t > 0:
                prev = jnp.where(lane36 < 16 * (t - 1), last, lastt)
                out = prev if t == 8 else jnp.where(lane36 >= 16 * t, main, prev)
            GW[:, s * D + 128 * t : s * D + 128 * t + 128] = out.astype(GW.dtype)
            if t < 8:
                last = main
                tl = FL[t, 3 * RP : 3 * RP + RP // 2, :].astype(F32)
                halves = [roll(tl, 16 * t - 32 * s - 16 * h) for h in range(2)]
                lastt = jnp.concatenate(halves, axis=0)
    parts = [None] * 3
    for r in range(NREP):
        at = 3 * D + 128 * r
        GW[:, at : at + 128] = FL[r, RA : RA + RP, :].astype(GW.dtype)
        tl = FL[r, RA + RP : RA + RP + 12, :].astype(F32)
        for t in range(3):
            v = roll(jnp.where(lane12 // 16 == t, tl, 0.0), 16 * (r - t))
            parts[t] = v if parts[t] is None else parts[t] + v
    GW[:, 3 * D + 1024 :] = jnp.concatenate(parts, axis=0).astype(GW.dtype)
    gw_out = pltpu.make_async_copy(GW, gw_ref, lsem.at[1])
    gw_out.start()
    gi_out.wait()
    gw_out.wait()


def finish(gi_ref, gw_ref, gi_out, gw_out, GI, GW, GF, sem):
    ins = [pltpu.make_async_copy(gw_ref, GW, sem.at[0]), pltpu.make_async_copy(gi_ref, GI, sem.at[1])]
    outs = [pltpu.make_async_copy(GF, gw_out, sem.at[2]), pltpu.make_async_copy(GI, gi_out, sem.at[3])]
    for i in ins:
        i.start()
    ins[0].wait()
    GF[...] = GW[...].astype(F32)
    outs[0].start()
    ins[1].wait()
    outs[1].start()
    for o in outs:
        o.wait()


def vm(*shape, dtype=BF):
    return pltpu.VMEM(shape, dtype)


def local(tokens, out_grad, wq, wk, wv, wo):
    rows = tokens.reshape(-1, D)
    drows = out_grad.reshape(-1, D)
    dma = lambda n: pltpu.SemaphoreType.DMA((n,))
    hbm = pl.BlockSpec(memory_space=pl.ANY)
    gi, gw = pl.pallas_call(
        kernel,
        out_shape=(
            jax.ShapeDtypeStruct((ROWS, D), BF),
            jax.ShapeDtypeStruct((RP, 4 * D), BF),
        ),
        in_specs=[hbm] * 6,
        out_specs=(hbm, hbm),
        scratch_shapes=[
            vm(NY, 256, D), vm(NY, 256, D), vm(4, RP, D),
            vm(RA, 128), vm(RO, 128), vm(RO, 128), vm(NPIX, RA, 128), vm(NPIX, RO, 128),
            vm(D, 768), vm(256, D), vm(NY, 256, 768), vm(NY, 256, 256),
            vm(NY, 256, D), vm(NY, ROWS, D), vm(3, ROWS, D), vm(2, 64, D), vm(2, ROWS, D),
            vm(D, 768), vm(COLS, D), vm(NX, 8, RA, 128), *[vm(8, RA, 128)] * 5, vm(NZ, RA, 128),
            vm(NX, 8, RO, 128), *[vm(8, RO, 128)] * 5, vm(NZ, RO, 128),
            vm(RO, 128), vm(NREP, RF, 128), vm(ROWS, D), vm(RP, 4 * D),
            dma(6), dma(18), dma(8), dma(4), dma(1), dma(18), dma(18), dma(5), dma(2), dma(10),
            dma(5), dma(2), dma(1), dma(2),
        ],
        compiler_params=pltpu.CompilerParams(
            collective_id=0, has_side_effects=True, vmem_limit_bytes=60 * 2**20
        ),
    )(rows, drows, wq, wk, wv, wo)
    gi, gw = pl.pallas_call(
        finish,
        out_shape=(
            jax.ShapeDtypeStruct((ROWS, D), BF),
            jax.ShapeDtypeStruct((RP, 4 * D), F32),
        ),
        in_specs=[hbm] * 2,
        out_specs=(hbm, hbm),
        scratch_shapes=[vm(ROWS, D), vm(RP, 4 * D), vm(RP, 4 * D, dtype=F32), dma(4)],
        compiler_params=pltpu.CompilerParams(vmem_limit_bytes=63 * 2**20),
    )(gi, gw)
    return gi.reshape(tokens.shape), gw


def solution(mesh):
    torus = Mesh(mesh.devices.reshape(ZH, NX, NC, NY, ZL), AXES)
    act = P(AXES, None, None)
    w = P(("zh", "x", "c"), None)
    return jax.shard_map(
        local,
        mesh=torus,
        in_specs=(act, act, w, w, w, w),
        out_specs=(act, w),
        check_vma=False,
    )
```
